32 devices in a mesh: rep: 4 (over y, core), shard: 8 (over z, x).
Axes of the slice: x: 2, y: 2, z: 4, core: 2. Of those that a mesh axis runs over, the one named last changes fastest.
Arguments:
- tokens_in: bfloat16 [8192, 1152], P(('rep', 'shard')), may hold values from -6 to 6
- cotangent: bfloat16 [8192, 1152], P(('rep', 'shard'))
- segment_ids: int32 [32, 256], P(('rep', 'shard')), may hold values from 0 to 12, never falling along the last dimension, each value on 1 to 64 neighbouring positions
- parent_ids: int32 [32, 13], P(('rep', 'shard')), may hold values from 0 to 11, as said below
- weight_query: bfloat16 [1152, 1152], P('shard')
- weight_key: bfloat16 [1152, 384], P('shard')
- weight_value: bfloat16 [1152, 384], P('shard')
- weight_output: bfloat16 [1152, 1152], P('shard')
- weight_gate: bfloat16 [1152, 3072], P('shard')
- weight_up: bfloat16 [1152, 3072], P('shard')
- weight_down: bfloat16 [1152, 3072], P('shard')
- norm_attention: float32 [1152], replicated, may hold values from 0.25 to 1.75
- norm_feedforward: float32 [1152], replicated, may hold values from 0.25 to 1.75
- moment_query: float32 [1152, 1152], P('shard')
- moment_key: float32 [1152, 384], P('shard')
- moment_value: float32 [1152, 384], P('shard')
- moment_output: float32 [1152, 1152], P('shard')
- moment_gate: float32 [1152, 3072], P('shard')
- moment_up: float32 [1152, 3072], P('shard')
- moment_down: float32 [1152, 3072], P('shard')
- variance_query: float32 [1152, 1152], P('shard'), as said below
- variance_key: float32 [1152, 384], P('shard'), as said below
- variance_value: float32 [1152, 384], P('shard'), as said below
- variance_output: float32 [1152, 1152], P('shard'), as said below
- variance_gate: float32 [1152, 3072], P('shard'), as said below
- variance_up: float32 [1152, 3072], P('shard'), as said below
- variance_down: float32 [1152, 3072], P('shard'), as said below
- moment_norm_attention: float32 [1152], replicated, may hold values from -448 to 448
- moment_norm_feedforward: float32 [1152], replicated, may hold values from -160 to 160
- variance_norm_attention: float32 [1152], replicated, may hold values from 163.84 to 1228.8
- variance_norm_feedforward: float32 [1152], replicated, may hold values from 16.384 to 163.84
Outputs:
- layer_out: bfloat16 [8192, 1152], P(('rep', 'shard'))
- tokens_grad: bfloat16 [8192, 1152], P(('rep', 'shard'))
- update_query: float32 [1152, 1152], P('shard')
- update_key: float32 [1152, 384], P('shard')
- update_value: float32 [1152, 384], P('shard')
- update_output: float32 [1152, 1152], P('shard')
- update_gate: float32 [1152, 3072], P('shard')
- update_up: float32 [1152, 3072], P('shard')
- update_down: float32 [1152, 3072], P('shard')
- next_moment_query: float32 [1152, 1152], P('shard')
- next_moment_key: float32 [1152, 384], P('shard')
- next_moment_value: float32 [1152, 384], P('shard')
- next_moment_output: float32 [1152, 1152], P('shard')
- next_moment_gate: float32 [1152, 3072], P('shard')
- next_moment_up: float32 [1152, 3072], P('shard')
- next_moment_down: float32 [1152, 3072], P('shard')
- next_variance_query: float32 [1152, 1152], P('shard')
- next_variance_key: float32 [1152, 384], P('shard')
- next_variance_value: float32 [1152, 384], P('shard')
- next_variance_output: float32 [1152, 1152], P('shard')
- next_variance_gate: float32 [1152, 3072], P('shard')
- next_variance_up: float32 [1152, 3072], P('shard')
- next_variance_down: float32 [1152, 3072], P('shard')
- update_norm_attention: float32 [1152], replicated
- update_norm_feedforward: float32 [1152], replicated
- next_moment_norm_attention: float32 [1152], replicated
- next_moment_norm_feedforward: float32 [1152], replicated
- next_variance_norm_attention: float32 [1152], replicated
- next_variance_norm_feedforward: float32 [1152], replicated
- norm_pairs: float32 [9, 2], replicated
The draws below stay inside these ranges and needn't reach their ends.
Inputs may be any that keep to these rules, and one draw needn't show every extreme that they name: `segment_ids`: within a tree's row the segments never fall and each of the 13 segments is present. `parent_ids`: entry s of a row is the parent of segment s, a segment below s for s >= 1; entry 0 is 0. `variance_query`: positive. `variance_key`: positive. `variance_value`: positive. `variance_output`: positive. `variance_gate`: positive. `variance_up`: positive. `variance_down`: positive.
All inputs are finite; a program needn't handle non-finite values.
Results may differ from the reference program's by a relative error of at most 0.025.
Values may be sent and summed in bfloat16 or wider, within the bound.
A program may use at most 256 MiB of HBM per device.

```python
import math
import jax
import jax.numpy as jnp
import numpy as np
from jax import lax

D = 1152
HEADS = 18
KV_HEADS = 6
HEAD_DIM = 64
FF = 3072
TOK_DEV = 256
SEGS = 13
TREES = 32
TOKENS = 8192
REPLICAS = 4
GROUP_SIZE = 8


def rising_rows(source, row_count, col_count, spread):
    first_key, second_key = jax.random.split(source)
    sample = jax.random.truncated_normal(first_key, -4.0, 4.0, (row_count, col_count), jnp.float32)
    position = jnp.arange(row_count, dtype=jnp.float32) / max(row_count - 1, 1) - 0.5
    jitter = jax.random.uniform(second_key, (row_count,), jnp.float32, 0.8, 1.25)
    factor = jnp.exp(position * 1.0986123) * jitter
    return sample * spread * factor[:, None]


def positive_rows(source, row_count, col_count, level):
    exponent = jax.random.uniform(source, (row_count, col_count), jnp.float32, -1.2039728, 1.0986123)
    return level * jnp.exp(exponent)


def moment_level(weight_scale):
    return 0.11 * weight_scale * math.sqrt(TOKENS)


def variance_level(weight_scale):
    return 0.001 * weight_scale * weight_scale * TOKENS


def draw_cotangent(key, part):
    source = jax.random.fold_in(key, 401)
    sample = jax.random.truncated_normal(source, -4.0, 4.0, (TOKENS, D), jnp.float32)
    device_rows = jnp.arange(TOKENS, dtype=jnp.int32) // TOK_DEV
    replica_place = (device_rows // GROUP_SIZE).astype(jnp.float32) / max(REPLICAS - 1, 1)
    shard_place = (device_rows % GROUP_SIZE).astype(jnp.float32) / max(GROUP_SIZE - 1, 1)
    factor = jnp.exp((replica_place + shard_place - 1.0) * 1.0986123)
    return (sample * factor[:, None]).astype(jnp.bfloat16)


def draw_parent_ids(key, part):
    limits = jnp.maximum(jnp.arange(SEGS, dtype=jnp.int32), 1)
    drawn = jax.random.randint(jax.random.fold_in(key, 501), (TREES, SEGS), 0, limits[None, :], dtype=jnp.int32)
    tree_index = jnp.arange(TREES, dtype=jnp.int32)
    segment_index = jnp.arange(SEGS, dtype=jnp.int32)
    forced = (tree_index[:, None] == 0) & (segment_index[None, :] == SEGS - 1)
    return jnp.where(forced, SEGS - 2, drawn).astype(jnp.int32)


def draw_weight_query(key, part):
    return rising_rows(jax.random.fold_in(key, 101), D, HEADS * HEAD_DIM, 1.41 / math.sqrt(D)).astype(jnp.bfloat16)


def draw_weight_key(key, part):
    return rising_rows(jax.random.fold_in(key, 102), D, KV_HEADS * HEAD_DIM, 1.41 / math.sqrt(D)).astype(jnp.bfloat16)


def draw_weight_value(key, part):
    return rising_rows(jax.random.fold_in(key, 103), D, KV_HEADS * HEAD_DIM, 1.0 / math.sqrt(D)).astype(jnp.bfloat16)


def draw_weight_output(key, part):
    return rising_rows(jax.random.fold_in(key, 104), D, HEADS * HEAD_DIM, 3.3 / math.sqrt(HEADS * HEAD_DIM)).astype(jnp.bfloat16)


def draw_weight_gate(key, part):
    return rising_rows(jax.random.fold_in(key, 105), D, FF, 1.0 / math.sqrt(D)).astype(jnp.bfloat16)


def draw_weight_up(key, part):
    return rising_rows(jax.random.fold_in(key, 106), D, FF, 1.0 / math.sqrt(D)).astype(jnp.bfloat16)


def draw_weight_down(key, part):
    return rising_rows(jax.random.fold_in(key, 107), D, FF, 2.42 / math.sqrt(FF)).astype(jnp.bfloat16)


def draw_moment_query(key, part):
    return rising_rows(jax.random.fold_in(key, 201), D, HEADS * HEAD_DIM, moment_level(11.3))


def draw_moment_key(key, part):
    return rising_rows(jax.random.fold_in(key, 202), D, KV_HEADS * HEAD_DIM, moment_level(19.8))


def draw_moment_value(key, part):
    return rising_rows(jax.random.fold_in(key, 203), D, KV_HEADS * HEAD_DIM, moment_level(15.0))


def draw_moment_output(key, part):
    return rising_rows(jax.random.fold_in(key, 204), D, HEADS * HEAD_DIM, moment_level(0.55))


def draw_moment_gate(key, part):
    return rising_rows(jax.random.fold_in(key, 205), D, FF, moment_level(0.9))


def draw_moment_up(key, part):
    return rising_rows(jax.random.fold_in(key, 206), D, FF, moment_level(0.9))


def draw_moment_down(key, part):
    return rising_rows(jax.random.fold_in(key, 207), D, FF, moment_level(0.9))


def draw_variance_query(key, part):
    return positive_rows(jax.random.fold_in(key, 301), D, HEADS * HEAD_DIM, variance_level(11.3))


def draw_variance_key(key, part):
    return positive_rows(jax.random.fold_in(key, 302), D, KV_HEADS * HEAD_DIM, variance_level(19.8))


def draw_variance_value(key, part):
    return positive_rows(jax.random.fold_in(key, 303), D, KV_HEADS * HEAD_DIM, variance_level(15.0))


def draw_variance_output(key, part):
    return positive_rows(jax.random.fold_in(key, 304), D, HEADS * HEAD_DIM, variance_level(0.55))


def draw_variance_gate(key, part):
    return positive_rows(jax.random.fold_in(key, 305), D, FF, variance_level(0.9))


def draw_variance_up(key, part):
    return positive_rows(jax.random.fold_in(key, 306), D, FF, variance_level(0.9))


def draw_variance_down(key, part):
    return positive_rows(jax.random.fold_in(key, 307), D, FF, variance_level(0.9))


def steps_of(own_key, dims, cuts, low, largest):
    def one(dim, parts):
        heights = jax.random.uniform(jax.random.fold_in(jax.random.fold_in(own_key, 6), dim), (parts,), jnp.float32, low / len(cuts), largest / len(cuts))
        return jnp.repeat(jnp.exp(heights), dims[dim] // parts).reshape((-1,) + (1,) * (len(dims) - dim - 1))

    level = one(*cuts[0])
    for cut in cuts[1:]:
        level = level * one(*cut)
    return level


def split_up(amount, total, bound, slope):
    weights = [(1 << 20) // math.isqrt(rank ** slope) + 1 for rank in range(2, amount + 1)]
    surplus, given = total - bound - (amount - 1), [1] * (amount - 1)
    while surplus > 0:
        movable = [i for i in range(amount - 1) if given[i] < bound]
        pool, left = sum([weights[i] for i in movable]), surplus
        for i in movable:
            addition = min(bound - given[i], max(1, left * weights[i] // pool), surplus)
            given[i] = given[i] + addition
            surplus = surplus - addition
    return np.array([bound] + given)


def uneven(own_key, amount, total, reach, skew):
    if amount == 2:
        one = jax.random.randint(own_key, (), max(1, total - reach), min(reach, total - 1) + 1)
        return jnp.stack([one, total - one])
    tallies = jnp.asarray(split_up(amount, total, reach, skew), jnp.int32)
    pairs = (amount - 1) // 2
    donor, receiver = tallies[1:1 + 2 * pairs:2], tallies[2:2 + 2 * pairs:2]
    room = jnp.minimum(donor - 1, reach - receiver)
    moved = jax.random.randint(jax.random.fold_in(own_key, 1), (pairs,), 0, 1 << 20) % (room + 1)
    tallies = tallies.at[1:1 + 2 * pairs:2].set(donor - moved).at[2:2 + 2 * pairs:2].set(receiver + moved)
    return tallies[jax.random.permutation(jax.random.fold_in(own_key, 2), amount)]


def normal_values(rng, shape, width, bound, shards=(), held_as=jnp.bfloat16):
    array = jax.random.normal(rng, shape, jnp.float32) * width
    if len(shards) > 0:
        array = steps_of(rng, shape, shards, -0.22, 0.18) * array
    return jnp.clip(array, min=-bound, max=bound).astype(held_as)


def setup_inputs(seed: int = 0) -> dict:
    arg_keys = jax.random.split(jax.random.key(seed), 32)
    tokens_in = normal_values(arg_keys[0], (TOKENS, D), 1.0, 6.0, ((0, 32),))
    cotangent = draw_cotangent(jax.random.fold_in(arg_keys[31], 71), 0)
    segment_ids = jax.vmap(lambda own: jnp.searchsorted(jnp.cumsum(uneven(own, SEGS, TOK_DEV, TOK_DEV // 4, 2)), jnp.arange(TOK_DEV), side="right"))(jax.random.split(arg_keys[2], TREES)).reshape((TREES, TOK_DEV)).astype(jnp.int32)
    parent_ids = draw_parent_ids(jax.random.fold_in(arg_keys[31], 71), 0)
    weight_query = draw_weight_query(jax.random.fold_in(arg_keys[31], 71), 0)
    weight_key = draw_weight_key(jax.random.fold_in(arg_keys[31], 71), 0)
    weight_value = draw_weight_value(jax.random.fold_in(arg_keys[31], 71), 0)
    weight_output = draw_weight_output(jax.random.fold_in(arg_keys[31], 71), 0)
    weight_gate = draw_weight_gate(jax.random.fold_in(arg_keys[31], 71), 0)
    weight_up = draw_weight_up(jax.random.fold_in(arg_keys[31], 71), 0)
    weight_down = draw_weight_down(jax.random.fold_in(arg_keys[31], 71), 0)
    norm_attention = jnp.clip(1.0 + 0.15 * jax.random.normal(arg_keys[11], (D,), jnp.float32), 0.25, 1.75)
    norm_feedforward = jnp.clip(1.0 + 0.15 * jax.random.normal(arg_keys[12], (D,), jnp.float32), 0.25, 1.75)
    moment_query = draw_moment_query(jax.random.fold_in(arg_keys[31], 71), 0)
    moment_key = draw_moment_key(jax.random.fold_in(arg_keys[31], 71), 0)
    moment_value = draw_moment_value(jax.random.fold_in(arg_keys[31], 71), 0)
    moment_output = draw_moment_output(jax.random.fold_in(arg_keys[31], 71), 0)
    moment_gate = draw_moment_gate(jax.random.fold_in(arg_keys[31], 71), 0)
    moment_up = draw_moment_up(jax.random.fold_in(arg_keys[31], 71), 0)
    moment_down = draw_moment_down(jax.random.fold_in(arg_keys[31], 71), 0)
    variance_query = draw_variance_query(jax.random.fold_in(arg_keys[31], 71), 0)
    variance_key = draw_variance_key(jax.random.fold_in(arg_keys[31], 71), 0)
    variance_value = draw_variance_value(jax.random.fold_in(arg_keys[31], 71), 0)
    variance_output = draw_variance_output(jax.random.fold_in(arg_keys[31], 71), 0)
    variance_gate = draw_variance_gate(jax.random.fold_in(arg_keys[31], 71), 0)
    variance_up = draw_variance_up(jax.random.fold_in(arg_keys[31], 71), 0)
    variance_down = draw_variance_down(jax.random.fold_in(arg_keys[31], 71), 0)
    moment_norm_attention = normal_values(arg_keys[27], (D,), (0.8 * TOKENS ** 0.5), 448.0, (), jnp.float32)
    moment_norm_feedforward = normal_values(arg_keys[28], (D,), (0.28 * TOKENS ** 0.5), 160.0, (), jnp.float32)
    variance_norm_attention = jnp.clip(jnp.exp(jax.random.uniform(arg_keys[29], (D,), jnp.float32, math.log(163.84), math.log(1228.8))), 163.84, 1228.8)
    variance_norm_feedforward = jnp.clip(jnp.exp(jax.random.uniform(arg_keys[30], (D,), jnp.float32, math.log(16.384), math.log(163.84))), 16.384, 163.84)
    return dict(tokens_in=tokens_in, cotangent=cotangent, segment_ids=segment_ids, parent_ids=parent_ids, weight_query=weight_query, weight_key=weight_key, weight_value=weight_value, weight_output=weight_output, weight_gate=weight_gate, weight_up=weight_up, weight_down=weight_down, norm_attention=norm_attention, norm_feedforward=norm_feedforward, moment_query=moment_query, moment_key=moment_key, moment_value=moment_value, moment_output=moment_output, moment_gate=moment_gate, moment_up=moment_up, moment_down=moment_down, variance_query=variance_query, variance_key=variance_key, variance_value=variance_value, variance_output=variance_output, variance_gate=variance_gate, variance_up=variance_up, variance_down=variance_down, moment_norm_attention=moment_norm_attention, moment_norm_feedforward=moment_norm_feedforward, variance_norm_attention=variance_norm_attention, variance_norm_feedforward=variance_norm_feedforward)


ROPE_BASE = 10000.0
ATTENTION_SCALE = 0.125
RESIDUAL_SCALE = 1.0
NORM_EPS = 1e-05
BETA_FIRST = 0.9
BETA_SECOND = 0.999
ADAM_EPS = 1e-06
DECAY_RATE = 0.01
STEP_RATE = 0.25
TRUST_EPS = 1e-06
MASK_FILL = -1e+30

@jax.custom_vjp
def low(v):
    return lax.optimization_barrier(v.astype(jnp.bfloat16)).astype(jnp.float32)

@jax.custom_vjp
def low_back(v):
    return v

def low_keep(v):
    return (low(v), None)

def low_pass(kept, grad):
    return (grad,)

def back_keep(v):
    return (v, None)

def back_low(kept, grad):
    return (low(grad),)
low.defvjp(low_keep, low_pass)
low_back.defvjp(back_keep, back_low)

def tree_layout(segment_row, parent_row):
    segment_count = parent_row.shape[0]
    labels = jnp.arange(segment_count, dtype=jnp.int32)
    parent_hot = (parent_row[:, None] == labels[None, :]).astype(jnp.int32)
    identity = (labels[:, None] == labels[None, :]).astype(jnp.int32)

    def climb(counter, ancestry):
        return jnp.minimum(identity + jnp.dot(parent_hot, ancestry), 1).astype(jnp.int32)
    ancestry = lax.fori_loop(0, segment_count, climb, identity)
    segment_hot = (segment_row[:, None] == labels[None, :]).astype(jnp.int32)
    lengths = lax.optimization_barrier(jnp.sum(segment_hot, axis=0, dtype=jnp.int32))
    depth_sum = jnp.dot(ancestry - identity, lengths).astype(jnp.int32)
    token_index = jnp.arange(segment_row.shape[0], dtype=jnp.int32)
    earlier = lax.optimization_barrier(jnp.sum((segment_row[None, :] < segment_row[:, None]).astype(jnp.int32), axis=1, dtype=jnp.int32))
    positions = token_index - earlier + jnp.dot(segment_hot, depth_sum).astype(jnp.int32)
    reach_count = jnp.dot(jnp.dot(segment_hot, ancestry), segment_hot.T)
    visible = (reach_count > 0) & (token_index[None, :] <= token_index[:, None])
    return (positions, visible)

def rope_tables(positions, head_size):
    half_size = head_size // 2
    exponent = jnp.arange(half_size, dtype=jnp.float32) * (-2.0 / head_size)
    frequency = jnp.power(ROPE_BASE, exponent)
    angles = positions.astype(jnp.float32)[:, None] * frequency[None, :]
    angles = jnp.concatenate([angles, angles], axis=1)
    return (jnp.cos(angles), jnp.sin(angles))

def rotate(states, cosine_table, sine_table):
    half_size = states.shape[-1] // 2
    turned = jnp.concatenate([-states[..., half_size:], states[..., :half_size]], axis=-1)
    return states * cosine_table[:, None, :] + turned * sine_table[:, None, :]

def product(left_side, right_side):
    return jnp.dot(left_side, right_side, preferred_element_type=jnp.float32, precision=lax.Precision.HIGHEST)

def normalize(inputs):
    return inputs * lax.rsqrt(lax.optimization_barrier(jnp.mean(inputs * inputs, axis=-1, keepdims=True)) + NORM_EPS)

def tree_attention(pieces):
    query_rows, key_rows, value_rows, cosine_table, sine_table, visible = pieces
    per_group = HEADS // KV_HEADS
    query_turned = low(rotate(query_rows.reshape(TOK_DEV, HEADS, HEAD_DIM), cosine_table, sine_table))
    query_turned = query_turned.reshape(TOK_DEV, KV_HEADS, per_group, HEAD_DIM)
    key_turned = low(rotate(key_rows.reshape(TOK_DEV, KV_HEADS, HEAD_DIM), cosine_table, sine_table))
    value_heads = value_rows.reshape(TOK_DEV, KV_HEADS, HEAD_DIM)
    scores = ATTENTION_SCALE * jnp.einsum('tkgd,ukd->kgtu', query_turned, key_turned, precision=lax.Precision.HIGHEST)
    scores = low_back(scores)
    scores = jnp.where(visible[None, None], scores, MASK_FILL)
    softmax_low = low(jnp.exp(scores - jax.nn.logsumexp(scores, axis=-1, keepdims=True)))
    mixed = jnp.einsum('kgtu,ukd->tkgd', softmax_low, value_heads, precision=lax.Precision.HIGHEST)
    return mixed.reshape(TOK_DEV, HEADS * HEAD_DIM)

def layer(inputs, weight_query, weight_key, weight_value, weight_output, weight_gate, weight_up, weight_down, norm_attention, norm_feedforward, cosine_table, sine_table, visible):
    normed_one = low(normalize(inputs) * norm_attention)
    query_states = low_back(product(normed_one, weight_query))
    key_states = low_back(product(normed_one, weight_key))
    value_states = low(low_back(product(normed_one, weight_value)))
    pieces = (query_states.reshape(TREES, TOK_DEV, HEADS * HEAD_DIM), key_states.reshape(TREES, TOK_DEV, KV_HEADS * HEAD_DIM), value_states.reshape(TREES, TOK_DEV, KV_HEADS * HEAD_DIM), cosine_table, sine_table, visible)
    mixed = lax.map(jax.checkpoint(tree_attention), pieces).reshape(TREES * TOK_DEV, HEADS * HEAD_DIM)
    mixed = low(low_back(mixed))
    hidden_state = inputs + RESIDUAL_SCALE * low_back(product(mixed, weight_output.T))
    normed_two = low(normalize(hidden_state) * norm_feedforward)
    gate_states = low_back(product(normed_two, weight_gate))
    up_states = low_back(product(normed_two, weight_up))
    activated = low(jax.nn.silu(gate_states) * up_states)
    return hidden_state + RESIDUAL_SCALE * low_back(product(activated, weight_down.T))

def lamb_step(weight, gradient, moment, variance):
    next_moment = BETA_FIRST * moment + (1.0 - BETA_FIRST) * gradient
    next_variance = BETA_SECOND * variance + (1.0 - BETA_SECOND) * gradient * gradient
    direction = next_moment / (jnp.sqrt(next_variance) + ADAM_EPS) + DECAY_RATE * weight
    weight_sum = jnp.sum(weight * weight)
    step_sum = jnp.sum(direction * direction)
    update = -STEP_RATE * jnp.sqrt(weight_sum) * lax.rsqrt(step_sum + TRUST_EPS) * direction
    return (update, next_moment, next_variance, jnp.stack([jnp.sqrt(weight_sum), jnp.sqrt(step_sum)]))

def reference(tokens_in, cotangent, segment_ids, parent_ids, weight_query, weight_key, weight_value, weight_output, weight_gate, weight_up, weight_down, norm_attention, norm_feedforward, moment_query, moment_key, moment_value, moment_output, moment_gate, moment_up, moment_down, variance_query, variance_key, variance_value, variance_output, variance_gate, variance_up, variance_down, moment_norm_attention, moment_norm_feedforward, variance_norm_attention, variance_norm_feedforward):
    positions, visible = jax.vmap(tree_layout)(segment_ids, parent_ids)
    cosine_table, sine_table = jax.vmap(lambda row_positions: rope_tables(row_positions, HEAD_DIM))(positions)
    params = [weight_query.astype(jnp.float32), weight_key.astype(jnp.float32), weight_value.astype(jnp.float32), weight_output.astype(jnp.float32), weight_gate.astype(jnp.float32), weight_up.astype(jnp.float32), weight_down.astype(jnp.float32), norm_attention, norm_feedforward]
    inputs = tokens_in.astype(jnp.float32)

    def forward(layer_inputs, *weights):
        return layer(layer_inputs, *weights, cosine_table, sine_table, visible)
    result, pullback = jax.vjp(forward, inputs, *params)
    gradients = pullback(cotangent.astype(jnp.float32))
    moments = [moment_query, moment_key, moment_value, moment_output, moment_gate, moment_up, moment_down, moment_norm_attention, moment_norm_feedforward]
    variances = [variance_query, variance_key, variance_value, variance_output, variance_gate, variance_up, variance_down, variance_norm_attention, variance_norm_feedforward]
    outcomes = [lamb_step(weight, gradient, moment, variance) for weight, gradient, moment, variance in zip(params, gradients[1:], moments, variances)]
    updates = [entry[0] for entry in outcomes]
    next_moments = [entry[1] for entry in outcomes]
    next_variances = [entry[2] for entry in outcomes]
    norm_pairs = jnp.stack([entry[3] for entry in outcomes])
    return (result.astype(jnp.bfloat16), gradients[0].astype(jnp.bfloat16), updates[0], updates[1], updates[2], updates[3], updates[4], updates[5], updates[6], next_moments[0], next_moments[1], next_moments[2], next_moments[3], next_moments[4], next_moments[5], next_moments[6], next_variances[0], next_variances[1], next_variances[2], next_variances[3], next_variances[4], next_variances[5], next_variances[6], updates[7], updates[8], next_moments[7], next_moments[8], next_variances[7], next_variances[8], norm_pairs)
```

```python
import functools

import jax
import jax.numpy as jnp
from jax import lax
from jax.experimental import pallas as pl
from jax.experimental.pallas import tpu as pltpu
from jax.sharding import PartitionSpec as P

MESH = pl.DeviceIdType.MESH

HEADS = 18
KV_HEADS = 6
HEAD_DIM = 64


ROPE_BASE = 10000.0
ATTENTION_SCALE = 0.125
RESIDUAL_SCALE = 1.0
NORM_EPS = 1e-05
BETA_FIRST = 0.9
BETA_SECOND = 0.999
ADAM_EPS = 1e-06
DECAY_RATE = 0.01
STEP_RATE = 0.25
TRUST_EPS = 1e-06
MASK_FILL = -1e30


def shard_factors(count):
    factors = []
    while count > 4:
        factors.append(4)
        count //= 4
    factors.append(count)
    return tuple(factors)

def coordinates(index, factors):
    out = []
    for factor in reversed(factors):
        out.append(lax.rem(index, factor))
        index = lax.div(index, factor)
    return out[::-1]

def index_of(coords, factors):
    index = 0
    for c, f in zip(coords, factors):
        index = index * f + c
    return index

def gather_chunks(width, blocks):
    out = []
    for b in range(blocks):
        wide, narrow = [], []
        start = 0
        n = width // 512
        kinds = [True, False, True, True, False, True][:n]
        for i in range(n):
            out.append((b, i * 512, 512, kinds[i % 6]))
    return out

def gather_kernel(factors, blocks, *refs):
    srcs, outs = refs[:blocks], refs[blocks:2*blocks]
    local_sem, send_sem, recv_sem = refs[2*blocks:]
    rep, shard = lax.axis_index("rep"), lax.axis_index("shard")
    y, core = lax.div(rep, 2), lax.rem(rep, 2)
    coords = coordinates(shard, factors)
    peers = []
    for i, f in enumerate(factors):
        ids = []
        for d in range(1, f):
            moved = list(coords); moved[i] = lax.rem(coords[i] + d, f)
            ids.append((rep, index_of(moved, factors)))
        peers.append(ids)
    peers.append([((1 - y) * 2 + core, shard)])
    peers.append([(y * 2 + 1 - core, shard)])
    flat = [p for ids in peers for p in ids]
    barrier = pltpu.get_barrier_semaphore()
    for p in flat:
        pl.semaphore_signal(barrier, inc=1, device_id=p, device_id_type=MESH)
    chunks = gather_chunks(srcs[0].shape[1], blocks)
    nph = len(factors) + 2
    base = []
    total = 0
    for ids in peers:
        base.append(total); total += len(ids)
    def columns(k):
        b, c0, w, split = chunks[k]
        if split:
            q = w // 4
            return c0 + (core * 2 + y) * q, q
        return c0 + core * (w // 2), w // 2
    locals_ = []
    for k, (b, c0, w, split) in enumerate(chunks):
        off, width = columns(k)
        cols = pl.ds(pl.multiple_of(off, 128), width)
        cp = pltpu.make_async_copy(srcs[b].at[:, cols], outs[b].at[tuple(coords) + (slice(None), cols)], local_sem.at[k])
        cp.start(); locals_.append(cp)
    pl.semaphore_wait(barrier, len(flat))
    def copies(k, ph):
        b, c0, w, split = chunks[k]
        off, width = columns(k)
        nf = len(factors)
        if ph < nf:
            lead = (slice(None),) * ph + tuple(coords[ph:])
        else:
            lead = (slice(None),) * nf
            if ph == nf + 1:
                off, width = c0 + core * (w // 2), w // 2
        cols = pl.ds(pl.multiple_of(off, 128), width)
        where = lead + (slice(None), cols)
        src = srcs[b].at[:, cols] if ph == 0 else outs[b].at[where]
        return [pltpu.make_async_remote_copy(src_ref=src, dst_ref=outs[b].at[where],
                  send_sem=send_sem.at[k, base[ph] + j], recv_sem=recv_sem.at[k, base[ph] + j], device_id=p, device_id_type=MESH)
                for j, p in enumerate(peers[ph])]
    n = len(chunks)
    started = {}
    def start(k, ph):
        cs = copies(k, ph)
        for c in cs: c.start()
        started[k, ph] = cs
    def phases(k):
        return [p for p in range(nph) if p != nph - 2 or chunks[k][3]]
    ahead = 4
    for k in range(min(ahead, n)):
        start(k, 0)
    for t in range(n + 2 * nph):
        for lag in range(nph - 1, -1, -1):
            k = t - 2 * lag
            if 0 <= k < n:
                ps = phases(k)
                if lag < len(ps):
                    for c in started[k, ps[lag]]: c.wait_recv()
                    if lag == 0:
                        locals_[k].wait()
                        if k + ahead < n:
                            start(k + ahead, 0)
                    if lag + 1 < len(ps): start(k, ps[lag + 1])
    for cs in started.values():
        for c in cs: c.wait_send()

def gather_weights(shards, shard_count, rep_count=4):
    blocks = len(shards)
    factors = shard_factors(shard_count)
    rows, width = shards[0].shape
    n = len(gather_chunks(width, blocks))
    total = sum(f - 1 for f in factors) + 2
    outs = pl.pallas_call(
        functools.partial(gather_kernel, factors, blocks),
        out_shape=[jax.ShapeDtypeStruct(factors + (rows, width), jnp.bfloat16)] * blocks,
        in_specs=[pl.BlockSpec(memory_space=pltpu.VMEM)] * blocks,
        out_specs=[pl.BlockSpec(memory_space=pl.ANY)] * blocks,
        scratch_shapes=[pltpu.SemaphoreType.DMA((n,)), pltpu.SemaphoreType.DMA((n, total)), pltpu.SemaphoreType.DMA((n, total))],
        compiler_params=pltpu.CompilerParams(collective_id=0, has_side_effects=True),
        name="gather_weights",
    )(*shards)
    return [o.reshape(shard_count * rows, width) for o in outs]


def scatter_kernel(factors, parts, blocks, layout, *refs):
    nf = len(factors)
    nl = len(layout["lefts"])
    lefts = refs[:nl]
    rights = refs[nl:nl + blocks]
    small_in = refs[nl + blocks]
    outs = refs[nl + blocks + 1:nl + 2 * blocks + 1]
    small_out = refs[nl + 2 * blocks + 1]
    scratch = list(refs[nl + 2 * blocks + 2:])
    stage, pair_in, wide_y, final = scratch[:4]
    lean = scratch[4:4 + nf]
    quart = scratch[4 + nf:4 + 2 * nf]
    lean_y = scratch[4 + 2 * nf]
    small = scratch[5 + 2 * nf:5 + 2 * nf + nf + 2]
    send_sem, recv_sem, out_sem, small_send, small_recv = scratch[5 + 2 * nf + nf + 2:]
    rows = final.shape[1]
    steps = final.shape[0]
    ring = stage.shape[0]
    rep, shard = lax.axis_index("rep"), lax.axis_index("shard")
    y, core = lax.div(rep, 2), lax.rem(rep, 2)
    coords = coordinates(shard, factors)
    y_peer = ((1 - y) * 2 + core, shard)
    core_peer = (y * 2 + 1 - core, shard)

    def factor_peer(i, d):
        moved = list(coords)
        moved[i] = lax.rem(coords[i] + d, factors[i])
        return (rep, index_of(moved, factors)), moved[i]

    everyone = [y_peer, core_peer]
    for i, f in enumerate(factors):
        everyone += [factor_peer(i, d)[0] for d in range(1, f)]
    barrier = pltpu.get_barrier_semaphore()
    for p in everyone:
        pl.semaphore_signal(barrier, inc=1, device_id=p, device_id_type=MESH)

    order = list(range(nf - 1, -1, -1))
    column = {"core": 0, "y_wide": 1, "y_lean": 2, "y_back": 3, "core_back": 4}
    used = 5
    for i in order:
        column["lean", i] = used
        used += factors[i] - 1
        column["quart", i] = used
        used += factors[i] - 1

    def remote(k, c, src, dst, peer):
        return pltpu.make_async_remote_copy(
            src_ref=src, dst_ref=dst, send_sem=send_sem.at[lax.rem(k, ring), c],
            recv_sem=recv_sem.at[k, c], device_id=peer, device_id_type=MESH)

    half, quarter = 512, 128
    mine = pl.multiple_of(core * half, half)
    other = pl.multiple_of((1 - core) * half, half)
    my_q = pl.multiple_of(256 + y * quarter, quarter)
    other_q = pl.multiple_of(256 + (1 - y) * quarter, quarter)
    whole = (slice(None),) * nf

    def core_copy(k):
        slot = lax.rem(k, ring)
        return [remote(k, column["core"], stage.at[(slot,) + whole + (slice(None), pl.ds(other, half))], pair_in.at[k], core_peer)]

    def y_wide_copy(k):
        return [remote(k, column["y_wide"], pair_in.at[(k,) + whole + (slice(None), pl.ds(other_q, quarter))], wide_y.at[k], y_peer)]

    def view(kind, i, k):
        if i == nf - 1:
            if kind == "lean":
                return pair_in.at[(k,) + whole + (slice(None), pl.ds(0, 256))]
            return wide_y.at[k]
        box = lean if kind == "lean" else quart
        return box[i + 1].at[k, 0]

    def factor_copies(kind, i, k):
        box = lean if kind == "lean" else quart
        source = view(kind, i, k)
        out = []
        for d in range(1, factors[i]):
            peer, j = factor_peer(i, d)
            out.append(remote(k, column[kind, i] + d - 1, source.at[(slice(None),) * i + (j,)], box[i].at[k, d - 1], peer))
        return out

    def factor_sum(kind, i, k):
        box = lean if kind == "lean" else quart
        total = view(kind, i, k)[(slice(None),) * i + (coords[i],)].astype(jnp.float32)
        for d in range(1, factors[i]):
            total = total + box[i][k, d - 1].astype(jnp.float32)
        return total

    def y_lean_copy(k):
        return [remote(k, column["y_lean"], lean[0].at[k, 0], lean_y.at[k], y_peer)]

    def y_back_copy(k):
        where = (k, slice(None), pl.ds(pl.multiple_of(mine + my_q, quarter), quarter))
        return [remote(k, column["y_back"], final.at[where], final.at[where], y_peer)]

    def core_back_copy(k):
        where = (k, slice(None), pl.ds(mine, half))
        return [remote(k, column["core_back"], final.at[where], final.at[where], core_peer)]

    def begin(copies):
        for c in copies:
            c.start()

    def finish(copies):
        for c in copies:
            c.wait()

    def product(left, right_ref, cols, slot, at, part):
        width = cols[1] - cols[0]
        for c in range(0, width, 256):
            w = min(256, width - c)
            right = right_ref[:, cols[0] + c:cols[0] + c + w]
            if rows % 16 == 0:
                lhs = left[part].reshape(-1, left.shape[-1])
                got = jnp.dot(lhs, right, preferred_element_type=jnp.float32).astype(jnp.bfloat16)
                stage[(slot,) + whole + (slice(None), slice(at + c, at + c + w))] = got.reshape(factors + (rows, w))
            else:
                def one(s, carry):
                    got = jnp.dot(left[part, s], right, preferred_element_type=jnp.float32).astype(jnp.bfloat16)
                    where = tuple(coordinates(s, factors))
                    stage[(slot,) + where + (slice(None), slice(at + c, at + c + w))] = got
                    return carry
                lax.fori_loop(0, left.shape[1], one, 0)

    groups = layout["groups"]

    def compute(k):
        group, part = lax.div(k, parts), lax.rem(k, parts)
        slot = lax.rem(k, ring)
        for g, pieces in enumerate(groups):
            @pl.when(group == g)
            def _():
                at = 0
                for left, right, c0, c1 in pieces:
                    product(lefts[left], rights[right], (c0, c1), slot, at, part)
                    at += c1 - c0

    def out_copies(k, g, part):
        block, start = layout["places"][g]
        return pltpu.make_async_copy(final.at[k], outs[block].at[pl.ds(pl.multiple_of(part * rows, rows), rows), pl.ds(start, 1024)], out_sem.at[k])

    stages = [[] for _ in range(nf + 5)]

    def stage0(k):
        compute(k)
        begin(core_copy(k))

    def stage1(k):
        finish(core_copy(k))
        slot = lax.rem(k, ring)
        pair_in[k] = (pair_in[k].astype(jnp.float32) + stage[(slot,) + whole + (slice(None), pl.ds(mine, half))].astype(jnp.float32)).astype(jnp.bfloat16)
        begin(y_wide_copy(k))
        begin(factor_copies("lean", order[0], k))

    def middle(pos):
        def run(k):
            i = order[pos]
            if pos == 0:
                finish(y_wide_copy(k))
                wide_y[k] = (wide_y[k].astype(jnp.float32) + pair_in[(k,) + whole + (slice(None), pl.ds(my_q, quarter))].astype(jnp.float32)).astype(jnp.bfloat16)
            else:
                before = order[pos - 1]
                finish(factor_copies("quart", before, k))
                quart[before][k, 0] = factor_sum("quart", before, k).astype(jnp.bfloat16)
            begin(factor_copies("quart", i, k))
            finish(factor_copies("lean", i, k))
            lean[i][k, 0] = factor_sum("lean", i, k).astype(jnp.bfloat16)
            if pos + 1 < nf:
                begin(factor_copies("lean", order[pos + 1], k))
            else:
                begin(y_lean_copy(k))
        return run

    def settle(k):
        finish(factor_copies("quart", 0, k))
        final[k, :, pl.ds(pl.multiple_of(mine + my_q, quarter), quarter)] = factor_sum("quart", 0, k).astype(jnp.bfloat16)
        begin(y_back_copy(k))
        finish(y_lean_copy(k))
        final[k, :, pl.ds(mine, 256)] = (lean[0][k, 0].astype(jnp.float32) + lean_y[k].astype(jnp.float32)).astype(jnp.bfloat16)

    def give(k):
        finish(y_back_copy(k))
        begin(core_back_copy(k))

    def leave(k):
        finish(core_back_copy(k))
        group, part = lax.div(k, parts), lax.rem(k, parts)
        for g in range(len(groups)):
            pl.when(group == g)(lambda g=g: out_copies(k, g, part).start())

    stages = [stage0, stage1] + [middle(p) for p in range(nf)] + [settle, give, leave]
    lags = layout["lags"]

    small_stages = [("core", 2, core, lambda d: core_peer), ("y", 2, y, lambda d: y_peer)]
    for i in order:
        small_stages.append((i, factors[i], coords[i], lambda d, i=i: factor_peer(i, d)[0]))
    small_base = []
    count = 0
    for s in small_stages:
        small_base.append(count)
        count += s[1] - 1

    def small_copies(j):
        _, f, own, peer = small_stages[j]
        return [pltpu.make_async_remote_copy(src_ref=small[j].at[own], dst_ref=small[j].at[own],
                 send_sem=small_send.at[small_base[j] + d - 1], recv_sem=small_recv.at[small_base[j] + d - 1],
                 device_id=peer(d), device_id_type=MESH) for d in range(1, f)]

    def small_step(j):
        if j > 0:
            finish(small_copies(j - 1))
            total = small[j - 1][0]
            for a in range(1, small_stages[j - 1][1]):
                total = total + small[j - 1][a]
        else:
            total = small_in[...]
        if j < len(small_stages):
            small[j][small_stages[j][2]] = total
            begin(small_copies(j))
        else:
            small_out[...] = total

    pl.semaphore_wait(barrier, len(everyone))

    def step(t, carry):
        for lag, run in reversed(list(zip(lags, stages))):
            k = t - lag
            @pl.when((k >= 0) & (k < steps))
            def _():
                run(k)
        for j in range(len(small_stages) + 1):
            pl.when(t == j + 1)(functools.partial(small_step, j))
        return carry
    lax.fori_loop(0, steps + lags[-1], step, 0)

    def drain(k, carry):
        group, part = lax.div(k, parts), lax.rem(k, parts)
        for g in range(len(groups)):
            pl.when(group == g)(lambda g=g: out_copies(k, g, part).wait())
        return carry
    lax.fori_loop(0, steps, drain, 0)


def scatter_gradients(lefts, rights, small, layout, shard_count, lags=None):
    factors = shard_factors(shard_count)
    nf = len(factors)
    tokens, model = lefts[0].shape
    rows_all = model // shard_count
    parts = 3 if rows_all % 48 == 0 else 1
    rows = rows_all // parts
    blocks = len(rights)
    steps = len(layout["groups"]) * parts
    layout = dict(layout)
    layout["lags"] = lags or ([0, 1] + [1 + 2 * (p + 1) for p in range(nf + 1)] + [1 + 2 * (nf + 1) + 1, 1 + 2 * (nf + 1) + 2])
    ring = layout["lags"][-1] + 1 if layout["lags"][-1] < 4 else 4
    layout["lefts"] = lefts
    turned = [v.T.reshape(shard_count, parts, rows, tokens).transpose(1, 0, 2, 3) for v in lefts]
    bf = jnp.bfloat16
    lean = [pltpu.VMEM((steps, factors[i] - 1) + factors[:i] + (rows, 256), bf) for i in range(nf)]
    quart = [pltpu.VMEM((steps, factors[i] - 1) + factors[:i] + (rows, 128), bf) for i in range(nf)]
    order = list(range(nf - 1, -1, -1))
    smalls = [pltpu.VMEM((f,) + small.shape, jnp.float32) for f in [2, 2] + [factors[i] for i in order]]
    ncol = 5 + 2 * sum(f - 1 for f in factors)
    nsmall = 2 + sum(f - 1 for f in factors)
    vm = pl.BlockSpec(memory_space=pltpu.VMEM)
    layout["lefts"] = list(range(len(lefts)))
    outs = pl.pallas_call(
        functools.partial(scatter_kernel, factors, parts, blocks, layout),
        out_shape=[jax.ShapeDtypeStruct((rows_all, rights[0].shape[1]), bf)] * blocks + [jax.ShapeDtypeStruct(small.shape, jnp.float32)],
        in_specs=[vm] * (len(lefts) + blocks + 1),
        out_specs=[pl.BlockSpec(memory_space=pl.ANY)] * blocks + [vm],
        scratch_shapes=[
            pltpu.VMEM((ring,) + factors + (rows, 1024), bf),
            pltpu.VMEM((steps,) + factors + (rows, 512), bf),
            pltpu.VMEM((steps,) + factors + (rows, 128), bf),
            pltpu.VMEM((steps, rows, 1024), bf),
        ] + lean + quart + [pltpu.VMEM((steps, rows, 256), bf)] + smalls + [
            pltpu.SemaphoreType.DMA((ring, ncol)),
            pltpu.SemaphoreType.DMA((steps, ncol)),
            pltpu.SemaphoreType.DMA((steps,)),
            pltpu.SemaphoreType.DMA((nsmall,)),
            pltpu.SemaphoreType.DMA((nsmall,)),
        ],
        compiler_params=pltpu.CompilerParams(collective_id=1, has_side_effects=True, vmem_limit_bytes=62 << 20),
        name="scatter_gradients",
    )(*turned, *rights, small)
    return outs[:blocks], outs[blocks]


def gradient_layout(cut):
    groups = [[(2, 1, c, c + 1024)] for c in (0, 1024, 2048)]
    groups += [[(2, 2, c, c + 1024)] for c in (0, 1024, 2048)]
    groups += [[(3, 3, c, c + 1024)] for c in (0, 1024, 2048)]
    for c in (0, 1024, 2048):
        if c + 1024 <= cut:
            groups.append([(0, 0, c, c + 1024)])
        elif c >= cut:
            groups.append([(1, 0, c, c + 1024)])
        else:
            groups.append([(0, 0, c, cut), (1, 0, cut, c + 1024)])
    places = [(b, c) for b in (1, 2, 3, 0) for c in (0, 1024, 2048)]
    return {"groups": groups, "places": places}

def total_kernel(factors, in_ref, out_ref, *scratch):
    nf = len(factors)
    slots = scratch[:nf]
    send_sem, recv_sem = scratch[nf:]
    rep, shard = lax.axis_index("rep"), lax.axis_index("shard")
    coords = coordinates(shard, factors)

    def peers(i):
        out = []
        for d in range(1, factors[i]):
            moved = list(coords)
            moved[i] = lax.rem(coords[i] + d, factors[i])
            out.append((rep, index_of(moved, factors)))
        return out

    everyone = [p for i in range(nf) for p in peers(i)]
    barrier = pltpu.get_barrier_semaphore()
    for p in everyone:
        pl.semaphore_signal(barrier, inc=1, device_id=p, device_id_type=MESH)
    pl.semaphore_wait(barrier, len(everyone))
    total = in_ref[...]
    base = 0
    for i in range(nf):
        slots[i][coords[i]] = total
        copies = []
        for j, p in enumerate(peers(i)):
            where = slots[i].at[coords[i]]
            copies.append(pltpu.make_async_remote_copy(
                src_ref=where, dst_ref=where, send_sem=send_sem.at[base + j],
                recv_sem=recv_sem.at[base + j], device_id=p, device_id_type=MESH))
        base += len(copies)
        for c in copies:
            c.start()
        for c in copies:
            c.wait()
        total = slots[i][0]
        for a in range(1, factors[i]):
            total = total + slots[i][a]
    out_ref[...] = total


def total_over_shards(values, shard_count):
    factors = shard_factors(shard_count)
    links = sum(f - 1 for f in factors)
    vm = pl.BlockSpec(memory_space=pltpu.VMEM)
    return pl.pallas_call(
        functools.partial(total_kernel, factors),
        out_shape=jax.ShapeDtypeStruct(values.shape, jnp.float32),
        in_specs=[vm],
        out_specs=vm,
        scratch_shapes=[pltpu.VMEM((f,) + values.shape, jnp.float32) for f in factors]
        + [pltpu.SemaphoreType.DMA((links,)), pltpu.SemaphoreType.DMA((links,))],
        compiler_params=pltpu.CompilerParams(collective_id=2, has_side_effects=True),
        name="total_over_shards",
    )(values)


def tree_layout(segment_row, parent_row):
    segment_count = parent_row.shape[0]
    labels = jnp.arange(segment_count, dtype=jnp.int32)
    parent_hot = (parent_row[:, None] == labels[None, :]).astype(jnp.int32)
    identity = (labels[:, None] == labels[None, :]).astype(jnp.int32)

    def climb(counter, ancestry):
        return jnp.minimum(identity + jnp.dot(parent_hot, ancestry), 1)

    ancestry = lax.fori_loop(0, segment_count, climb, identity)
    segment_hot = (segment_row[:, None] == labels[None, :]).astype(jnp.int32)
    lengths = jnp.sum(segment_hot, axis=0, dtype=jnp.int32)
    depth_sum = jnp.dot(ancestry - identity, lengths)
    token_index = jnp.arange(segment_row.shape[0], dtype=jnp.int32)
    earlier = jnp.sum(
        (segment_row[None, :] < segment_row[:, None]).astype(jnp.int32), axis=1, dtype=jnp.int32
    )
    positions = token_index - earlier + jnp.dot(segment_hot, depth_sum)
    reach_count = jnp.dot(jnp.dot(segment_hot, ancestry), segment_hot.T)
    visible = (reach_count > 0) & (token_index[None, :] <= token_index[:, None])
    return (positions, visible)


def rope_tables(positions, head_size):
    half_size = head_size // 2
    exponent = jnp.arange(half_size, dtype=jnp.float32) * (-2.0 / head_size)
    frequency = jnp.power(ROPE_BASE, exponent)
    angles = positions.astype(jnp.float32)[:, None] * frequency[None, :]
    angles = jnp.concatenate([angles, angles], axis=1)
    return (jnp.cos(angles), jnp.sin(angles))


def rotate(states, cosine_table, sine_table):
    half_size = states.shape[-1] // 2
    turned = jnp.concatenate([-states[..., half_size:], states[..., :half_size]], axis=-1)
    return states * cosine_table[:, None, :] + turned * sine_table[:, None, :]


def unrotate(gradient, cosine_table, sine_table):
    half_size = gradient.shape[-1] // 2
    scaled = gradient * sine_table[:, None, :]
    turned = jnp.concatenate([scaled[..., half_size:], -scaled[..., :half_size]], axis=-1)
    return gradient * cosine_table[:, None, :] + turned


def dense(left_side, right_side):
    return jnp.dot(left_side, right_side, preferred_element_type=jnp.float32)


def dense_back(left_side, right_side):
    return lax.dot_general(
        left_side, right_side, (((1,), (1,)), ((), ())), preferred_element_type=jnp.float32
    )


def dense_rows(left_side, right_side):
    return lax.dot_general(
        left_side, right_side, (((0,), (0,)), ((), ())), preferred_element_type=jnp.float32
    )


def normalize(inputs):
    inverse_root = lax.rsqrt(jnp.mean(inputs * inputs, axis=-1, keepdims=True) + NORM_EPS)
    return (inputs * inverse_root, inverse_root)


def norm_backward(upstream, unit_rows, inverse_root, gain_vector):
    scaled = upstream * gain_vector
    return inverse_root * (
        scaled - unit_rows * jnp.mean(scaled * unit_rows, axis=-1, keepdims=True)
    )


def attention_scores(query_turned, key_turned, visible):
    scores = ATTENTION_SCALE * jnp.einsum(
        "tkgd,ukd->kgtu", query_turned, key_turned, preferred_element_type=jnp.float32
    )
    return jnp.where(visible[None, None], scores, MASK_FILL)


def adam_direction(weight, gradient, moment, variance):
    next_moment = BETA_FIRST * moment + (1.0 - BETA_FIRST) * gradient
    next_variance = BETA_SECOND * variance + (1.0 - BETA_SECOND) * gradient * gradient
    direction = next_moment / (jnp.sqrt(next_variance) + ADAM_EPS) + DECAY_RATE * weight
    return (next_moment, next_variance, direction)


def on_device(
    shard_count,
    tokens_in,
    cotangent,
    segment_ids,
    parent_ids,
    weight_query,
    weight_key,
    weight_value,
    weight_output,
    weight_gate,
    weight_up,
    weight_down,
    norm_attention,
    norm_feedforward,
    moment_query,
    moment_key,
    moment_value,
    moment_output,
    moment_gate,
    moment_up,
    moment_down,
    variance_query,
    variance_key,
    variance_value,
    variance_output,
    variance_gate,
    variance_up,
    variance_down,
    moment_norm_attention,
    moment_norm_feedforward,
    variance_norm_attention,
    variance_norm_feedforward,
):
    token_count = tokens_in.shape[0]
    query_width = weight_query.shape[1]
    kv_width = weight_key.shape[1]
    hidden_width = weight_gate.shape[1]
    per_group = HEADS // KV_HEADS
    positions, visible = tree_layout(segment_ids[0], parent_ids[0])
    cosine_table, sine_table = rope_tables(positions, HEAD_DIM)
    inputs = tokens_in.astype(jnp.float32)
    unit_one, inverse_one = normalize(inputs)
    normed_one = (unit_one * norm_attention).astype(jnp.bfloat16)
    second_cut = query_width + kv_width
    third_cut = query_width + 2 * kv_width
    attention_rows = jnp.concatenate([weight_query, weight_key, weight_value, weight_output], axis=1)
    full_attention, full_gate, full_up, full_down = gather_weights(
        [attention_rows, weight_gate, weight_up, weight_down], shard_count
    )
    full_input, full_output = full_attention[:, :third_cut], full_attention[:, third_cut:]
    input_states = dense(normed_one, full_input)
    query_states = input_states[:, :query_width]
    key_states = input_states[:, query_width:second_cut]
    value_states = input_states[:, second_cut:]
    query_turned = rotate(
        query_states.reshape(token_count, HEADS, HEAD_DIM), cosine_table, sine_table
    ).astype(jnp.bfloat16)
    query_turned = query_turned.reshape(token_count, KV_HEADS, per_group, HEAD_DIM)
    key_turned = rotate(
        key_states.reshape(token_count, KV_HEADS, HEAD_DIM), cosine_table, sine_table
    ).astype(jnp.bfloat16)
    value_heads = value_states.astype(jnp.bfloat16).reshape(token_count, KV_HEADS, HEAD_DIM)
    scores = attention_scores(query_turned, key_turned, visible)
    row_max = jnp.max(scores, axis=-1, keepdims=True)
    log_total = row_max + jnp.log(jnp.sum(jnp.exp(scores - row_max), axis=-1, keepdims=True))
    softmax_low = jnp.exp(scores - log_total).astype(jnp.bfloat16)
    mixed_low = jnp.einsum(
        "kgtu,ukd->tkgd", softmax_low, value_heads, preferred_element_type=jnp.float32
    )
    mixed_low = mixed_low.reshape(token_count, query_width).astype(jnp.bfloat16)
    attention_branch = dense_back(mixed_low, full_output)
    hidden_state = inputs + RESIDUAL_SCALE * attention_branch
    unit_two, inverse_two = normalize(hidden_state)
    normed_two = (unit_two * norm_feedforward).astype(jnp.bfloat16)
    gate_states = dense(normed_two, full_gate)
    up_states = dense(normed_two, full_up)
    sigmoid_gate = jax.nn.sigmoid(gate_states)
    swish = gate_states * sigmoid_gate
    activated_low = (swish * up_states).astype(jnp.bfloat16)
    feed_branch = dense_back(activated_low, full_down)
    layer_out = (hidden_state + RESIDUAL_SCALE * feed_branch).astype(jnp.bfloat16)
    upstream = cotangent.astype(jnp.float32)
    down_grad = (RESIDUAL_SCALE * upstream).astype(jnp.bfloat16)
    activation_grad = dense(down_grad, full_down)
    slope = sigmoid_gate * (1.0 + gate_states * (1.0 - sigmoid_gate))
    gate_grad = (activation_grad * up_states * slope).astype(jnp.bfloat16)
    up_grad = (activation_grad * swish).astype(jnp.bfloat16)
    normed_two_grad = dense_back(gate_grad, full_gate) + dense_back(up_grad, full_up)
    gain_part_two = jnp.sum(normed_two_grad * unit_two, axis=0)
    residual_grad = upstream + norm_backward(
        normed_two_grad, unit_two, inverse_two, norm_feedforward
    )
    branch_grad = (RESIDUAL_SCALE * residual_grad).astype(jnp.bfloat16)
    mixed_grad = dense(branch_grad, full_output)
    mixed_grad_low = mixed_grad.astype(jnp.bfloat16).reshape(
        token_count, KV_HEADS, per_group, HEAD_DIM
    )
    scores = attention_scores(query_turned, key_turned, visible)
    softmax_out = jnp.exp(scores - log_total)
    softmax_low = softmax_out.astype(jnp.bfloat16)
    probability_grad = jnp.einsum(
        "tkgd,ukd->kgtu", mixed_grad_low, value_heads, preferred_element_type=jnp.float32
    )
    row_inner = jnp.sum(softmax_out * probability_grad, axis=-1, keepdims=True)
    score_grad = (softmax_out * (probability_grad - row_inner)).astype(jnp.bfloat16)
    value_grad = jnp.einsum(
        "kgtu,tkgd->ukd", softmax_low, mixed_grad_low, preferred_element_type=jnp.float32
    )
    query_turn_grad = ATTENTION_SCALE * jnp.einsum(
        "kgtu,ukd->tkgd", score_grad, key_turned, preferred_element_type=jnp.float32
    )
    key_turn_grad = ATTENTION_SCALE * jnp.einsum(
        "kgtu,tkgd->ukd", score_grad, query_turned, preferred_element_type=jnp.float32
    )
    query_grad = unrotate(
        query_turn_grad.reshape(token_count, HEADS, HEAD_DIM), cosine_table, sine_table
    ).reshape(token_count, query_width)
    key_grad = unrotate(key_turn_grad, cosine_table, sine_table).reshape(token_count, kv_width)
    projection_grad = jnp.concatenate(
        [query_grad, key_grad, value_grad.reshape(token_count, kv_width)], axis=1
    ).astype(jnp.bfloat16)
    normed_one_grad = dense_back(projection_grad, full_input)
    gain_part_one = jnp.sum(normed_one_grad * unit_one, axis=0)
    tokens_grad = (
        residual_grad + norm_backward(normed_one_grad, unit_one, inverse_one, norm_attention)
    ).astype(jnp.bfloat16)
    weight_list = [
        weight_query,
        weight_key,
        weight_value,
        weight_output,
        weight_gate,
        weight_up,
        weight_down,
    ]
    moment_list = [
        moment_query,
        moment_key,
        moment_value,
        moment_output,
        moment_gate,
        moment_up,
        moment_down,
    ]
    variance_list = [
        variance_query,
        variance_key,
        variance_value,
        variance_output,
        variance_gate,
        variance_up,
        variance_down,
    ]
    weights_wide = [weight.astype(jnp.float32) for weight in weight_list]
    weight_sums = jnp.stack([jnp.sum(weight * weight) for weight in weights_wide])
    small = jnp.concatenate(
        [gain_part_one, gain_part_two, weight_sums, jnp.zeros(6 * 128 - 7, jnp.float32)]
    ).reshape(-1, 128)
    attention_right = jnp.concatenate([projection_grad, mixed_low], axis=1)
    blocks, small_total = scatter_gradients(
        [normed_one, branch_grad, normed_two, down_grad],
        [attention_right, gate_grad, up_grad, activated_low],
        small,
        gradient_layout(third_cut),
        shard_count,
    )
    model_width = tokens_in.shape[1]
    small_total = small_total.reshape(-1)
    gain_grad_one = small_total[:model_width]
    gain_grad_two = small_total[model_width : 2 * model_width]
    weight_total = small_total[2 * model_width : 2 * model_width + 7] * 0.25
    gradient_list = [
        part.astype(jnp.float32)
        for part in (
            blocks[0][:, :query_width],
            blocks[0][:, query_width:second_cut],
            blocks[0][:, second_cut:third_cut],
            blocks[0][:, third_cut:],
            blocks[1],
            blocks[2],
            blocks[3],
        )
    ]
    outcomes = [
        adam_direction(weight, gradient, moment, variance)
        for weight, gradient, moment, variance in zip(
            weights_wide, gradient_list, moment_list, variance_list
        )
    ]
    step_sums = jnp.stack([jnp.sum(entry[2] * entry[2]) for entry in outcomes])
    step_row = jnp.concatenate([step_sums, jnp.zeros(8 * 128 - 7, jnp.float32)]).reshape(8, 128)
    step_total = total_over_shards(step_row, shard_count)[0, :7]
    updates = []
    for matrix_index in range(7):
        factor = jnp.sqrt(weight_total[matrix_index]) * lax.rsqrt(
            step_total[matrix_index] + TRUST_EPS
        )
        updates.append(-STEP_RATE * factor * outcomes[matrix_index][2])
    gain_outcomes = [
        adam_direction(
            norm_attention, gain_grad_one, moment_norm_attention, variance_norm_attention
        ),
        adam_direction(
            norm_feedforward, gain_grad_two, moment_norm_feedforward, variance_norm_feedforward
        ),
    ]
    gain_weights = [norm_attention, norm_feedforward]
    gain_updates = []
    gain_pairs = []
    for gain_vector, entry in zip(gain_weights, gain_outcomes):
        gain_sum = jnp.sum(gain_vector * gain_vector)
        gain_step = jnp.sum(entry[2] * entry[2])
        gain_updates.append(
            -STEP_RATE * jnp.sqrt(gain_sum) * lax.rsqrt(gain_step + TRUST_EPS) * entry[2]
        )
        gain_pairs.append(jnp.stack([jnp.sqrt(gain_sum), jnp.sqrt(gain_step)]))
    matrix_pairs = jnp.stack([jnp.sqrt(weight_total), jnp.sqrt(step_total)], axis=1)
    norm_pairs = jnp.concatenate([matrix_pairs, jnp.stack(gain_pairs)], axis=0)
    return (
        layer_out,
        tokens_grad,
        updates[0],
        updates[1],
        updates[2],
        updates[3],
        updates[4],
        updates[5],
        updates[6],
        outcomes[0][0],
        outcomes[1][0],
        outcomes[2][0],
        outcomes[3][0],
        outcomes[4][0],
        outcomes[5][0],
        outcomes[6][0],
        outcomes[0][1],
        outcomes[1][1],
        outcomes[2][1],
        outcomes[3][1],
        outcomes[4][1],
        outcomes[5][1],
        outcomes[6][1],
        gain_updates[0],
        gain_updates[1],
        gain_outcomes[0][0],
        gain_outcomes[1][0],
        gain_outcomes[0][1],
        gain_outcomes[1][1],
        norm_pairs,
    )


def solution(mesh):
    in_specs = (
        P(("rep", "shard"), None),
        P(("rep", "shard"), None),
        P(("rep", "shard"), None),
        P(("rep", "shard"), None),
        P("shard", None),
        P("shard", None),
        P("shard", None),
        P("shard", None),
        P("shard", None),
        P("shard", None),
        P("shard", None),
        P(),
        P(),
        P("shard", None),
        P("shard", None),
        P("shard", None),
        P("shard", None),
        P("shard", None),
        P("shard", None),
        P("shard", None),
        P("shard", None),
        P("shard", None),
        P("shard", None),
        P("shard", None),
        P("shard", None),
        P("shard", None),
        P("shard", None),
        P(),
        P(),
        P(),
        P(),
    )
    out_specs = (
        P(("rep", "shard"), None),
        P(("rep", "shard"), None),
        P("shard", None),
        P("shard", None),
        P("shard", None),
        P("shard", None),
        P("shard", None),
        P("shard", None),
        P("shard", None),
        P("shard", None),
        P("shard", None),
        P("shard", None),
        P("shard", None),
        P("shard", None),
        P("shard", None),
        P("shard", None),
        P("shard", None),
        P("shard", None),
        P("shard", None),
        P("shard", None),
        P("shard", None),
        P("shard", None),
        P("shard", None),
        P(),
        P(),
        P(),
        P(),
        P(),
        P(),
        P(),
    )
    return jax.shard_map(
        functools.partial(on_device, mesh.shape["shard"]), mesh=mesh, in_specs=in_specs, out_specs=out_specs, check_vma=False
    )
```

```python
import functools

import jax
import jax.numpy as jnp
from jax import lax
from jax.experimental import pallas as pl
from jax.experimental.pallas import tpu as pltpu
from jax.sharding import PartitionSpec as P

MESH = pl.DeviceIdType.MESH

HEADS = 18
KV_HEADS = 6
HEAD_DIM = 64


ROPE_BASE = 10000.0
ATTENTION_SCALE = 0.125
RESIDUAL_SCALE = 1.0
NORM_EPS = 1e-05
BETA_FIRST = 0.9
BETA_SECOND = 0.999
ADAM_EPS = 1e-06
DECAY_RATE = 0.01
STEP_RATE = 0.25
TRUST_EPS = 1e-06
MASK_FILL = -1e30


def shard_factors(count):
    factors = []
    while count > 4:
        factors.append(4)
        count //= 4
    factors.append(count)
    return tuple(factors)

def coordinates(index, factors):
    out = []
    for factor in reversed(factors):
        out.append(lax.rem(index, factor))
        index = lax.div(index, factor)
    return out[::-1]

def index_of(coords, factors):
    index = 0
    for c, f in zip(coords, factors):
        index = index * f + c
    return index

def gather_chunks(width, blocks):
    out = []
    for b in range(blocks):
        wide, narrow = [], []
        start = 0
        n = width // 512
        kinds = [True, False, True, True, False, True][:n]
        for i in range(n):
            out.append((b, i * 512, 512, kinds[i % 6]))
    return out

def gather_kernel(factors, blocks, *refs):
    srcs, outs = refs[:blocks], refs[blocks:2*blocks]
    local_sem, send_sem, recv_sem = refs[2*blocks:]
    rep, shard = lax.axis_index("rep"), lax.axis_index("shard")
    y, core = lax.div(rep, 2), lax.rem(rep, 2)
    coords = coordinates(shard, factors)
    peers = []
    for i, f in enumerate(factors):
        ids = []
        for d in range(1, f):
            moved = list(coords); moved[i] = lax.rem(coords[i] + d, f)
            ids.append((rep, index_of(moved, factors)))
        peers.append(ids)
    peers.append([((1 - y) * 2 + core, shard)])
    peers.append([(y * 2 + 1 - core, shard)])
    flat = [p for ids in peers for p in ids]
    barrier = pltpu.get_barrier_semaphore()
    for p in flat:
        pl.semaphore_signal(barrier, inc=1, device_id=p, device_id_type=MESH)
    chunks = gather_chunks(srcs[0].shape[1], blocks)
    nph = len(factors) + 2
    base = []
    total = 0
    for ids in peers:
        base.append(total); total += len(ids)
    def columns(k):
        b, c0, w, split = chunks[k]
        if split:
            q = w // 4
            return c0 + (core * 2 + y) * q, q
        return c0 + core * (w // 2), w // 2
    locals_ = []
    for k, (b, c0, w, split) in enumerate(chunks):
        off, width = columns(k)
        cols = pl.ds(pl.multiple_of(off, 128), width)
        cp = pltpu.make_async_copy(srcs[b].at[:, cols], outs[b].at[tuple(coords) + (slice(None), cols)], local_sem.at[k])
        cp.start(); locals_.append(cp)
    pl.semaphore_wait(barrier, len(flat))
    def copies(k, ph):
        b, c0, w, split = chunks[k]
        off, width = columns(k)
        nf = len(factors)
        if ph < nf:
            lead = (slice(None),) * ph + tuple(coords[ph:])
        else:
            lead = (slice(None),) * nf
            if ph == nf + 1:
                off, width = c0 + core * (w // 2), w // 2
        cols = pl.ds(pl.multiple_of(off, 128), width)
        where = lead + (slice(None), cols)
        src = srcs[b].at[:, cols] if ph == 0 else outs[b].at[where]
        return [pltpu.make_async_remote_copy(src_ref=src, dst_ref=outs[b].at[where],
                  send_sem=send_sem.at[k, base[ph] + j], recv_sem=recv_sem.at[k, base[ph] + j], device_id=p, device_id_type=MESH)
                for j, p in enumerate(peers[ph])]
    n = len(chunks)
    started = {}
    def start(k, ph):
        cs = copies(k, ph)
        for c in cs: c.start()
        started[k, ph] = cs
    def phases(k):
        return [p for p in range(nph) if p != nph - 2 or chunks[k][3]]
    ahead = 4
    for k in range(min(ahead, n)):
        start(k, 0)
    for t in range(n + 2 * nph):
        for lag in range(nph - 1, -1, -1):
            k = t - 2 * lag
            if 0 <= k < n:
                ps = phases(k)
                if lag < len(ps):
                    for c in started[k, ps[lag]]: c.wait_recv()
                    if lag == 0:
                        locals_[k].wait()
                        if k + ahead < n:
                            start(k + ahead, 0)
                    if lag + 1 < len(ps): start(k, ps[lag + 1])
    for cs in started.values():
        for c in cs: c.wait_send()

def gather_weights(shards, shard_count, rep_count=4):
    blocks = len(shards)
    factors = shard_factors(shard_count)
    rows, width = shards[0].shape
    n = len(gather_chunks(width, blocks))
    total = sum(f - 1 for f in factors) + 2
    outs = pl.pallas_call(
        functools.partial(gather_kernel, factors, blocks),
        out_shape=[jax.ShapeDtypeStruct(factors + (rows, width), jnp.bfloat16)] * blocks,
        in_specs=[pl.BlockSpec(memory_space=pltpu.VMEM)] * blocks,
        out_specs=[pl.BlockSpec(memory_space=pl.ANY)] * blocks,
        scratch_shapes=[pltpu.SemaphoreType.DMA((n,)), pltpu.SemaphoreType.DMA((n, total)), pltpu.SemaphoreType.DMA((n, total))],
        compiler_params=pltpu.CompilerParams(collective_id=0, has_side_effects=True),
        name="gather_weights",
    )(*shards)
    return [o.reshape(shard_count * rows, width) for o in outs]


def scatter_kernel(factors, parts, blocks, layout, *refs):
    nf = len(factors)
    nl = len(layout["lefts"])
    lefts = refs[:nl]
    rights = refs[nl:nl + blocks]
    small_in = refs[nl + blocks]
    at = nl + blocks + 1
    params = layout["params"]
    weights = refs[at:at + blocks]
    moments = refs[at + blocks:at + blocks + params]
    variances = refs[at + blocks + params:at + blocks + 2 * params]
    at += blocks + 2 * params
    outs = refs[at:at + blocks]
    small_out, norm_out = refs[at + blocks:at + blocks + 2]
    scratch = list(refs[at + blocks + 2:])
    stage, pair_in, wide_y, final = scratch[:4]
    lean = scratch[4:4 + nf]
    quart = scratch[4 + nf:4 + 2 * nf]
    lean_y = scratch[4 + 2 * nf]
    small = scratch[5 + 2 * nf:5 + 2 * nf + nf + 2]
    rest = scratch[5 + 2 * nf + nf + 2:]
    norm_slots = rest[:nf]
    held_m, held_v, held_w, step_acc, weight_acc = rest[nf:nf + 5]
    send_sem, recv_sem, out_sem, small_send, small_recv, fetch_sem, norm_send, norm_recv = rest[nf + 5:]
    rows = final.shape[1]
    steps = final.shape[0]
    ring = stage.shape[0]
    rep, shard = lax.axis_index("rep"), lax.axis_index("shard")
    y, core = lax.div(rep, 2), lax.rem(rep, 2)
    coords = coordinates(shard, factors)
    y_peer = ((1 - y) * 2 + core, shard)
    core_peer = (y * 2 + 1 - core, shard)

    def factor_peer(i, d):
        moved = list(coords)
        moved[i] = lax.rem(coords[i] + d, factors[i])
        return (rep, index_of(moved, factors)), moved[i]

    everyone = [y_peer, core_peer]
    for i, f in enumerate(factors):
        everyone += [factor_peer(i, d)[0] for d in range(1, f)]
    barrier = pltpu.get_barrier_semaphore()
    for p in everyone:
        pl.semaphore_signal(barrier, inc=1, device_id=p, device_id_type=MESH)

    order = list(range(nf - 1, -1, -1))
    column = {"core": 0, "y_wide": 1, "y_lean": 2, "y_back": 3, "core_back": 4}
    used = 5
    for i in order:
        column["lean", i] = used
        used += factors[i] - 1
        column["quart", i] = used
        used += factors[i] - 1

    def remote(k, c, src, dst, peer):
        return pltpu.make_async_remote_copy(
            src_ref=src, dst_ref=dst, send_sem=send_sem.at[lax.rem(k, ring), c],
            recv_sem=recv_sem.at[k, c], device_id=peer, device_id_type=MESH)

    half, quarter = 512, 128
    mine = pl.multiple_of(core * half, half)
    other = pl.multiple_of((1 - core) * half, half)
    my_q = pl.multiple_of(256 + y * quarter, quarter)
    other_q = pl.multiple_of(256 + (1 - y) * quarter, quarter)
    whole = (slice(None),) * nf

    def core_copy(k):
        slot = lax.rem(k, ring)
        return [remote(k, column["core"], stage.at[(slot,) + whole + (slice(None), pl.ds(other, half))], pair_in.at[k], core_peer)]

    def y_wide_copy(k):
        return [remote(k, column["y_wide"], pair_in.at[(k,) + whole + (slice(None), pl.ds(other_q, quarter))], wide_y.at[k], y_peer)]

    def view(kind, i, k):
        if i == nf - 1:
            if kind == "lean":
                return pair_in.at[(k,) + whole + (slice(None), pl.ds(0, 256))]
            return wide_y.at[k]
        box = lean if kind == "lean" else quart
        return box[i + 1].at[k, 0]

    def factor_copies(kind, i, k):
        box = lean if kind == "lean" else quart
        source = view(kind, i, k)
        out = []
        for d in range(1, factors[i]):
            peer, j = factor_peer(i, d)
            out.append(remote(k, column[kind, i] + d - 1, source.at[(slice(None),) * i + (j,)], box[i].at[k, d - 1], peer))
        return out

    def factor_sum(kind, i, k):
        box = lean if kind == "lean" else quart
        total = view(kind, i, k)[(slice(None),) * i + (coords[i],)].astype(jnp.float32)
        for d in range(1, factors[i]):
            total = total + box[i][k, d - 1].astype(jnp.float32)
        return total

    def y_lean_copy(k):
        return [remote(k, column["y_lean"], lean[0].at[k, 0], lean_y.at[k], y_peer)]

    def y_back_copy(k):
        where = (k, slice(None), pl.ds(pl.multiple_of(mine + my_q, quarter), quarter))
        return [remote(k, column["y_back"], final.at[where], final.at[where], y_peer)]

    def core_back_copy(k):
        where = (k, slice(None), pl.ds(mine, half))
        return [remote(k, column["core_back"], final.at[where], final.at[where], core_peer)]

    def begin(copies):
        for c in copies:
            c.start()

    def finish(copies):
        for c in copies:
            c.wait()

    def product(left, right_ref, cols, slot, at, part):
        width = cols[1] - cols[0]
        for c in range(0, width, 256):
            w = min(256, width - c)
            right = right_ref[:, cols[0] + c:cols[0] + c + w]
            if rows % 16 == 0:
                lhs = left[part].reshape(-1, left.shape[-1])
                got = jnp.dot(lhs, right, preferred_element_type=jnp.float32).astype(jnp.bfloat16)
                stage[(slot,) + whole + (slice(None), slice(at + c, at + c + w))] = got.reshape(factors + (rows, w))
            else:
                def one(s, carry):
                    got = jnp.dot(left[part, s], right, preferred_element_type=jnp.float32).astype(jnp.bfloat16)
                    where = tuple(coordinates(s, factors))
                    stage[(slot,) + where + (slice(None), slice(at + c, at + c + w))] = got
                    return carry
                lax.fori_loop(0, left.shape[1], one, 0)

    groups = layout["groups"]

    def compute(k):
        group, part = lax.div(k, parts), lax.rem(k, parts)
        slot = lax.rem(k, ring)
        for g, pieces in enumerate(groups):
            @pl.when(group == g)
            def _():
                at = 0
                for left, right, c0, c1 in pieces:
                    product(lefts[left], rights[right], (c0, c1), slot, at, part)
                    at += c1 - c0

    def out_copies(k, g, part):
        block, start = layout["places"][g]
        return pltpu.make_async_copy(final.at[k], outs[block].at[pl.ds(pl.multiple_of(part * rows, rows), rows), pl.ds(start, 1024)], out_sem.at[k])

    stages = [[] for _ in range(nf + 5)]

    def stage0(k):
        compute(k)
        begin(core_copy(k))

    def stage1(k):
        finish(core_copy(k))
        slot = lax.rem(k, ring)
        pair_in[k] = (pair_in[k].astype(jnp.float32) + stage[(slot,) + whole + (slice(None), pl.ds(mine, half))].astype(jnp.float32)).astype(jnp.bfloat16)
        begin(y_wide_copy(k))
        begin(factor_copies("lean", order[0], k))

    def middle(pos):
        def run(k):
            i = order[pos]
            if pos == 0:
                finish(y_wide_copy(k))
                wide_y[k] = (wide_y[k].astype(jnp.float32) + pair_in[(k,) + whole + (slice(None), pl.ds(my_q, quarter))].astype(jnp.float32)).astype(jnp.bfloat16)
            else:
                before = order[pos - 1]
                finish(factor_copies("quart", before, k))
                quart[before][k, 0] = factor_sum("quart", before, k).astype(jnp.bfloat16)
            begin(factor_copies("quart", i, k))
            finish(factor_copies("lean", i, k))
            lean[i][k, 0] = factor_sum("lean", i, k).astype(jnp.bfloat16)
            if pos + 1 < nf:
                begin(factor_copies("lean", order[pos + 1], k))
            else:
                begin(y_lean_copy(k))
        return run

    def settle(k):
        finish(factor_copies("quart", 0, k))
        final[k, :, pl.ds(pl.multiple_of(mine + my_q, quarter), quarter)] = factor_sum("quart", 0, k).astype(jnp.bfloat16)
        begin(y_back_copy(k))
        finish(y_lean_copy(k))
        final[k, :, pl.ds(mine, 256)] = (lean[0][k, 0].astype(jnp.float32) + lean_y[k].astype(jnp.float32)).astype(jnp.bfloat16)

    def give(k):
        finish(y_back_copy(k))
        begin(core_back_copy(k))

    hold = held_m.shape[0]

    def fetches(k, g, part):
        slot = lax.rem(k, hold)
        down = pl.ds(pl.multiple_of(part * rows, rows), rows)
        block, start = layout["places"][g]
        found = [pltpu.make_async_copy(weights[block].at[down, pl.ds(start, 1024)], held_w.at[slot], fetch_sem.at[slot, 0])]
        c = 0
        for j, (param, first, width) in enumerate(layout["cuts"][g]):
            for box, source, column_of in ((held_m, moments, 1), (held_v, variances, 5)):
                found.append(pltpu.make_async_copy(
                    source[param].at[down, pl.ds(first, width)], box.at[slot, :, pl.ds(c, width)],
                    fetch_sem.at[slot, column_of + j]))
            c += width
        return found

    def by_group(k, action):
        group, part = lax.div(k, parts), lax.rem(k, parts)
        for g in range(len(groups)):
            pl.when(group == g)(lambda g=g: action(k, g, part))

    def fetch(k):
        by_group(k, lambda k, g, part: begin(fetches(k, g, part)))

    def leave(k):
        finish(core_back_copy(k))
        by_group(k, lambda k, g, part: out_copies(k, g, part).start())
        by_group(k, lambda k, g, part: finish(fetches(k, g, part)))
        slot, group = lax.rem(k, hold), lax.div(k, parts)
        gradient = final[k].astype(jnp.float32)
        weight = held_w[slot].astype(jnp.float32)
        direction = adam_direction(weight, gradient, held_m[slot], held_v[slot])[2]
        step_acc[group] += jnp.sum(direction * direction, axis=0, keepdims=True)
        weight_acc[group] += jnp.sum(weight * weight, axis=0, keepdims=True)

    lags = list(layout["lags"])
    stages = [stage0, stage1] + [middle(p) for p in range(nf)] + [settle, give, leave, fetch]
    lags.append(lags[-1] - 3)
    step_acc[...] = jnp.zeros_like(step_acc)
    weight_acc[...] = jnp.zeros_like(weight_acc)

    small_stages = [("core", 2, core, lambda d: core_peer), ("y", 2, y, lambda d: y_peer)]
    for i in order:
        small_stages.append((i, factors[i], coords[i], lambda d, i=i: factor_peer(i, d)[0]))
    small_base = []
    count = 0
    for s in small_stages:
        small_base.append(count)
        count += s[1] - 1

    def small_copies(j):
        _, f, own, peer = small_stages[j]
        return [pltpu.make_async_remote_copy(src_ref=small[j].at[own], dst_ref=small[j].at[own],
                 send_sem=small_send.at[small_base[j] + d - 1], recv_sem=small_recv.at[small_base[j] + d - 1],
                 device_id=peer(d), device_id_type=MESH) for d in range(1, f)]

    def small_step(j):
        if j > 0:
            finish(small_copies(j - 1))
            total = small[j - 1][0]
            for a in range(1, small_stages[j - 1][1]):
                total = total + small[j - 1][a]
        else:
            total = small_in[...]
        if j < len(small_stages):
            small[j][small_stages[j][2]] = total
            begin(small_copies(j))
        else:
            small_out[...] = total

    pl.semaphore_wait(barrier, len(everyone))

    def step(t, carry):
        for lag, run in reversed(list(zip(lags, stages))):
            k = t - lag
            @pl.when((k >= 0) & (k < steps))
            def _():
                run(k)
        for j in range(len(small_stages) + 1):
            pl.when(t == j + 1)(functools.partial(small_step, j))
        return carry
    lax.fori_loop(0, steps + max(lags), step, 0)

    lines = lax.broadcasted_iota(jnp.int32, (16, 128), 0)
    total = jnp.zeros((16, 128), jnp.float32)
    for acc, offset in ((step_acc, 0), (weight_acc, 8)):
        sums = [None] * params
        for g in range(len(groups)):
            c = 0
            for param, _, width in layout["cuts"][g]:
                value = jnp.sum(acc[g, :, c:c + width])
                sums[param] = value if sums[param] is None else sums[param] + value
                c += width
        for param in range(params):
            total = jnp.where(lines == offset + param, sums[param], total)
    done = 0
    for i in order:
        norm_slots[i][coords[i]] = total
        copies = []
        for d in range(1, factors[i]):
            where = norm_slots[i].at[coords[i]]
            copies.append(pltpu.make_async_remote_copy(
                src_ref=where, dst_ref=where, send_sem=norm_send.at[done], recv_sem=norm_recv.at[done],
                device_id=factor_peer(i, d)[0], device_id_type=MESH))
            done += 1
        begin(copies)
        finish(copies)
        total = norm_slots[i][0]
        for a in range(1, factors[i]):
            total = total + norm_slots[i][a]
    norm_out[...] = total

    def drain(k, carry):
        group, part = lax.div(k, parts), lax.rem(k, parts)
        for g in range(len(groups)):
            pl.when(group == g)(lambda g=g: out_copies(k, g, part).wait())
        return carry
    lax.fori_loop(0, steps, drain, 0)


def scatter_gradients(lefts, rights, small, weights, moments, variances, layout, shard_count, lags=None):
    factors = shard_factors(shard_count)
    nf = len(factors)
    tokens, model = lefts[0].shape
    rows_all = model // shard_count
    parts = 3 if rows_all % 48 == 0 else 1
    rows = rows_all // parts
    blocks = len(rights)
    steps = len(layout["groups"]) * parts
    layout = dict(layout)
    layout["lags"] = lags or ([0, 1] + [1 + 2 * (p + 1) for p in range(nf + 1)] + [1 + 2 * (nf + 1) + 1, 1 + 2 * (nf + 1) + 2])
    ring = layout["lags"][-1] + 1 if layout["lags"][-1] < 4 else 4
    layout["lefts"] = lefts
    turned = [v.T.reshape(shard_count, parts, rows, tokens).transpose(1, 0, 2, 3) for v in lefts]
    bf = jnp.bfloat16
    lean = [pltpu.VMEM((steps, factors[i] - 1) + factors[:i] + (rows, 256), bf) for i in range(nf)]
    quart = [pltpu.VMEM((steps, factors[i] - 1) + factors[:i] + (rows, 128), bf) for i in range(nf)]
    order = list(range(nf - 1, -1, -1))
    smalls = [pltpu.VMEM((f,) + small.shape, jnp.float32) for f in [2, 2] + [factors[i] for i in order]]
    ncol = 5 + 2 * sum(f - 1 for f in factors)
    nsmall = 2 + sum(f - 1 for f in factors)
    vm = pl.BlockSpec(memory_space=pltpu.VMEM)
    layout["lefts"] = list(range(len(lefts)))
    params = layout["params"] = len(moments)
    anywhere = pl.BlockSpec(memory_space=pl.ANY)
    hold = 5
    outs = pl.pallas_call(
        functools.partial(scatter_kernel, factors, parts, blocks, layout),
        out_shape=[jax.ShapeDtypeStruct((rows_all, rights[0].shape[1]), bf)] * blocks + [jax.ShapeDtypeStruct(small.shape, jnp.float32), jax.ShapeDtypeStruct((16, 128), jnp.float32)],
        in_specs=[vm] * (len(lefts) + blocks + 1) + [anywhere] * (blocks + 2 * params),
        out_specs=[anywhere] * blocks + [vm, vm],
        scratch_shapes=[
            pltpu.VMEM((ring,) + factors + (rows, 1024), bf),
            pltpu.VMEM((steps,) + factors + (rows, 512), bf),
            pltpu.VMEM((steps,) + factors + (rows, 128), bf),
            pltpu.VMEM((steps, rows, 1024), bf),
        ] + lean + quart + [pltpu.VMEM((steps, rows, 256), bf)] + smalls + [
            pltpu.VMEM((f, 16, 128), jnp.float32) for f in factors
        ] + [
            pltpu.VMEM((hold, rows, 1024), jnp.float32),
            pltpu.VMEM((hold, rows, 1024), jnp.float32),
            pltpu.VMEM((hold, rows, 1024), bf),
            pltpu.VMEM((len(layout["groups"]), 1, 1024), jnp.float32),
            pltpu.VMEM((len(layout["groups"]), 1, 1024), jnp.float32),
            pltpu.SemaphoreType.DMA((ring, ncol)),
            pltpu.SemaphoreType.DMA((steps, ncol)),
            pltpu.SemaphoreType.DMA((steps,)),
            pltpu.SemaphoreType.DMA((nsmall,)),
            pltpu.SemaphoreType.DMA((nsmall,)),
            pltpu.SemaphoreType.DMA((hold, 9)),
            pltpu.SemaphoreType.DMA((nsmall,)),
            pltpu.SemaphoreType.DMA((nsmall,)),
        ],
        compiler_params=pltpu.CompilerParams(collective_id=1, has_side_effects=True, vmem_limit_bytes=62 << 20),
        name="scatter_gradients",
    )(*turned, *rights, small, *weights, *moments, *variances)
    return outs[:blocks], outs[blocks], outs[blocks + 1]


def gradient_layout(widths):
    spans, start = [], 0
    for param, width in enumerate(widths[:4]):
        spans.append((param, start, start + width))
        start += width
    cut = spans[3][1]
    groups, places, cuts = [], [], []
    for block in (1, 2, 3):
        for c in range(0, widths[3 + block], 1024):
            groups.append([(3 if block == 3 else 2, block, c, c + 1024)])
            places.append((block, c))
            cuts.append([(3 + block, c, 1024)])
    for c in range(0, start, 1024):
        pieces = [(0, 0, c, min(c + 1024, cut)), (1, 0, max(c, cut), c + 1024)]
        groups.append([p for p in pieces if p[2] < p[3]])
        places.append((0, c))
        found = []
        for param, low, high in spans:
            if max(low, c) < min(high, c + 1024):
                found.append((param, max(low, c) - low, min(high, c + 1024) - max(low, c)))
        cuts.append(found)
    return {"groups": groups, "places": places, "cuts": cuts}


def tree_layout(segment_row, parent_row):
    segment_count = parent_row.shape[0]
    labels = jnp.arange(segment_count, dtype=jnp.int32)
    parent_hot = (parent_row[:, None] == labels[None, :]).astype(jnp.int32)
    identity = (labels[:, None] == labels[None, :]).astype(jnp.int32)

    ancestry = jnp.minimum(identity + parent_hot, 1)
    reach = 1
    while reach < segment_count:
        ancestry = jnp.minimum(jnp.sum(ancestry[:, :, None] * ancestry[None, :, :], axis=1), 1)
        reach *= 2
    segment_hot = (segment_row[:, None] == labels[None, :]).astype(jnp.int32)
    lengths = jnp.sum(segment_hot, axis=0, dtype=jnp.int32)
    depth_sum = jnp.dot(ancestry - identity, lengths)
    token_index = jnp.arange(segment_row.shape[0], dtype=jnp.int32)
    earlier = jnp.sum(
        (segment_row[None, :] < segment_row[:, None]).astype(jnp.int32), axis=1, dtype=jnp.int32
    )
    positions = token_index - earlier + jnp.dot(segment_hot, depth_sum)
    reach_count = jnp.dot(jnp.dot(segment_hot, ancestry), segment_hot.T)
    visible = (reach_count > 0) & (token_index[None, :] <= token_index[:, None])
    return (positions, visible)


def rope_tables(positions, head_size):
    half_size = head_size // 2
    exponent = jnp.arange(half_size, dtype=jnp.float32) * (-2.0 / head_size)
    frequency = jnp.power(ROPE_BASE, exponent)
    angles = positions.astype(jnp.float32)[:, None] * frequency[None, :]
    angles = jnp.concatenate([angles, angles], axis=1)
    return (jnp.cos(angles), jnp.sin(angles))


def rotate(states, cosine_table, sine_table):
    half_size = states.shape[-1] // 2
    turned = jnp.concatenate([-states[..., half_size:], states[..., :half_size]], axis=-1)
    return states * cosine_table[:, None, :] + turned * sine_table[:, None, :]


def unrotate(gradient, cosine_table, sine_table):
    half_size = gradient.shape[-1] // 2
    scaled = gradient * sine_table[:, None, :]
    turned = jnp.concatenate([scaled[..., half_size:], -scaled[..., :half_size]], axis=-1)
    return gradient * cosine_table[:, None, :] + turned


def dense(left_side, right_side):
    return jnp.dot(left_side, right_side, preferred_element_type=jnp.float32)


def dense_back(left_side, right_side):
    return lax.dot_general(
        left_side, right_side, (((1,), (1,)), ((), ())), preferred_element_type=jnp.float32
    )


def dense_rows(left_side, right_side):
    return lax.dot_general(
        left_side, right_side, (((0,), (0,)), ((), ())), preferred_element_type=jnp.float32
    )


def normalize(inputs):
    inverse_root = lax.rsqrt(jnp.mean(inputs * inputs, axis=-1, keepdims=True) + NORM_EPS)
    return (inputs * inverse_root, inverse_root)


def norm_backward(upstream, unit_rows, inverse_root, gain_vector):
    scaled = upstream * gain_vector
    return inverse_root * (
        scaled - unit_rows * jnp.mean(scaled * unit_rows, axis=-1, keepdims=True)
    )


def attention_scores(query_turned, key_turned, visible):
    scores = ATTENTION_SCALE * jnp.einsum(
        "tkgd,ukd->kgtu", query_turned, key_turned, preferred_element_type=jnp.float32
    )
    return jnp.where(visible[None, None], scores, MASK_FILL)


def adam_direction(weight, gradient, moment, variance):
    next_moment = BETA_FIRST * moment + (1.0 - BETA_FIRST) * gradient
    next_variance = BETA_SECOND * variance + (1.0 - BETA_SECOND) * gradient * gradient
    direction = next_moment / (jnp.sqrt(next_variance) + ADAM_EPS) + DECAY_RATE * weight
    return (next_moment, next_variance, direction)


def on_device(
    shard_count,
    tokens_in,
    cotangent,
    segment_ids,
    parent_ids,
    weight_query,
    weight_key,
    weight_value,
    weight_output,
    weight_gate,
    weight_up,
    weight_down,
    norm_attention,
    norm_feedforward,
    moment_query,
    moment_key,
    moment_value,
    moment_output,
    moment_gate,
    moment_up,
    moment_down,
    variance_query,
    variance_key,
    variance_value,
    variance_output,
    variance_gate,
    variance_up,
    variance_down,
    moment_norm_attention,
    moment_norm_feedforward,
    variance_norm_attention,
    variance_norm_feedforward,
):
    token_count = tokens_in.shape[0]
    query_width = weight_query.shape[1]
    kv_width = weight_key.shape[1]
    hidden_width = weight_gate.shape[1]
    per_group = HEADS // KV_HEADS
    positions, visible = tree_layout(segment_ids[0], parent_ids[0])
    cosine_table, sine_table = rope_tables(positions, HEAD_DIM)
    inputs = tokens_in.astype(jnp.float32)
    unit_one, inverse_one = normalize(inputs)
    normed_one = (unit_one * norm_attention).astype(jnp.bfloat16)
    second_cut = query_width + kv_width
    third_cut = query_width + 2 * kv_width
    attention_rows = jnp.concatenate([weight_query, weight_key, weight_value, weight_output], axis=1)
    full_attention, full_gate, full_up, full_down = gather_weights(
        [attention_rows, weight_gate, weight_up, weight_down], shard_count
    )
    full_input, full_output = full_attention[:, :third_cut], full_attention[:, third_cut:]
    input_states = dense(normed_one, full_input)
    query_states = input_states[:, :query_width]
    key_states = input_states[:, query_width:second_cut]
    value_states = input_states[:, second_cut:]
    query_turned = rotate(
        query_states.reshape(token_count, HEADS, HEAD_DIM), cosine_table, sine_table
    ).astype(jnp.bfloat16)
    query_turned = query_turned.reshape(token_count, KV_HEADS, per_group, HEAD_DIM)
    key_turned = rotate(
        key_states.reshape(token_count, KV_HEADS, HEAD_DIM), cosine_table, sine_table
    ).astype(jnp.bfloat16)
    value_heads = value_states.astype(jnp.bfloat16).reshape(token_count, KV_HEADS, HEAD_DIM)
    scores = attention_scores(query_turned, key_turned, visible)
    row_max = jnp.max(scores, axis=-1, keepdims=True)
    log_total = row_max + jnp.log(jnp.sum(jnp.exp(scores - row_max), axis=-1, keepdims=True))
    softmax_low = jnp.exp(scores - log_total).astype(jnp.bfloat16)
    mixed_low = jnp.einsum(
        "kgtu,ukd->tkgd", softmax_low, value_heads, preferred_element_type=jnp.float32
    )
    mixed_low = mixed_low.reshape(token_count, query_width).astype(jnp.bfloat16)
    attention_branch = dense_back(mixed_low, full_output)
    hidden_state = inputs + RESIDUAL_SCALE * attention_branch
    unit_two, inverse_two = normalize(hidden_state)
    normed_two = (unit_two * norm_feedforward).astype(jnp.bfloat16)
    gate_states = dense(normed_two, full_gate)
    up_states = dense(normed_two, full_up)
    sigmoid_gate = jax.nn.sigmoid(gate_states)
    swish = gate_states * sigmoid_gate
    activated_low = (swish * up_states).astype(jnp.bfloat16)
    feed_branch = dense_back(activated_low, full_down)
    layer_out = (hidden_state + RESIDUAL_SCALE * feed_branch).astype(jnp.bfloat16)
    upstream = cotangent.astype(jnp.float32)
    down_grad = (RESIDUAL_SCALE * upstream).astype(jnp.bfloat16)
    activation_grad = dense(down_grad, full_down)
    slope = sigmoid_gate * (1.0 + gate_states * (1.0 - sigmoid_gate))
    gate_grad = (activation_grad * up_states * slope).astype(jnp.bfloat16)
    up_grad = (activation_grad * swish).astype(jnp.bfloat16)
    normed_two_grad = dense_back(gate_grad, full_gate) + dense_back(up_grad, full_up)
    gain_part_two = jnp.sum(normed_two_grad * unit_two, axis=0)
    residual_grad = upstream + norm_backward(
        normed_two_grad, unit_two, inverse_two, norm_feedforward
    )
    branch_grad = (RESIDUAL_SCALE * residual_grad).astype(jnp.bfloat16)
    mixed_grad = dense(branch_grad, full_output)
    mixed_grad_low = mixed_grad.astype(jnp.bfloat16).reshape(
        token_count, KV_HEADS, per_group, HEAD_DIM
    )
    scores = attention_scores(query_turned, key_turned, visible)
    softmax_out = jnp.exp(scores - log_total)
    softmax_low = softmax_out.astype(jnp.bfloat16)
    probability_grad = jnp.einsum(
        "tkgd,ukd->kgtu", mixed_grad_low, value_heads, preferred_element_type=jnp.float32
    )
    row_inner = jnp.sum(softmax_out * probability_grad, axis=-1, keepdims=True)
    score_grad = (softmax_out * (probability_grad - row_inner)).astype(jnp.bfloat16)
    value_grad = jnp.einsum(
        "kgtu,tkgd->ukd", softmax_low, mixed_grad_low, preferred_element_type=jnp.float32
    )
    query_turn_grad = ATTENTION_SCALE * jnp.einsum(
        "kgtu,ukd->tkgd", score_grad, key_turned, preferred_element_type=jnp.float32
    )
    key_turn_grad = ATTENTION_SCALE * jnp.einsum(
        "kgtu,tkgd->ukd", score_grad, query_turned, preferred_element_type=jnp.float32
    )
    query_grad = unrotate(
        query_turn_grad.reshape(token_count, HEADS, HEAD_DIM), cosine_table, sine_table
    ).reshape(token_count, query_width)
    key_grad = unrotate(key_turn_grad, cosine_table, sine_table).reshape(token_count, kv_width)
    projection_grad = jnp.concatenate(
        [query_grad, key_grad, value_grad.reshape(token_count, kv_width)], axis=1
    ).astype(jnp.bfloat16)
    normed_one_grad = dense_back(projection_grad, full_input)
    gain_part_one = jnp.sum(normed_one_grad * unit_one, axis=0)
    tokens_grad = (
        residual_grad + norm_backward(normed_one_grad, unit_one, inverse_one, norm_attention)
    ).astype(jnp.bfloat16)
    weight_list = [
        weight_query,
        weight_key,
        weight_value,
        weight_output,
        weight_gate,
        weight_up,
        weight_down,
    ]
    moment_list = [
        moment_query,
        moment_key,
        moment_value,
        moment_output,
        moment_gate,
        moment_up,
        moment_down,
    ]
    variance_list = [
        variance_query,
        variance_key,
        variance_value,
        variance_output,
        variance_gate,
        variance_up,
        variance_down,
    ]
    small = jnp.concatenate([gain_part_one, gain_part_two]).reshape(-1, 128)
    attention_right = jnp.concatenate([projection_grad, mixed_low], axis=1)
    blocks, small_total, norm_squares = scatter_gradients(
        [normed_one, branch_grad, normed_two, down_grad],
        [attention_right, gate_grad, up_grad, activated_low],
        small,
        [attention_rows, weight_gate, weight_up, weight_down],
        moment_list,
        variance_list,
        gradient_layout([weight.shape[1] for weight in weight_list]),
        shard_count,
    )
    model_width = tokens_in.shape[1]
    small_total = small_total.reshape(-1)
    gain_grad_one = small_total[:model_width]
    gain_grad_two = small_total[model_width : 2 * model_width]
    step_total, weight_total = norm_squares[:7, 0], norm_squares[8:15, 0]
    weights_wide = [weight.astype(jnp.float32) for weight in weight_list]
    gradient_list = [
        part.astype(jnp.float32)
        for part in (
            blocks[0][:, :query_width],
            blocks[0][:, query_width:second_cut],
            blocks[0][:, second_cut:third_cut],
            blocks[0][:, third_cut:],
            blocks[1],
            blocks[2],
            blocks[3],
        )
    ]
    outcomes = [
        adam_direction(weight, gradient, moment, variance)
        for weight, gradient, moment, variance in zip(
            weights_wide, gradient_list, moment_list, variance_list
        )
    ]
    updates = []
    for matrix_index in range(7):
        factor = jnp.sqrt(weight_total[matrix_index]) * lax.rsqrt(
            step_total[matrix_index] + TRUST_EPS
        )
        updates.append(-STEP_RATE * factor * outcomes[matrix_index][2])
    gain_outcomes = [
        adam_direction(
            norm_attention, gain_grad_one, moment_norm_attention, variance_norm_attention
        ),
        adam_direction(
            norm_feedforward, gain_grad_two, moment_norm_feedforward, variance_norm_feedforward
        ),
    ]
    gain_weights = [norm_attention, norm_feedforward]
    gain_updates = []
    gain_pairs = []
    for gain_vector, entry in zip(gain_weights, gain_outcomes):
        gain_sum = jnp.sum(gain_vector * gain_vector)
        gain_step = jnp.sum(entry[2] * entry[2])
        gain_updates.append(
            -STEP_RATE * jnp.sqrt(gain_sum) * lax.rsqrt(gain_step + TRUST_EPS) * entry[2]
        )
        gain_pairs.append(jnp.stack([jnp.sqrt(gain_sum), jnp.sqrt(gain_step)]))
    matrix_pairs = jnp.stack([jnp.sqrt(weight_total), jnp.sqrt(step_total)], axis=1)
    norm_pairs = jnp.concatenate([matrix_pairs, jnp.stack(gain_pairs)], axis=0)
    return (
        layer_out,
        tokens_grad,
        updates[0],
        updates[1],
        updates[2],
        updates[3],
        updates[4],
        updates[5],
        updates[6],
        outcomes[0][0],
        outcomes[1][0],
        outcomes[2][0],
        outcomes[3][0],
        outcomes[4][0],
        outcomes[5][0],
        outcomes[6][0],
        outcomes[0][1],
        outcomes[1][1],
        outcomes[2][1],
        outcomes[3][1],
        outcomes[4][1],
        outcomes[5][1],
        outcomes[6][1],
        gain_updates[0],
        gain_updates[1],
        gain_outcomes[0][0],
        gain_outcomes[1][0],
        gain_outcomes[0][1],
        gain_outcomes[1][1],
        norm_pairs,
    )


def solution(mesh):
    in_specs = (
        P(("rep", "shard"), None),
        P(("rep", "shard"), None),
        P(("rep", "shard"), None),
        P(("rep", "shard"), None),
        P("shard", None),
        P("shard", None),
        P("shard", None),
        P("shard", None),
        P("shard", None),
        P("shard", None),
        P("shard", None),
        P(),
        P(),
        P("shard", None),
        P("shard", None),
        P("shard", None),
        P("shard", None),
        P("shard", None),
        P("shard", None),
        P("shard", None),
        P("shard", None),
        P("shard", None),
        P("shard", None),
        P("shard", None),
        P("shard", None),
        P("shard", None),
        P("shard", None),
        P(),
        P(),
        P(),
        P(),
    )
    out_specs = (
        P(("rep", "shard"), None),
        P(("rep", "shard"), None),
        P("shard", None),
        P("shard", None),
        P("shard", None),
        P("shard", None),
        P("shard", None),
        P("shard", None),
        P("shard", None),
        P("shard", None),
        P("shard", None),
        P("shard", None),
        P("shard", None),
        P("shard", None),
        P("shard", None),
        P("shard", None),
        P("shard", None),
        P("shard", None),
        P("shard", None),
        P("shard", None),
        P("shard", None),
        P("shard", None),
        P("shard", None),
        P(),
        P(),
        P(),
        P(),
        P(),
        P(),
        P(),
    )
    return jax.shard_map(
        functools.partial(on_device, mesh.shape["shard"]), mesh=mesh, in_specs=in_specs, out_specs=out_specs, check_vma=False
    )
```

```python
import functools

import jax
import jax.numpy as jnp
from jax import lax
from jax.experimental import pallas as pl
from jax.experimental.pallas import tpu as pltpu
from jax.sharding import PartitionSpec as P

MESH = pl.DeviceIdType.MESH

HEADS = 18
KV_HEADS = 6
HEAD_DIM = 64


ROPE_BASE = 10000.0
ATTENTION_SCALE = 0.125
RESIDUAL_SCALE = 1.0
NORM_EPS = 1e-05
BETA_FIRST = 0.9
BETA_SECOND = 0.999
ADAM_EPS = 1e-06
DECAY_RATE = 0.01
STEP_RATE = 0.25
TRUST_EPS = 1e-06
MASK_FILL = -1e30


def shard_factors(count):
    factors = []
    while count > 4:
        factors.append(4)
        count //= 4
    factors.append(count)
    return tuple(factors)

def coordinates(index, factors):
    out = []
    for factor in reversed(factors):
        out.append(lax.rem(index, factor))
        index = lax.div(index, factor)
    return out[::-1]

def index_of(coords, factors):
    index = 0
    for c, f in zip(coords, factors):
        index = index * f + c
    return index

def gather_chunks(width, blocks):
    out = []
    for b in range(blocks):
        wide, narrow = [], []
        start = 0
        n = width // 512
        kinds = [True, False, True, True, False, True][:n]
        for i in range(n):
            out.append((b, i * 512, 512, kinds[i % 6]))
    return out

def gather_kernel(factors, blocks, *refs):
    srcs, outs = refs[:blocks], refs[blocks:2*blocks]
    local_sem, send_sem, recv_sem = refs[2*blocks:]
    rep, shard = lax.axis_index("rep"), lax.axis_index("shard")
    y, core = lax.div(rep, 2), lax.rem(rep, 2)
    coords = coordinates(shard, factors)
    peers = []
    for i, f in enumerate(factors):
        ids = []
        for d in range(1, f):
            moved = list(coords); moved[i] = lax.rem(coords[i] + d, f)
            ids.append((rep, index_of(moved, factors)))
        peers.append(ids)
    peers.append([((1 - y) * 2 + core, shard)])
    peers.append([(y * 2 + 1 - core, shard)])
    flat = [p for ids in peers for p in ids]
    barrier = pltpu.get_barrier_semaphore()
    for p in flat:
        pl.semaphore_signal(barrier, inc=1, device_id=p, device_id_type=MESH)
    chunks = gather_chunks(srcs[0].shape[1], blocks)
    nph = len(factors) + 2
    base = []
    total = 0
    for ids in peers:
        base.append(total); total += len(ids)
    def columns(k):
        b, c0, w, split = chunks[k]
        if split:
            q = w // 4
            return c0 + (core * 2 + y) * q, q
        return c0 + core * (w // 2), w // 2
    locals_ = []
    for k, (b, c0, w, split) in enumerate(chunks):
        off, width = columns(k)
        cols = pl.ds(pl.multiple_of(off, 128), width)
        cp = pltpu.make_async_copy(srcs[b].at[:, cols], outs[b].at[tuple(coords) + (slice(None), cols)], local_sem.at[k])
        cp.start(); locals_.append(cp)
    pl.semaphore_wait(barrier, len(flat))
    def copies(k, ph):
        b, c0, w, split = chunks[k]
        off, width = columns(k)
        nf = len(factors)
        if ph < nf:
            lead = (slice(None),) * ph + tuple(coords[ph:])
        else:
            lead = (slice(None),) * nf
            if ph == nf + 1:
                off, width = c0 + core * (w // 2), w // 2
        cols = pl.ds(pl.multiple_of(off, 128), width)
        where = lead + (slice(None), cols)
        src = srcs[b].at[:, cols] if ph == 0 else outs[b].at[where]
        return [pltpu.make_async_remote_copy(src_ref=src, dst_ref=outs[b].at[where],
                  send_sem=send_sem.at[k, base[ph] + j], recv_sem=recv_sem.at[k, base[ph] + j], device_id=p, device_id_type=MESH)
                for j, p in enumerate(peers[ph])]
    n = len(chunks)
    started = {}
    def start(k, ph):
        cs = copies(k, ph)
        for c in cs: c.start()
        started[k, ph] = cs
    def phases(k):
        return [p for p in range(nph) if p != nph - 2 or chunks[k][3]]
    ahead = 4
    for k in range(min(ahead, n)):
        start(k, 0)
    for t in range(n + 2 * nph):
        for lag in range(nph - 1, -1, -1):
            k = t - 2 * lag
            if 0 <= k < n:
                ps = phases(k)
                if lag < len(ps):
                    for c in started[k, ps[lag]]: c.wait_recv()
                    if lag == 0:
                        locals_[k].wait()
                        if k + ahead < n:
                            start(k + ahead, 0)
                    if lag + 1 < len(ps): start(k, ps[lag + 1])
    for cs in started.values():
        for c in cs: c.wait_send()

def gather_weights(shards, shard_count, rep_count=4):
    blocks = len(shards)
    factors = shard_factors(shard_count)
    rows, width = shards[0].shape
    n = len(gather_chunks(width, blocks))
    total = sum(f - 1 for f in factors) + 2
    outs = pl.pallas_call(
        functools.partial(gather_kernel, factors, blocks),
        out_shape=[jax.ShapeDtypeStruct(factors + (rows, width), jnp.bfloat16)] * blocks,
        in_specs=[pl.BlockSpec(memory_space=pltpu.VMEM)] * blocks,
        out_specs=[pl.BlockSpec(memory_space=pl.ANY)] * blocks,
        scratch_shapes=[pltpu.SemaphoreType.DMA((n,)), pltpu.SemaphoreType.DMA((n, total)), pltpu.SemaphoreType.DMA((n, total))],
        compiler_params=pltpu.CompilerParams(collective_id=0, has_side_effects=True),
        name="gather_weights",
    )(*shards)
    return [o.reshape(shard_count * rows, width) for o in outs]


def head_half(odd, tile):
    lane = lax.broadcasted_iota(jnp.int32, tile.shape, 1)
    keep = lane >= HEAD_DIM if odd else lane < HEAD_DIM
    return jnp.where(keep, tile, jnp.zeros_like(tile))


def low_lane(shape):
    lane = lax.broadcasted_iota(jnp.int32, shape, 1)
    return lax.rem(lane, HEAD_DIM) < HEAD_DIM // 2


def turn(tile, cosine, sine):
    low = low_lane(tile.shape)
    turned = jnp.where(low, -pltpu.roll(tile, 128 - HEAD_DIM // 2, 1), pltpu.roll(tile, HEAD_DIM // 2, 1))
    return tile * cosine + turned * sine


def turn_back(tile, cosine, sine):
    low = low_lane(tile.shape)
    scaled = tile * sine
    turned = jnp.where(low, pltpu.roll(scaled, 128 - HEAD_DIM // 2, 1), -pltpu.roll(scaled, HEAD_DIM // 2, 1))
    return tile * cosine + turned


def spread(tile, odd):
    wide = tile.astype(jnp.float32)
    other = pltpu.roll(wide, HEAD_DIM, 1)
    lane = lax.broadcasted_iota(jnp.int32, wide.shape, 1)
    pick = (lane >= HEAD_DIM) if odd else (lane < HEAD_DIM)
    return jnp.where(pick, wide, other).astype(tile.dtype)


def dot_nn(a, b):
    return jnp.dot(a, b, preferred_element_type=jnp.float32)


def dot_nt(a, b):
    return lax.dot_general(a, b, (((1,), (1,)), ((), ())), preferred_element_type=jnp.float32)


def dot_tn(a, b):
    return jnp.dot(a.T, b, preferred_element_type=jnp.float32)


def layer_kernel(factors, widths, *refs):
    (tokens_ref, cot_ref, gain_one_ref, gain_two_ref, cosine_ref, sine_ref, mask_ref) = refs[:7]
    srcs = refs[7:11]
    (out_ref, grad_ref, one_t, branch_t, two_t, cot_t, right_a, right_g, right_u, right_d, gains_ref) = refs[11:22]
    w = refs[22:26]
    (one_low, query_low, key_two, value_two, log_ref, hidden_ref, two_low, gate_ref, up_ref, feed_ref,
     upstream_ref, mixed_grad_ref, kv_grad_ref) = refs[26:39]
    local_sem, send_sem, recv_sem = refs[39:]
    query_width, kv_width, hidden_width = widths
    kv_start, value_start, out_start = query_width, query_width + kv_width, query_width + 2 * kv_width
    rep, shard = lax.axis_index("rep"), lax.axis_index("shard")
    y, core = lax.div(rep, 2), lax.rem(rep, 2)
    coords = coordinates(shard, factors)
    nf = len(factors)
    whole = (slice(None),) * nf
    peers = []
    for i, f in enumerate(factors):
        ids = []
        for d in range(1, f):
            moved = list(coords)
            moved[i] = lax.rem(coords[i] + d, f)
            ids.append((rep, index_of(moved, factors)))
        peers.append(ids)
    peers.append([((1 - y) * 2 + core, shard)])
    peers.append([(y * 2 + 1 - core, shard)])
    flat = [p for ids in peers for p in ids]
    barrier = pltpu.get_barrier_semaphore()
    for p in flat:
        pl.semaphore_signal(barrier, inc=1, device_id=p, device_id_type=MESH)
    chunks = gather_chunks(3072, 4)
    nph = nf + 2
    base, total = [], 0
    for ids in peers:
        base.append(total)
        total += len(ids)

    def columns(k):
        b, c0, width, split = chunks[k]
        if split:
            return c0 + (core * 2 + y) * (width // 4), width // 4
        return c0 + core * (width // 2), width // 2

    def own_source(k):
        b = chunks[k][0]
        off, width = columns(k)
        return srcs[b].at[:, pl.ds(pl.multiple_of(off, 128), width)]

    locals_ = []
    for k, (b, _, _, _) in enumerate(chunks):
        off, width = columns(k)
        cols = pl.ds(pl.multiple_of(off, 128), width)
        copy = pltpu.make_async_copy(own_source(k), w[b].at[tuple(coords) + (slice(None), cols)], local_sem.at[k])
        copy.start()
        locals_.append(copy)
    pl.semaphore_wait(barrier, len(flat))

    def copies(k, ph):
        b, c0, wide, _ = chunks[k]
        off, width = columns(k)
        if ph < nf:
            lead = (slice(None),) * ph + tuple(coords[ph:])
        else:
            lead = whole
            if ph == nf + 1:
                off, width = c0 + core * (wide // 2), wide // 2
        where = lead + (slice(None), pl.ds(pl.multiple_of(off, 128), width))
        src = own_source(k) if ph == 0 else w[b].at[where]
        return [
            pltpu.make_async_remote_copy(
                src_ref=src, dst_ref=w[b].at[where], send_sem=send_sem.at[k, base[ph] + j],
                recv_sem=recv_sem.at[k, base[ph] + j], device_id=p, device_id_type=MESH)
            for j, p in enumerate(peers[ph])
        ]

    n = len(chunks)
    started = {}

    def start(k, ph):
        cs = copies(k, ph)
        for c in cs:
            c.start()
        started[k, ph] = cs

    def phases(k):
        return [p for p in range(nph) if p != nph - 2 or chunks[k][3]]

    def weight(b, c0, c1):
        got = w[b][whole + (slice(None), slice(c0, c1))]
        return got.reshape(-1, c1 - c0)

    def gain(ref):
        return ref[...]

    def open_norm():
        inputs = tokens_ref[...].astype(jnp.float32)
        inverse = lax.rsqrt(jnp.mean(inputs * inputs, axis=-1, keepdims=True) + NORM_EPS)
        low = (inputs * inverse * gain(gain_one_ref)).astype(jnp.bfloat16)
        one_low[...] = low
        one_t[...] = low.T
        cot_t[...] = cot_ref[...].T

    def project(c0, c1):
        low = one_low[...]
        for c in range(c0, min(c1, out_start), 256):
            e = min(c + 256, c1, out_start)
            got = dot_nn(low, weight(0, c, e))
            for s in range(c, e, 128):
                tile = got[:, s - c:s - c + 128]
                if s < kv_start:
                    query_low[:, s:s + 128] = turn(tile, cosine_ref[...], sine_ref[...]).astype(jnp.bfloat16)
                elif s < value_start:
                    turned = turn(tile, cosine_ref[...], sine_ref[...]).astype(jnp.bfloat16)
                    j = (s - kv_start) // 64
                    key_two[j] = spread(turned, False)
                    key_two[j + 1] = spread(turned, True)
                else:
                    low_tile = tile.astype(jnp.bfloat16)
                    j = (s - value_start) // 64
                    value_two[j] = spread(low_tile, False)
                    value_two[j + 1] = spread(low_tile, True)

    per_group = HEADS // KV_HEADS

    def scores_of(query, j):
        scores = ATTENTION_SCALE * dot_nt(query, key_two[j])
        return jnp.where(mask_ref[...] > 0, scores, MASK_FILL)

    def attend(pair):
        tile = query_low[:, pair * 128:pair * 128 + 128]
        halves = []
        for odd in (False, True):
            h = 2 * pair + odd
            j = h // per_group
            scores = scores_of(head_half(odd, tile), j)
            top = jnp.max(scores, axis=-1, keepdims=True)
            raised = jnp.exp(scores - top)
            log_total = top + jnp.log(jnp.sum(raised, axis=-1, keepdims=True))
            log_ref[h] = log_total
            probs = jnp.exp(scores - log_total).astype(jnp.bfloat16)
            halves.append(dot_nn(probs, value_two[j]))
        lane = lax.broadcasted_iota(jnp.int32, halves[0].shape, 1)
        right_a[:, out_start + pair * 128:out_start + pair * 128 + 128] = jnp.where(
            lane < HEAD_DIM, halves[0], halves[1]).astype(jnp.bfloat16)

    def mix():
        hidden_ref[...] = tokens_ref[...].astype(jnp.float32) + dot_nt(
            right_a[:, out_start:], weight(0, out_start, out_start + query_width))

    def second_norm():
        hidden = hidden_ref[...]
        inverse = lax.rsqrt(jnp.mean(hidden * hidden, axis=-1, keepdims=True) + NORM_EPS)
        low = (hidden * inverse * gain(gain_two_ref)).astype(jnp.bfloat16)
        two_low[...] = low
        two_t[...] = low.T

    def gate(c0, c1):
        for c in range(c0, c1, 256):
            gate_ref[:, c:c + 256] = dot_nn(two_low[...], weight(1, c, c + 256))

    def up(c0, c1):
        for c in range(c0, c1, 256):
            got = dot_nn(two_low[...], weight(2, c, c + 256))
            up_ref[:, c:c + 256] = got
            g = gate_ref[:, c:c + 256]
            right_d[:, c:c + 256] = (g * jax.nn.sigmoid(g) * got).astype(jnp.bfloat16)

    first_down = [True]

    def down(c0, c1):
        piece = weight(3, c0, c1)
        feed = dot_nt(right_d[:, c0:c1], piece)
        for c in range(c0, c1, 256):
            back = dot_nn(cot_ref[...], weight(3, c, c + 256))
            g, u = gate_ref[:, c:c + 256], up_ref[:, c:c + 256]
            s = jax.nn.sigmoid(g)
            right_g[:, c:c + 256] = (back * u * (s * (1.0 + g * (1.0 - s)))).astype(jnp.bfloat16)
            right_u[:, c:c + 256] = (back * (g * s)).astype(jnp.bfloat16)
        up_part = dot_nt(right_g[:, c0:c1], weight(1, c0, c1)) + dot_nt(right_u[:, c0:c1], weight(2, c0, c1))
        if first_down[0]:
            feed_ref[...] = feed
            upstream_ref[...] = up_part
            first_down[0] = False
        else:
            feed_ref[...] += feed
            upstream_ref[...] += up_part

    def close_feed():
        hidden = hidden_ref[...]
        out_ref[...] = (hidden + feed_ref[...]).astype(jnp.bfloat16)
        inverse = lax.rsqrt(jnp.mean(hidden * hidden, axis=-1, keepdims=True) + NORM_EPS)
        unit = hidden * inverse
        upstream = upstream_ref[...]
        gains_ref[1:2, :] = jnp.sum(upstream * unit, axis=0, keepdims=True)
        scaled = upstream * gain(gain_two_ref)
        residual = cot_ref[...].astype(jnp.float32) + inverse * (
            scaled - unit * jnp.mean(scaled * unit, axis=-1, keepdims=True))
        hidden_ref[...] = residual
        low = residual.astype(jnp.bfloat16)
        branch_t[...] = low.T
        mixed_grad_ref[...] = dot_nn(low, weight(0, out_start, out_start + query_width)).astype(jnp.bfloat16)
        kv_grad_ref[...] = jnp.zeros_like(kv_grad_ref)

    def attend_back(pair):
        cols = slice(pair * 128, pair * 128 + 128)
        tile, grad_tile = query_low[:, cols], mixed_grad_ref[:, cols]
        halves = []
        for odd in (False, True):
            h = 2 * pair + odd
            j = h // per_group
            query, grad = head_half(odd, tile), head_half(odd, grad_tile)
            probs = jnp.exp(scores_of(query, j) - log_ref[h])
            prob_grad = dot_nt(grad, value_two[j])
            inner = jnp.sum(probs * prob_grad, axis=-1, keepdims=True)
            score_grad = (probs * (prob_grad - inner)).astype(jnp.bfloat16)
            halves.append(dot_nn(score_grad, key_two[j]))
            kv_grad_ref[j] += dot_tn(score_grad, query)
            kv_grad_ref[KV_HEADS + j] += dot_tn(probs.astype(jnp.bfloat16), grad)
        lane = lax.broadcasted_iota(jnp.int32, halves[0].shape, 1)
        both = ATTENTION_SCALE * jnp.where(lane < HEAD_DIM, halves[0], halves[1])
        right_a[:, cols] = turn_back(both, cosine_ref[...], sine_ref[...]).astype(jnp.bfloat16)

    def fold(j):
        first, second = kv_grad_ref[j], kv_grad_ref[j + 1]
        first = first + pltpu.roll(first, HEAD_DIM, 1)
        second = second + pltpu.roll(second, HEAD_DIM, 1)
        lane = lax.broadcasted_iota(jnp.int32, first.shape, 1)
        return jnp.where(lane < HEAD_DIM, first, second)

    def close_attention():
        for j in range(0, KV_HEADS, 2):
            c = kv_start + j * HEAD_DIM
            right_a[:, c:c + 128] = turn_back(
                ATTENTION_SCALE * fold(j), cosine_ref[...], sine_ref[...]).astype(jnp.bfloat16)
            c = value_start + j * HEAD_DIM
            right_a[:, c:c + 128] = fold(KV_HEADS + j).astype(jnp.bfloat16)
        upstream = dot_nt(right_a[:, :out_start], weight(0, 0, out_start))
        inputs = tokens_ref[...].astype(jnp.float32)
        inverse = lax.rsqrt(jnp.mean(inputs * inputs, axis=-1, keepdims=True) + NORM_EPS)
        unit = inputs * inverse
        gains_ref[0:1, :] = jnp.sum(upstream * unit, axis=0, keepdims=True)
        scaled = upstream * gain(gain_one_ref)
        grad_ref[...] = (hidden_ref[...] + inverse * (
            scaled - unit * jnp.mean(scaled * unit, axis=-1, keepdims=True))).astype(jnp.bfloat16)

    per_block = n // 4
    tasks = [((), 3.0, open_norm)]
    for c in range(per_block):
        c0, c1 = chunks[c][1], chunks[c][1] + chunks[c][2]
        if c0 < out_start:
            tasks.append(((c,), 0.8, functools.partial(project, c0, c1)))
    for pair in range(HEADS // 2):
        tasks.append(((), 1.3, functools.partial(attend, pair)))
    tasks.append((tuple(range(per_block)), 1.5, mix))
    tasks.append(((), 1.2, second_norm))
    for b, run, cost in ((1, gate, 0.5), (2, up, 0.7), (3, down, 2.5)):
        for c in range(per_block):
            k = b * per_block + c
            tasks.append(((k,), cost, functools.partial(run, chunks[k][1], chunks[k][1] + chunks[k][2])))
    tasks.append(((), 3.0, close_feed))
    for pair in range(HEADS // 2):
        tasks.append(((), 2.5, functools.partial(attend_back, pair)))
    tasks.append(((), 3.0, close_attention))
    finished = set()
    gains_ref[...] = jnp.zeros_like(gains_ref)

    def advance(budget):
        while tasks and budget > 0 and all(k in finished for k in tasks[0][0]):
            _, cost, run = tasks.pop(0)
            run()
            budget -= cost

    ahead = 4
    for k in range(min(ahead, n)):
        start(k, 0)
    for t in range(n + 2 * nph):
        for lag in range(nph - 1, -1, -1):
            k = t - 2 * lag
            if 0 <= k < n:
                ps = phases(k)
                if lag < len(ps):
                    for c in started[k, ps[lag]]:
                        c.wait_recv()
                    if lag == 0:
                        locals_[k].wait()
                        if k + ahead < n:
                            start(k + ahead, 0)
                    if lag + 1 < len(ps):
                        start(k, ps[lag + 1])
                    else:
                        finished.add(k)
        advance(BUDGET)
    advance(1e9)
    for cs in started.values():
        for c in cs:
            c.wait_send()


BUDGET = 3.5


def run_layer(tokens, cotangent, gain_one, gain_two, cosine, sine, visible, shards, widths, shard_count):
    factors = shard_factors(shard_count)
    count, model = tokens.shape
    query_width, kv_width, hidden_width = widths
    rows = shards[0].shape[0]
    n = len(gather_chunks(3072, 4))
    links = sum(f - 1 for f in factors) + 2
    bf, f32 = jnp.bfloat16, jnp.float32
    vm, anywhere = pl.BlockSpec(memory_space=pltpu.VMEM), pl.BlockSpec(memory_space=pl.ANY)
    turned = jax.ShapeDtypeStruct((model, count), bf)
    flat = jax.ShapeDtypeStruct((count, model), bf)
    wide = jax.ShapeDtypeStruct((count, hidden_width), bf)
    return pl.pallas_call(
        functools.partial(layer_kernel, factors, widths),
        out_shape=[flat, flat, turned, turned, turned, turned, wide, wide, wide, wide,
                   jax.ShapeDtypeStruct((8, model), f32)],
        in_specs=[vm] * 7 + [anywhere] * 4,
        out_specs=[vm] * 11,
        scratch_shapes=[pltpu.VMEM(factors + (rows, hidden_width), bf)] * 4 + [
            pltpu.VMEM((count, model), bf),
            pltpu.VMEM((count, query_width), bf),
            pltpu.VMEM((KV_HEADS, count, 128), bf),
            pltpu.VMEM((KV_HEADS, count, 128), bf),
            pltpu.VMEM((HEADS, count, 1), f32),
            pltpu.VMEM((count, model), f32),
            pltpu.VMEM((count, model), bf),
            pltpu.VMEM((count, hidden_width), f32),
            pltpu.VMEM((count, hidden_width), f32),
            pltpu.VMEM((count, model), f32),
            pltpu.VMEM((count, model), f32),
            pltpu.VMEM((count, query_width), bf),
            pltpu.VMEM((2 * KV_HEADS, count, 128), f32),
            pltpu.SemaphoreType.DMA((n,)),
            pltpu.SemaphoreType.DMA((n, links)),
            pltpu.SemaphoreType.DMA((n, links)),
        ],
        compiler_params=pltpu.CompilerParams(collective_id=0, has_side_effects=True, vmem_limit_bytes=67043328),
        name="run_layer",
    )(tokens, cotangent, gain_one.reshape(1, -1), gain_two.reshape(1, -1), cosine, sine, visible, *shards)


def scatter_kernel(factors, parts, blocks, layout, *refs):
    nf = len(factors)
    nl = len(layout["lefts"])
    lefts = refs[:nl]
    rights = refs[nl:nl + blocks]
    small_in = refs[nl + blocks]
    at = nl + blocks + 1
    params = layout["params"]
    weights = refs[at:at + blocks]
    moments = refs[at + blocks:at + blocks + params]
    variances = refs[at + blocks + params:at + blocks + 2 * params]
    at += blocks + 2 * params
    outs = refs[at:at + blocks]
    small_out, norm_out = refs[at + blocks:at + blocks + 2]
    scratch = list(refs[at + blocks + 2:])
    stage, pair_in, wide_y, final = scratch[:4]
    lean = scratch[4:4 + nf]
    quart = scratch[4 + nf:4 + 2 * nf]
    lean_y = scratch[4 + 2 * nf]
    small = scratch[5 + 2 * nf:5 + 2 * nf + nf + 2]
    rest = scratch[5 + 2 * nf + nf + 2:]
    norm_slots = rest[:nf]
    held_m, held_v, held_w, step_acc, weight_acc = rest[nf:nf + 5]
    send_sem, recv_sem, out_sem, small_send, small_recv, fetch_sem, norm_send, norm_recv = rest[nf + 5:]
    rows = final.shape[1]
    steps = final.shape[0]
    ring = stage.shape[0]
    rep, shard = lax.axis_index("rep"), lax.axis_index("shard")
    y, core = lax.div(rep, 2), lax.rem(rep, 2)
    coords = coordinates(shard, factors)
    y_peer = ((1 - y) * 2 + core, shard)
    core_peer = (y * 2 + 1 - core, shard)

    def factor_peer(i, d):
        moved = list(coords)
        moved[i] = lax.rem(coords[i] + d, factors[i])
        return (rep, index_of(moved, factors)), moved[i]

    everyone = [y_peer, core_peer]
    for i, f in enumerate(factors):
        everyone += [factor_peer(i, d)[0] for d in range(1, f)]
    barrier = pltpu.get_barrier_semaphore()
    for p in everyone:
        pl.semaphore_signal(barrier, inc=1, device_id=p, device_id_type=MESH)

    order = list(range(nf - 1, -1, -1))
    column = {"core": 0, "y_wide": 1, "y_lean": 2, "y_back": 3, "core_back": 4}
    used = 5
    for i in order:
        column["lean", i] = used
        used += factors[i] - 1
        column["quart", i] = used
        used += factors[i] - 1

    def remote(k, c, src, dst, peer):
        return pltpu.make_async_remote_copy(
            src_ref=src, dst_ref=dst, send_sem=send_sem.at[lax.rem(k, ring), c],
            recv_sem=recv_sem.at[k, c], device_id=peer, device_id_type=MESH)

    half, quarter = 512, 128
    mine = pl.multiple_of(core * half, half)
    other = pl.multiple_of((1 - core) * half, half)
    my_q = pl.multiple_of(256 + y * quarter, quarter)
    other_q = pl.multiple_of(256 + (1 - y) * quarter, quarter)
    whole = (slice(None),) * nf

    def core_copy(k):
        slot = lax.rem(k, ring)
        return [remote(k, column["core"], stage.at[(slot,) + whole + (slice(None), pl.ds(other, half))], pair_in.at[k], core_peer)]

    def y_wide_copy(k):
        return [remote(k, column["y_wide"], pair_in.at[(k,) + whole + (slice(None), pl.ds(other_q, quarter))], wide_y.at[k], y_peer)]

    def view(kind, i, k):
        if i == nf - 1:
            if kind == "lean":
                return pair_in.at[(k,) + whole + (slice(None), pl.ds(0, 256))]
            return wide_y.at[k]
        box = lean if kind == "lean" else quart
        return box[i + 1].at[k, 0]

    def factor_copies(kind, i, k):
        box = lean if kind == "lean" else quart
        source = view(kind, i, k)
        out = []
        for d in range(1, factors[i]):
            peer, j = factor_peer(i, d)
            out.append(remote(k, column[kind, i] + d - 1, source.at[(slice(None),) * i + (j,)], box[i].at[k, d - 1], peer))
        return out

    def factor_sum(kind, i, k):
        box = lean if kind == "lean" else quart
        total = view(kind, i, k)[(slice(None),) * i + (coords[i],)].astype(jnp.float32)
        for d in range(1, factors[i]):
            total = total + box[i][k, d - 1].astype(jnp.float32)
        return total

    def y_lean_copy(k):
        return [remote(k, column["y_lean"], lean[0].at[k, 0], lean_y.at[k], y_peer)]

    def y_back_copy(k):
        where = (k, slice(None), pl.ds(pl.multiple_of(mine + my_q, quarter), quarter))
        return [remote(k, column["y_back"], final.at[where], final.at[where], y_peer)]

    def core_back_copy(k):
        where = (k, slice(None), pl.ds(mine, half))
        return [remote(k, column["core_back"], final.at[where], final.at[where], core_peer)]

    def begin(copies):
        for c in copies:
            c.start()

    def finish(copies):
        for c in copies:
            c.wait()

    def product(left, right_ref, cols, slot, at, part):
        width = cols[1] - cols[0]
        for c in range(0, width, 256):
            w = min(256, width - c)
            right = right_ref[:, cols[0] + c:cols[0] + c + w]
            if rows % 16 == 0:
                lhs = left[:, part].reshape(-1, left.shape[-1])
                got = jnp.dot(lhs, right, preferred_element_type=jnp.float32).astype(jnp.bfloat16)
                stage[(slot,) + whole + (slice(None), slice(at + c, at + c + w))] = got.reshape(factors + (rows, w))
            else:
                def one(s, carry):
                    got = jnp.dot(left[s, part], right, preferred_element_type=jnp.float32).astype(jnp.bfloat16)
                    where = tuple(coordinates(s, factors))
                    stage[(slot,) + where + (slice(None), slice(at + c, at + c + w))] = got
                    return carry
                lax.fori_loop(0, left.shape[0], one, 0)

    groups = layout["groups"]

    def compute(k):
        group, part = lax.div(k, parts), lax.rem(k, parts)
        slot = lax.rem(k, ring)
        for g, pieces in enumerate(groups):
            @pl.when(group == g)
            def _():
                at = 0
                for left, right, c0, c1 in pieces:
                    product(lefts[left], rights[right], (c0, c1), slot, at, part)
                    at += c1 - c0

    def out_copies(k, g, part):
        block, start = layout["places"][g]
        return pltpu.make_async_copy(final.at[k], outs[block].at[pl.ds(pl.multiple_of(part * rows, rows), rows), pl.ds(start, 1024)], out_sem.at[k])

    stages = [[] for _ in range(nf + 5)]

    def stage0(k):
        compute(k)
        begin(core_copy(k))

    def stage1(k):
        finish(core_copy(k))
        slot = lax.rem(k, ring)
        pair_in[k] = (pair_in[k].astype(jnp.float32) + stage[(slot,) + whole + (slice(None), pl.ds(mine, half))].astype(jnp.float32)).astype(jnp.bfloat16)
        begin(y_wide_copy(k))
        begin(factor_copies("lean", order[0], k))

    def middle(pos):
        def run(k):
            i = order[pos]
            if pos == 0:
                finish(y_wide_copy(k))
                wide_y[k] = (wide_y[k].astype(jnp.float32) + pair_in[(k,) + whole + (slice(None), pl.ds(my_q, quarter))].astype(jnp.float32)).astype(jnp.bfloat16)
            else:
                before = order[pos - 1]
                finish(factor_copies("quart", before, k))
                quart[before][k, 0] = factor_sum("quart", before, k).astype(jnp.bfloat16)
            begin(factor_copies("quart", i, k))
            finish(factor_copies("lean", i, k))
            lean[i][k, 0] = factor_sum("lean", i, k).astype(jnp.bfloat16)
            if pos + 1 < nf:
                begin(factor_copies("lean", order[pos + 1], k))
            else:
                begin(y_lean_copy(k))
        return run

    def settle(k):
        finish(factor_copies("quart", 0, k))
        final[k, :, pl.ds(pl.multiple_of(mine + my_q, quarter), quarter)] = factor_sum("quart", 0, k).astype(jnp.bfloat16)
        begin(y_back_copy(k))
        finish(y_lean_copy(k))
        final[k, :, pl.ds(mine, 256)] = (lean[0][k, 0].astype(jnp.float32) + lean_y[k].astype(jnp.float32)).astype(jnp.bfloat16)

    def give(k):
        finish(y_back_copy(k))
        begin(core_back_copy(k))

    hold = held_m.shape[0]

    def fetches(k, g, part):
        slot = lax.rem(k, hold)
        down = pl.ds(pl.multiple_of(part * rows, rows), rows)
        block, start = layout["places"][g]
        found = [pltpu.make_async_copy(weights[block].at[down, pl.ds(start, 1024)], held_w.at[slot], fetch_sem.at[slot, 0])]
        c = 0
        for j, (param, first, width) in enumerate(layout["cuts"][g]):
            for box, source, column_of in ((held_m, moments, 1), (held_v, variances, 5)):
                found.append(pltpu.make_async_copy(
                    source[param].at[down, pl.ds(first, width)], box.at[slot, :, pl.ds(c, width)],
                    fetch_sem.at[slot, column_of + j]))
            c += width
        return found

    def by_group(k, action):
        group, part = lax.div(k, parts), lax.rem(k, parts)
        for g in range(len(groups)):
            pl.when(group == g)(lambda g=g: action(k, g, part))

    def fetch(k):
        by_group(k, lambda k, g, part: begin(fetches(k, g, part)))

    def leave(k):
        finish(core_back_copy(k))
        by_group(k, lambda k, g, part: out_copies(k, g, part).start())
        by_group(k, lambda k, g, part: finish(fetches(k, g, part)))
        slot, group = lax.rem(k, hold), lax.div(k, parts)
        gradient = final[k].astype(jnp.float32)
        weight = held_w[slot].astype(jnp.float32)
        direction = adam_direction(weight, gradient, held_m[slot], held_v[slot])[2]
        step_acc[group] += jnp.sum(direction * direction, axis=0, keepdims=True)
        weight_acc[group] += jnp.sum(weight * weight, axis=0, keepdims=True)

    lags = list(layout["lags"])
    stages = [stage0, stage1] + [middle(p) for p in range(nf)] + [settle, give, leave, fetch]
    lags.append(lags[-1] - 3)
    step_acc[...] = jnp.zeros_like(step_acc)
    weight_acc[...] = jnp.zeros_like(weight_acc)

    small_stages = [("core", 2, core, lambda d: core_peer), ("y", 2, y, lambda d: y_peer)]
    for i in order:
        small_stages.append((i, factors[i], coords[i], lambda d, i=i: factor_peer(i, d)[0]))
    small_base = []
    count = 0
    for s in small_stages:
        small_base.append(count)
        count += s[1] - 1

    def small_copies(j):
        _, f, own, peer = small_stages[j]
        return [pltpu.make_async_remote_copy(src_ref=small[j].at[own], dst_ref=small[j].at[own],
                 send_sem=small_send.at[small_base[j] + d - 1], recv_sem=small_recv.at[small_base[j] + d - 1],
                 device_id=peer(d), device_id_type=MESH) for d in range(1, f)]

    def small_step(j):
        if j > 0:
            finish(small_copies(j - 1))
            total = small[j - 1][0]
            for a in range(1, small_stages[j - 1][1]):
                total = total + small[j - 1][a]
        else:
            total = small_in[...]
        if j < len(small_stages):
            small[j][small_stages[j][2]] = total
            begin(small_copies(j))
        else:
            small_out[...] = total

    pl.semaphore_wait(barrier, len(everyone))

    def step(t, carry):
        for lag, run in reversed(list(zip(lags, stages))):
            k = t - lag
            @pl.when((k >= 0) & (k < steps))
            def _():
                run(k)
        for j in range(len(small_stages) + 1):
            pl.when(t == j + 1)(functools.partial(small_step, j))
        return carry
    lax.fori_loop(0, steps + max(lags), step, 0)

    lines = lax.broadcasted_iota(jnp.int32, (16, 128), 0)
    total = jnp.zeros((16, 128), jnp.float32)
    for acc, offset in ((step_acc, 0), (weight_acc, 8)):
        sums = [None] * params
        for g in range(len(groups)):
            c = 0
            for param, _, width in layout["cuts"][g]:
                value = jnp.sum(acc[g, :, c:c + width])
                sums[param] = value if sums[param] is None else sums[param] + value
                c += width
        for param in range(params):
            total = jnp.where(lines == offset + param, sums[param], total)
    done = 0
    for i in order:
        norm_slots[i][coords[i]] = total
        copies = []
        for d in range(1, factors[i]):
            where = norm_slots[i].at[coords[i]]
            copies.append(pltpu.make_async_remote_copy(
                src_ref=where, dst_ref=where, send_sem=norm_send.at[done], recv_sem=norm_recv.at[done],
                device_id=factor_peer(i, d)[0], device_id_type=MESH))
            done += 1
        begin(copies)
        finish(copies)
        total = norm_slots[i][0]
        for a in range(1, factors[i]):
            total = total + norm_slots[i][a]
    norm_out[...] = total

    def drain(k, carry):
        group, part = lax.div(k, parts), lax.rem(k, parts)
        for g in range(len(groups)):
            pl.when(group == g)(lambda g=g: out_copies(k, g, part).wait())
        return carry
    lax.fori_loop(0, steps, drain, 0)


def scatter_gradients(lefts, rights, small, weights, moments, variances, layout, shard_count, lags=None):
    factors = shard_factors(shard_count)
    nf = len(factors)
    model, tokens = lefts[0].shape
    rows_all = model // shard_count
    parts = 3 if rows_all % 48 == 0 else 1
    rows = rows_all // parts
    blocks = len(rights)
    steps = len(layout["groups"]) * parts
    layout = dict(layout)
    layout["lags"] = lags or ([0, 1] + [1 + 2 * (p + 1) for p in range(nf + 1)] + [1 + 2 * (nf + 1) + 1, 1 + 2 * (nf + 1) + 2])
    ring = layout["lags"][-1] + 1 if layout["lags"][-1] < 4 else 4
    layout["lefts"] = lefts
    turned = [v.reshape(shard_count, parts, rows, tokens) for v in lefts]
    bf = jnp.bfloat16
    lean = [pltpu.VMEM((steps, factors[i] - 1) + factors[:i] + (rows, 256), bf) for i in range(nf)]
    quart = [pltpu.VMEM((steps, factors[i] - 1) + factors[:i] + (rows, 128), bf) for i in range(nf)]
    order = list(range(nf - 1, -1, -1))
    smalls = [pltpu.VMEM((f,) + small.shape, jnp.float32) for f in [2, 2] + [factors[i] for i in order]]
    ncol = 5 + 2 * sum(f - 1 for f in factors)
    nsmall = 2 + sum(f - 1 for f in factors)
    vm = pl.BlockSpec(memory_space=pltpu.VMEM)
    layout["lefts"] = list(range(len(lefts)))
    params = layout["params"] = len(moments)
    anywhere = pl.BlockSpec(memory_space=pl.ANY)
    hold = 5
    outs = pl.pallas_call(
        functools.partial(scatter_kernel, factors, parts, blocks, layout),
        out_shape=[jax.ShapeDtypeStruct((rows_all, rights[0].shape[1]), bf)] * blocks + [jax.ShapeDtypeStruct(small.shape, jnp.float32), jax.ShapeDtypeStruct((16, 128), jnp.float32)],
        in_specs=[vm] * (len(lefts) + blocks + 1) + [anywhere] * (blocks + 2 * params),
        out_specs=[anywhere] * blocks + [vm, vm],
        scratch_shapes=[
            pltpu.VMEM((ring,) + factors + (rows, 1024), bf),
            pltpu.VMEM((steps,) + factors + (rows, 512), bf),
            pltpu.VMEM((steps,) + factors + (rows, 128), bf),
            pltpu.VMEM((steps, rows, 1024), bf),
        ] + lean + quart + [pltpu.VMEM((steps, rows, 256), bf)] + smalls + [
            pltpu.VMEM((f, 16, 128), jnp.float32) for f in factors
        ] + [
            pltpu.VMEM((hold, rows, 1024), jnp.float32),
            pltpu.VMEM((hold, rows, 1024), jnp.float32),
            pltpu.VMEM((hold, rows, 1024), bf),
            pltpu.VMEM((len(layout["groups"]), 1, 1024), jnp.float32),
            pltpu.VMEM((len(layout["groups"]), 1, 1024), jnp.float32),
            pltpu.SemaphoreType.DMA((ring, ncol)),
            pltpu.SemaphoreType.DMA((steps, ncol)),
            pltpu.SemaphoreType.DMA((steps,)),
            pltpu.SemaphoreType.DMA((nsmall,)),
            pltpu.SemaphoreType.DMA((nsmall,)),
            pltpu.SemaphoreType.DMA((hold, 9)),
            pltpu.SemaphoreType.DMA((nsmall,)),
            pltpu.SemaphoreType.DMA((nsmall,)),
        ],
        compiler_params=pltpu.CompilerParams(collective_id=1, has_side_effects=True, vmem_limit_bytes=62 << 20),
        name="scatter_gradients",
    )(*turned, *rights, small, *weights, *moments, *variances)
    return outs[:blocks], outs[blocks], outs[blocks + 1]


def gradient_layout(widths):
    spans, start = [], 0
    for param, width in enumerate(widths[:4]):
        spans.append((param, start, start + width))
        start += width
    cut = spans[3][1]
    groups, places, cuts = [], [], []
    for block in (1, 2, 3):
        for c in range(0, widths[3 + block], 1024):
            groups.append([(3 if block == 3 else 2, block, c, c + 1024)])
            places.append((block, c))
            cuts.append([(3 + block, c, 1024)])
    for c in range(0, start, 1024):
        pieces = [(0, 0, c, min(c + 1024, cut)), (1, 0, max(c, cut), c + 1024)]
        groups.append([p for p in pieces if p[2] < p[3]])
        places.append((0, c))
        found = []
        for param, low, high in spans:
            if max(low, c) < min(high, c + 1024):
                found.append((param, max(low, c) - low, min(high, c + 1024) - max(low, c)))
        cuts.append(found)
    return {"groups": groups, "places": places, "cuts": cuts}


def tree_layout(segment_row, parent_row):
    segment_count = parent_row.shape[0]
    labels = jnp.arange(segment_count, dtype=jnp.int32)
    parent_hot = (parent_row[:, None] == labels[None, :]).astype(jnp.int32)
    identity = (labels[:, None] == labels[None, :]).astype(jnp.int32)

    ancestry = jnp.minimum(identity + parent_hot, 1)
    reach = 1
    while reach < segment_count:
        ancestry = jnp.minimum(jnp.sum(ancestry[:, :, None] * ancestry[None, :, :], axis=1), 1)
        reach *= 2
    segment_hot = (segment_row[:, None] == labels[None, :]).astype(jnp.int32)
    lengths = jnp.sum(segment_hot, axis=0, dtype=jnp.int32)
    depth_sum = jnp.dot(ancestry - identity, lengths)
    token_index = jnp.arange(segment_row.shape[0], dtype=jnp.int32)
    earlier = jnp.sum(
        (segment_row[None, :] < segment_row[:, None]).astype(jnp.int32), axis=1, dtype=jnp.int32
    )
    positions = token_index - earlier + jnp.dot(segment_hot, depth_sum)
    reach_count = jnp.dot(jnp.dot(segment_hot, ancestry), segment_hot.T)
    visible = (reach_count > 0) & (token_index[None, :] <= token_index[:, None])
    return (positions, visible)


def rope_tables(positions, head_size):
    half_size = head_size // 2
    exponent = jnp.arange(half_size, dtype=jnp.float32) * (-2.0 / head_size)
    frequency = jnp.power(ROPE_BASE, exponent)
    angles = positions.astype(jnp.float32)[:, None] * frequency[None, :]
    angles = jnp.concatenate([angles, angles], axis=1)
    return (jnp.cos(angles), jnp.sin(angles))


def rotate(states, cosine_table, sine_table):
    half_size = states.shape[-1] // 2
    turned = jnp.concatenate([-states[..., half_size:], states[..., :half_size]], axis=-1)
    return states * cosine_table[:, None, :] + turned * sine_table[:, None, :]


def unrotate(gradient, cosine_table, sine_table):
    half_size = gradient.shape[-1] // 2
    scaled = gradient * sine_table[:, None, :]
    turned = jnp.concatenate([scaled[..., half_size:], -scaled[..., :half_size]], axis=-1)
    return gradient * cosine_table[:, None, :] + turned


def dense(left_side, right_side):
    return jnp.dot(left_side, right_side, preferred_element_type=jnp.float32)


def dense_back(left_side, right_side):
    return lax.dot_general(
        left_side, right_side, (((1,), (1,)), ((), ())), preferred_element_type=jnp.float32
    )


def dense_rows(left_side, right_side):
    return lax.dot_general(
        left_side, right_side, (((0,), (0,)), ((), ())), preferred_element_type=jnp.float32
    )


def normalize(inputs):
    inverse_root = lax.rsqrt(jnp.mean(inputs * inputs, axis=-1, keepdims=True) + NORM_EPS)
    return (inputs * inverse_root, inverse_root)


def norm_backward(upstream, unit_rows, inverse_root, gain_vector):
    scaled = upstream * gain_vector
    return inverse_root * (
        scaled - unit_rows * jnp.mean(scaled * unit_rows, axis=-1, keepdims=True)
    )


def attention_scores(query_turned, key_turned, visible):
    scores = ATTENTION_SCALE * jnp.einsum(
        "tkgd,ukd->kgtu", query_turned, key_turned, preferred_element_type=jnp.float32
    )
    return jnp.where(visible[None, None], scores, MASK_FILL)


def adam_direction(weight, gradient, moment, variance):
    next_moment = BETA_FIRST * moment + (1.0 - BETA_FIRST) * gradient
    next_variance = BETA_SECOND * variance + (1.0 - BETA_SECOND) * gradient * gradient
    direction = next_moment / (jnp.sqrt(next_variance) + ADAM_EPS) + DECAY_RATE * weight
    return (next_moment, next_variance, direction)


def layer_apart(
    tokens_in, cotangent, norm_attention, norm_feedforward, cosine_table, sine_table, visible, shards, widths, shard_count
):
    query_width, kv_width, hidden_width = widths
    token_count = tokens_in.shape[0]
    per_group = HEADS // KV_HEADS
    inputs = tokens_in.astype(jnp.float32)
    unit_one, inverse_one = normalize(inputs)
    normed_one = (unit_one * norm_attention).astype(jnp.bfloat16)
    second_cut = query_width + kv_width
    third_cut = query_width + 2 * kv_width
    full_attention, full_gate, full_up, full_down = gather_weights(shards, shard_count)
    full_input, full_output = full_attention[:, :third_cut], full_attention[:, third_cut:]
    input_states = dense(normed_one, full_input)
    query_states = input_states[:, :query_width]
    key_states = input_states[:, query_width:second_cut]
    value_states = input_states[:, second_cut:]
    query_turned = rotate(
        query_states.reshape(token_count, HEADS, HEAD_DIM), cosine_table, sine_table
    ).astype(jnp.bfloat16)
    query_turned = query_turned.reshape(token_count, KV_HEADS, per_group, HEAD_DIM)
    key_turned = rotate(
        key_states.reshape(token_count, KV_HEADS, HEAD_DIM), cosine_table, sine_table
    ).astype(jnp.bfloat16)
    value_heads = value_states.astype(jnp.bfloat16).reshape(token_count, KV_HEADS, HEAD_DIM)
    scores = attention_scores(query_turned, key_turned, visible)
    row_max = jnp.max(scores, axis=-1, keepdims=True)
    log_total = row_max + jnp.log(jnp.sum(jnp.exp(scores - row_max), axis=-1, keepdims=True))
    softmax_low = jnp.exp(scores - log_total).astype(jnp.bfloat16)
    mixed_low = jnp.einsum(
        "kgtu,ukd->tkgd", softmax_low, value_heads, preferred_element_type=jnp.float32
    )
    mixed_low = mixed_low.reshape(token_count, query_width).astype(jnp.bfloat16)
    attention_branch = dense_back(mixed_low, full_output)
    hidden_state = inputs + RESIDUAL_SCALE * attention_branch
    unit_two, inverse_two = normalize(hidden_state)
    normed_two = (unit_two * norm_feedforward).astype(jnp.bfloat16)
    gate_states = dense(normed_two, full_gate)
    up_states = dense(normed_two, full_up)
    sigmoid_gate = jax.nn.sigmoid(gate_states)
    swish = gate_states * sigmoid_gate
    activated_low = (swish * up_states).astype(jnp.bfloat16)
    feed_branch = dense_back(activated_low, full_down)
    layer_out = (hidden_state + RESIDUAL_SCALE * feed_branch).astype(jnp.bfloat16)
    upstream = cotangent.astype(jnp.float32)
    down_grad = (RESIDUAL_SCALE * upstream).astype(jnp.bfloat16)
    activation_grad = dense(down_grad, full_down)
    slope = sigmoid_gate * (1.0 + gate_states * (1.0 - sigmoid_gate))
    gate_grad = (activation_grad * up_states * slope).astype(jnp.bfloat16)
    up_grad = (activation_grad * swish).astype(jnp.bfloat16)
    normed_two_grad = dense_back(gate_grad, full_gate) + dense_back(up_grad, full_up)
    gain_part_two = jnp.sum(normed_two_grad * unit_two, axis=0)
    residual_grad = upstream + norm_backward(
        normed_two_grad, unit_two, inverse_two, norm_feedforward
    )
    branch_grad = (RESIDUAL_SCALE * residual_grad).astype(jnp.bfloat16)
    mixed_grad = dense(branch_grad, full_output)
    mixed_grad_low = mixed_grad.astype(jnp.bfloat16).reshape(
        token_count, KV_HEADS, per_group, HEAD_DIM
    )
    scores = attention_scores(query_turned, key_turned, visible)
    softmax_out = jnp.exp(scores - log_total)
    softmax_low = softmax_out.astype(jnp.bfloat16)
    probability_grad = jnp.einsum(
        "tkgd,ukd->kgtu", mixed_grad_low, value_heads, preferred_element_type=jnp.float32
    )
    row_inner = jnp.sum(softmax_out * probability_grad, axis=-1, keepdims=True)
    score_grad = (softmax_out * (probability_grad - row_inner)).astype(jnp.bfloat16)
    value_grad = jnp.einsum(
        "kgtu,tkgd->ukd", softmax_low, mixed_grad_low, preferred_element_type=jnp.float32
    )
    query_turn_grad = ATTENTION_SCALE * jnp.einsum(
        "kgtu,ukd->tkgd", score_grad, key_turned, preferred_element_type=jnp.float32
    )
    key_turn_grad = ATTENTION_SCALE * jnp.einsum(
        "kgtu,tkgd->ukd", score_grad, query_turned, preferred_element_type=jnp.float32
    )
    query_grad = unrotate(
        query_turn_grad.reshape(token_count, HEADS, HEAD_DIM), cosine_table, sine_table
    ).reshape(token_count, query_width)
    key_grad = unrotate(key_turn_grad, cosine_table, sine_table).reshape(token_count, kv_width)
    projection_grad = jnp.concatenate(
        [query_grad, key_grad, value_grad.reshape(token_count, kv_width)], axis=1
    ).astype(jnp.bfloat16)
    normed_one_grad = dense_back(projection_grad, full_input)
    gain_part_one = jnp.sum(normed_one_grad * unit_one, axis=0)
    tokens_grad = (
        residual_grad + norm_backward(normed_one_grad, unit_one, inverse_one, norm_attention)
    ).astype(jnp.bfloat16)
    small = jnp.concatenate(
        [gain_part_one[None], gain_part_two[None], jnp.zeros((6, gain_part_one.shape[0]), jnp.float32)]
    )
    attention_right = jnp.concatenate([projection_grad, mixed_low], axis=1)
    lefts = [normed_one.T, branch_grad.T, normed_two.T, down_grad.T]
    return layer_out, tokens_grad, lefts, attention_right, gate_grad, up_grad, activated_low, small


def on_device(
    shard_count,
    tokens_in,
    cotangent,
    segment_ids,
    parent_ids,
    weight_query,
    weight_key,
    weight_value,
    weight_output,
    weight_gate,
    weight_up,
    weight_down,
    norm_attention,
    norm_feedforward,
    moment_query,
    moment_key,
    moment_value,
    moment_output,
    moment_gate,
    moment_up,
    moment_down,
    variance_query,
    variance_key,
    variance_value,
    variance_output,
    variance_gate,
    variance_up,
    variance_down,
    moment_norm_attention,
    moment_norm_feedforward,
    variance_norm_attention,
    variance_norm_feedforward,
):
    query_width = weight_query.shape[1]
    kv_width = weight_key.shape[1]
    hidden_width = weight_gate.shape[1]
    positions, visible = tree_layout(segment_ids[0], parent_ids[0])
    cosine_table, sine_table = rope_tables(positions, HEAD_DIM)
    attention_rows = jnp.concatenate([weight_query, weight_key, weight_value, weight_output], axis=1)
    second_cut = query_width + kv_width
    third_cut = query_width + 2 * kv_width
    shards = [attention_rows, weight_gate, weight_up, weight_down]
    widths = (query_width, kv_width, hidden_width)
    if weight_query.shape[0] % 16 == 0:
        pair_cosine = jnp.concatenate([cosine_table, cosine_table], axis=1)
        pair_sine = jnp.concatenate([sine_table, sine_table], axis=1)
        (layer_out, tokens_grad, *lefts, attention_right, gate_grad, up_grad, activated_low, small) = run_layer(
            tokens_in, cotangent, norm_attention, norm_feedforward, pair_cosine, pair_sine,
            visible.astype(jnp.float32), shards, widths, shard_count)
    else:
        (layer_out, tokens_grad, lefts, attention_right, gate_grad, up_grad, activated_low, small) = layer_apart(
            tokens_in, cotangent, norm_attention, norm_feedforward, cosine_table, sine_table,
            visible, shards, widths, shard_count)
    weight_list = [
        weight_query,
        weight_key,
        weight_value,
        weight_output,
        weight_gate,
        weight_up,
        weight_down,
    ]
    moment_list = [
        moment_query,
        moment_key,
        moment_value,
        moment_output,
        moment_gate,
        moment_up,
        moment_down,
    ]
    variance_list = [
        variance_query,
        variance_key,
        variance_value,
        variance_output,
        variance_gate,
        variance_up,
        variance_down,
    ]
    blocks, small_total, norm_squares = scatter_gradients(
        lefts,
        [attention_right, gate_grad, up_grad, activated_low],
        small,
        shards,
        moment_list,
        variance_list,
        gradient_layout([weight.shape[1] for weight in weight_list]),
        shard_count,
    )
    gain_grad_one, gain_grad_two = small_total[0], small_total[1]
    step_total, weight_total = norm_squares[:7, 0], norm_squares[8:15, 0]
    weights_wide = [weight.astype(jnp.float32) for weight in weight_list]
    gradient_list = [
        part.astype(jnp.float32)
        for part in (
            blocks[0][:, :query_width],
            blocks[0][:, query_width:second_cut],
            blocks[0][:, second_cut:third_cut],
            blocks[0][:, third_cut:],
            blocks[1],
            blocks[2],
            blocks[3],
        )
    ]
    outcomes = [
        adam_direction(weight, gradient, moment, variance)
        for weight, gradient, moment, variance in zip(
            weights_wide, gradient_list, moment_list, variance_list
        )
    ]
    updates = []
    for matrix_index in range(7):
        factor = jnp.sqrt(weight_total[matrix_index]) * lax.rsqrt(
            step_total[matrix_index] + TRUST_EPS
        )
        updates.append(-STEP_RATE * factor * outcomes[matrix_index][2])
    gain_outcomes = [
        adam_direction(
            norm_attention, gain_grad_one, moment_norm_attention, variance_norm_attention
        ),
        adam_direction(
            norm_feedforward, gain_grad_two, moment_norm_feedforward, variance_norm_feedforward
        ),
    ]
    gain_weights = [norm_attention, norm_feedforward]
    gain_updates = []
    gain_pairs = []
    for gain_vector, entry in zip(gain_weights, gain_outcomes):
        gain_sum = jnp.sum(gain_vector * gain_vector)
        gain_step = jnp.sum(entry[2] * entry[2])
        gain_updates.append(
            -STEP_RATE * jnp.sqrt(gain_sum) * lax.rsqrt(gain_step + TRUST_EPS) * entry[2]
        )
        gain_pairs.append(jnp.stack([jnp.sqrt(gain_sum), jnp.sqrt(gain_step)]))
    matrix_pairs = jnp.stack([jnp.sqrt(weight_total), jnp.sqrt(step_total)], axis=1)
    norm_pairs = jnp.concatenate([matrix_pairs, jnp.stack(gain_pairs)], axis=0)
    return (
        layer_out,
        tokens_grad,
        updates[0],
        updates[1],
        updates[2],
        updates[3],
        updates[4],
        updates[5],
        updates[6],
        outcomes[0][0],
        outcomes[1][0],
        outcomes[2][0],
        outcomes[3][0],
        outcomes[4][0],
        outcomes[5][0],
        outcomes[6][0],
        outcomes[0][1],
        outcomes[1][1],
        outcomes[2][1],
        outcomes[3][1],
        outcomes[4][1],
        outcomes[5][1],
        outcomes[6][1],
        gain_updates[0],
        gain_updates[1],
        gain_outcomes[0][0],
        gain_outcomes[1][0],
        gain_outcomes[0][1],
        gain_outcomes[1][1],
        norm_pairs,
    )


def solution(mesh):
    in_specs = (
        P(("rep", "shard"), None),
        P(("rep", "shard"), None),
        P(("rep", "shard"), None),
        P(("rep", "shard"), None),
        P("shard", None),
        P("shard", None),
        P("shard", None),
        P("shard", None),
        P("shard", None),
        P("shard", None),
        P("shard", None),
        P(),
        P(),
        P("shard", None),
        P("shard", None),
        P("shard", None),
        P("shard", None),
        P("shard", None),
        P("shard", None),
        P("shard", None),
        P("shard", None),
        P("shard", None),
        P("shard", None),
        P("shard", None),
        P("shard", None),
        P("shard", None),
        P("shard", None),
        P(),
        P(),
        P(),
        P(),
    )
    out_specs = (
        P(("rep", "shard"), None),
        P(("rep", "shard"), None),
        P("shard", None),
        P("shard", None),
        P("shard", None),
        P("shard", None),
        P("shard", None),
        P("shard", None),
        P("shard", None),
        P("shard", None),
        P("shard", None),
        P("shard", None),
        P("shard", None),
        P("shard", None),
        P("shard", None),
        P("shard", None),
        P("shard", None),
        P("shard", None),
        P("shard", None),
        P("shard", None),
        P("shard", None),
        P("shard", None),
        P("shard", None),
        P(),
        P(),
        P(),
        P(),
        P(),
        P(),
        P(),
    )
    return jax.shard_map(
        functools.partial(on_device, mesh.shape["shard"]), mesh=mesh, in_specs=in_specs, out_specs=out_specs, check_vma=False
    )
```

```python
import functools

import jax
import jax.numpy as jnp
from jax import lax
from jax.experimental import pallas as pl
from jax.experimental.pallas import tpu as pltpu
from jax.sharding import PartitionSpec as P

MESH = pl.DeviceIdType.MESH

HEADS = 18
KV_HEADS = 6
HEAD_DIM = 64


ROPE_BASE = 10000.0
ATTENTION_SCALE = 0.125
RESIDUAL_SCALE = 1.0
NORM_EPS = 1e-05
BETA_FIRST = 0.9
BETA_SECOND = 0.999
ADAM_EPS = 1e-06
DECAY_RATE = 0.01
STEP_RATE = 0.25
TRUST_EPS = 1e-06
MASK_FILL = -1e30


def shard_factors(count):
    factors = []
    while count > 4:
        factors.append(4)
        count //= 4
    factors.append(count)
    return tuple(factors)

def coordinates(index, factors):
    out = []
    for factor in reversed(factors):
        out.append(lax.rem(index, factor))
        index = lax.div(index, factor)
    return out[::-1]

def index_of(coords, factors):
    index = 0
    for c, f in zip(coords, factors):
        index = index * f + c
    return index

def gather_chunks(width, blocks):
    out = []
    for b in range(blocks):
        wide, narrow = [], []
        start = 0
        n = width // 512
        kinds = [True, False, True, True, False, True][:n]
        for i in range(n):
            out.append((b, i * 512, 512, kinds[i % 6]))
    return out

def gather_kernel(factors, blocks, *refs):
    srcs, outs = refs[:blocks], refs[blocks:2*blocks]
    local_sem, send_sem, recv_sem = refs[2*blocks:]
    rep, shard = lax.axis_index("rep"), lax.axis_index("shard")
    y, core = lax.div(rep, 2), lax.rem(rep, 2)
    coords = coordinates(shard, factors)
    peers = []
    for i, f in enumerate(factors):
        ids = []
        for d in range(1, f):
            moved = list(coords); moved[i] = lax.rem(coords[i] + d, f)
            ids.append((rep, index_of(moved, factors)))
        peers.append(ids)
    peers.append([((1 - y) * 2 + core, shard)])
    peers.append([(y * 2 + 1 - core, shard)])
    flat = [p for ids in peers for p in ids]
    barrier = pltpu.get_barrier_semaphore()
    for p in flat:
        pl.semaphore_signal(barrier, inc=1, device_id=p, device_id_type=MESH)
    chunks = gather_chunks(srcs[0].shape[1], blocks)
    nph = len(factors) + 2
    base = []
    total = 0
    for ids in peers:
        base.append(total); total += len(ids)
    def columns(k):
        b, c0, w, split = chunks[k]
        if split:
            q = w // 4
            return c0 + (core * 2 + y) * q, q
        return c0 + core * (w // 2), w // 2
    locals_ = []
    for k, (b, c0, w, split) in enumerate(chunks):
        off, width = columns(k)
        cols = pl.ds(pl.multiple_of(off, 128), width)
        cp = pltpu.make_async_copy(srcs[b].at[:, cols], outs[b].at[tuple(coords) + (slice(None), cols)], local_sem.at[k])
        cp.start(); locals_.append(cp)
    pl.semaphore_wait(barrier, len(flat))
    def copies(k, ph):
        b, c0, w, split = chunks[k]
        off, width = columns(k)
        nf = len(factors)
        if ph < nf:
            lead = (slice(None),) * ph + tuple(coords[ph:])
        else:
            lead = (slice(None),) * nf
            if ph == nf + 1:
                off, width = c0 + core * (w // 2), w // 2
        cols = pl.ds(pl.multiple_of(off, 128), width)
        where = lead + (slice(None), cols)
        src = srcs[b].at[:, cols] if ph == 0 else outs[b].at[where]
        return [pltpu.make_async_remote_copy(src_ref=src, dst_ref=outs[b].at[where],
                  send_sem=send_sem.at[k, base[ph] + j], recv_sem=recv_sem.at[k, base[ph] + j], device_id=p, device_id_type=MESH)
                for j, p in enumerate(peers[ph])]
    n = len(chunks)
    started = {}
    def start(k, ph):
        cs = copies(k, ph)
        for c in cs: c.start()
        started[k, ph] = cs
    def phases(k):
        return [p for p in range(nph) if p != nph - 2 or chunks[k][3]]
    ahead = 4
    for k in range(min(ahead, n)):
        start(k, 0)
    for t in range(n + 2 * nph):
        for lag in range(nph - 1, -1, -1):
            k = t - 2 * lag
            if 0 <= k < n:
                ps = phases(k)
                if lag < len(ps):
                    for c in started[k, ps[lag]]: c.wait_recv()
                    if lag == 0:
                        locals_[k].wait()
                        if k + ahead < n:
                            start(k + ahead, 0)
                    if lag + 1 < len(ps): start(k, ps[lag + 1])
    for cs in started.values():
        for c in cs: c.wait_send()

def gather_weights(shards, shard_count, rep_count=4):
    blocks = len(shards)
    factors = shard_factors(shard_count)
    rows, width = shards[0].shape
    n = len(gather_chunks(width, blocks))
    total = sum(f - 1 for f in factors) + 2
    outs = pl.pallas_call(
        functools.partial(gather_kernel, factors, blocks),
        out_shape=[jax.ShapeDtypeStruct(factors + (rows, width), jnp.bfloat16)] * blocks,
        in_specs=[pl.BlockSpec(memory_space=pltpu.VMEM)] * blocks,
        out_specs=[pl.BlockSpec(memory_space=pl.ANY)] * blocks,
        scratch_shapes=[pltpu.SemaphoreType.DMA((n,)), pltpu.SemaphoreType.DMA((n, total)), pltpu.SemaphoreType.DMA((n, total))],
        compiler_params=pltpu.CompilerParams(collective_id=0, has_side_effects=True),
        name="gather_weights",
    )(*shards)
    return [o.reshape(shard_count * rows, width) for o in outs]


def head_half(odd, tile):
    lane = lax.broadcasted_iota(jnp.int32, tile.shape, 1)
    keep = lane >= HEAD_DIM if odd else lane < HEAD_DIM
    return jnp.where(keep, tile, jnp.zeros_like(tile))


def low_lane(shape):
    lane = lax.broadcasted_iota(jnp.int32, shape, 1)
    return lax.rem(lane, HEAD_DIM) < HEAD_DIM // 2


def turn(tile, cosine, sine):
    low = low_lane(tile.shape)
    turned = jnp.where(low, -pltpu.roll(tile, 128 - HEAD_DIM // 2, 1), pltpu.roll(tile, HEAD_DIM // 2, 1))
    return tile * cosine + turned * sine


def turn_back(tile, cosine, sine):
    low = low_lane(tile.shape)
    scaled = tile * sine
    turned = jnp.where(low, pltpu.roll(scaled, 128 - HEAD_DIM // 2, 1), -pltpu.roll(scaled, HEAD_DIM // 2, 1))
    return tile * cosine + turned


def spread(tile, odd):
    wide = tile.astype(jnp.float32)
    other = pltpu.roll(wide, HEAD_DIM, 1)
    lane = lax.broadcasted_iota(jnp.int32, wide.shape, 1)
    pick = (lane >= HEAD_DIM) if odd else (lane < HEAD_DIM)
    return jnp.where(pick, wide, other).astype(tile.dtype)


def dot_nn(a, b):
    return jnp.dot(a, b, preferred_element_type=jnp.float32)


def dot_nt(a, b):
    return lax.dot_general(a, b, (((1,), (1,)), ((), ())), preferred_element_type=jnp.float32)


def dot_tn(a, b):
    return jnp.dot(a.T, b, preferred_element_type=jnp.float32)


def layer_kernel(factors, widths, *refs):
    (tokens_ref, cot_ref, gain_one_ref, gain_two_ref, segment_ref, parent_ref, frequency_ref) = refs[:7]
    given = refs[7:14]
    (out_ref, grad_ref, one_t, branch_t, two_t, cot_t, right_a, right_g, right_u, right_d, gains_ref) = refs[14:25]
    w = refs[25:29]
    (one_low, query_low, key_two, value_two, log_ref, hidden_ref, two_low, gate_ref, up_ref, feed_ref,
     upstream_ref, mixed_grad_ref, kv_grad_ref, cosine_ref, sine_ref, mask_ref, staged) = refs[29:46]
    local_sem, send_sem, recv_sem, staged_sem = refs[46:]
    srcs = (staged,) + tuple(given[4:])
    staging, at = [], 0
    for j in range(4):
        width = given[j].shape[1]
        staging.append(pltpu.make_async_copy(given[j], staged.at[:, pl.ds(at, width)], staged_sem.at[j]))
        at += width
    for c in staging:
        c.start()
    query_width, kv_width, hidden_width = widths
    kv_start, value_start, out_start = query_width, query_width + kv_width, query_width + 2 * kv_width
    rep, shard = lax.axis_index("rep"), lax.axis_index("shard")
    y, core = lax.div(rep, 2), lax.rem(rep, 2)
    coords = coordinates(shard, factors)
    nf = len(factors)
    whole = (slice(None),) * nf
    peers = []
    for i, f in enumerate(factors):
        ids = []
        for d in range(1, f):
            moved = list(coords)
            moved[i] = lax.rem(coords[i] + d, f)
            ids.append((rep, index_of(moved, factors)))
        peers.append(ids)
    peers.append([((1 - y) * 2 + core, shard)])
    peers.append([(y * 2 + 1 - core, shard)])
    flat = [p for ids in peers for p in ids]
    barrier = pltpu.get_barrier_semaphore()
    for p in flat:
        pl.semaphore_signal(barrier, inc=1, device_id=p, device_id_type=MESH)
    chunks = gather_chunks(3072, 4)
    nph = nf + 2
    base, total = [], 0
    for ids in peers:
        base.append(total)
        total += len(ids)

    def columns(k):
        b, c0, width, split = chunks[k]
        if split:
            return c0 + (core * 2 + y) * (width // 4), width // 4
        return c0 + core * (width // 2), width // 2

    def own_source(k):
        b = chunks[k][0]
        off, width = columns(k)
        return srcs[b].at[:, pl.ds(pl.multiple_of(off, 128), width)]

    locals_ = []
    for c in staging:
        c.wait()
    for k, (b, _, _, _) in enumerate(chunks):
        off, width = columns(k)
        cols = pl.ds(pl.multiple_of(off, 128), width)
        copy = pltpu.make_async_copy(own_source(k), w[b].at[tuple(coords) + (slice(None), cols)], local_sem.at[k])
        copy.start()
        locals_.append(copy)
    pl.semaphore_wait(barrier, len(flat))

    def copies(k, ph):
        b, c0, wide, _ = chunks[k]
        off, width = columns(k)
        if ph < nf:
            lead = (slice(None),) * ph + tuple(coords[ph:])
        else:
            lead = whole
            if ph == nf + 1:
                off, width = c0 + core * (wide // 2), wide // 2
        where = lead + (slice(None), pl.ds(pl.multiple_of(off, 128), width))
        src = own_source(k) if ph == 0 else w[b].at[where]
        return [
            pltpu.make_async_remote_copy(
                src_ref=src, dst_ref=w[b].at[where], send_sem=send_sem.at[k, base[ph] + j],
                recv_sem=recv_sem.at[k, base[ph] + j], device_id=p, device_id_type=MESH)
            for j, p in enumerate(peers[ph])
        ]

    n = len(chunks)
    started = {}

    def start(k, ph):
        cs = copies(k, ph)
        for c in cs:
            c.start()
        started[k, ph] = cs

    def phases(k):
        return [p for p in range(nph) if p != nph - 2 or chunks[k][3]]

    def weight(b, c0, c1):
        got = w[b][whole + (slice(None), slice(c0, c1))]
        return got.reshape(-1, c1 - c0)

    def gain(ref):
        return ref[...]

    def open_norm():
        inputs = tokens_ref[...].astype(jnp.float32)
        inverse = lax.rsqrt(jnp.mean(inputs * inputs, axis=-1, keepdims=True) + NORM_EPS)
        low = (inputs * inverse * gain(gain_one_ref)).astype(jnp.bfloat16)
        one_low[...] = low
        one_t[...] = low.T
        cot_t[...] = cot_ref[...].T

    def tables():
        def exact(flags):
            return jnp.where(flags, 1.0, 0.0)

        count = segment_ref.shape[1]
        segments = parent_ref.shape[1]
        line = lax.broadcasted_iota(jnp.int32, (128, 128), 0)
        lane = lax.broadcasted_iota(jnp.int32, (128, 128), 1)
        ancestry = jnp.where(line == lane, 1.0, 0.0)
        identity = ancestry
        parents = parent_ref[...]
        wide = jnp.concatenate([parents, jnp.full((1, 128 - segments), -1, jnp.int32)], axis=1)
        ancestry = jnp.minimum(ancestry + exact(line == wide), 1.0)
        reach = 1
        while reach < segments:
            low = ancestry.astype(jnp.bfloat16)
            ancestry = jnp.minimum(dot_nn(low, low), 1.0)
            reach *= 2
        hot = exact(lax.broadcasted_iota(jnp.int32, (128, count), 0) == segment_ref[...]).astype(jnp.bfloat16)
        lengths = jnp.broadcast_to(jnp.sum(hot.astype(jnp.float32), axis=1, keepdims=True), (128, 128))
        earlier = exact(line < lane)
        weights = (ancestry - identity - earlier).astype(jnp.bfloat16)
        offset = dot_tn(weights, lengths.astype(jnp.bfloat16))
        places = dot_tn(hot, offset.astype(jnp.bfloat16))
        places = places + lax.broadcasted_iota(jnp.int32, places.shape, 0).astype(jnp.float32)
        angles = places * frequency_ref[...]
        cosine_ref[...] = jnp.cos(angles)
        sine_ref[...] = jnp.sin(angles)
        above = dot_nn(ancestry.astype(jnp.bfloat16), hot).astype(jnp.bfloat16)
        seen = dot_tn(above, hot)
        ordered = lax.broadcasted_iota(jnp.int32, seen.shape, 1) <= lax.broadcasted_iota(jnp.int32, seen.shape, 0)
        mask_ref[...] = jnp.where(ordered & (seen > 0.5), 1.0, 0.0)

    def project(c0, c1):
        low = one_low[...]
        for c in range(c0, min(c1, out_start), 256):
            e = min(c + 256, c1, out_start)
            got = dot_nn(low, weight(0, c, e))
            for s in range(c, e, 128):
                tile = got[:, s - c:s - c + 128]
                if s < kv_start:
                    query_low[:, s:s + 128] = turn(tile, cosine_ref[...], sine_ref[...]).astype(jnp.bfloat16)
                elif s < value_start:
                    turned = turn(tile, cosine_ref[...], sine_ref[...]).astype(jnp.bfloat16)
                    j = (s - kv_start) // 64
                    key_two[j] = spread(turned, False)
                    key_two[j + 1] = spread(turned, True)
                else:
                    low_tile = tile.astype(jnp.bfloat16)
                    j = (s - value_start) // 64
                    value_two[j] = spread(low_tile, False)
                    value_two[j + 1] = spread(low_tile, True)

    per_group = HEADS // KV_HEADS

    def scores_of(query, j):
        scores = ATTENTION_SCALE * dot_nt(query, key_two[j])
        return jnp.where(mask_ref[...] > 0, scores, MASK_FILL)

    sets = KV_HEADS // 2

    def over_sets(body):
        def run(i):
            def one(u, carry):
                body(i, u)
                return carry
            lax.fori_loop(0, sets, one, 0)
        return run

    def pair_columns(i, u, start=0):
        return pl.ds(pl.multiple_of(start + (per_group * u + i) * 128, 128), 128)

    def attend(i, u):
        tile = query_low[:, pair_columns(i, u)]
        halves = []
        for odd in (False, True):
            h = 2 * per_group * u + 2 * i + int(odd)
            j = 2 * u + (2 * i + int(odd)) // per_group
            scores = scores_of(head_half(odd, tile), j)
            top = jnp.max(scores, axis=-1, keepdims=True)
            raised = jnp.exp(scores - top)
            log_total = top + jnp.log(jnp.sum(raised, axis=-1, keepdims=True))
            log_ref[h] = log_total
            probs = jnp.exp(scores - log_total).astype(jnp.bfloat16)
            halves.append(dot_nn(probs, value_two[j]))
        lane = lax.broadcasted_iota(jnp.int32, halves[0].shape, 1)
        right_a[:, pair_columns(i, u, out_start)] = jnp.where(
            lane < HEAD_DIM, halves[0], halves[1]).astype(jnp.bfloat16)

    def mix():
        hidden_ref[...] = tokens_ref[...].astype(jnp.float32) + dot_nt(
            right_a[:, out_start:], weight(0, out_start, out_start + query_width))

    def second_norm():
        hidden = hidden_ref[...]
        inverse = lax.rsqrt(jnp.mean(hidden * hidden, axis=-1, keepdims=True) + NORM_EPS)
        low = (hidden * inverse * gain(gain_two_ref)).astype(jnp.bfloat16)
        two_low[...] = low
        two_t[...] = low.T

    def gate(c0, c1):
        for c in range(c0, c1, 256):
            gate_ref[:, c:c + 256] = dot_nn(two_low[...], weight(1, c, c + 256))

    def up(c0, c1):
        for c in range(c0, c1, 256):
            got = dot_nn(two_low[...], weight(2, c, c + 256))
            up_ref[:, c:c + 256] = got
            g = gate_ref[:, c:c + 256]
            right_d[:, c:c + 256] = (g * jax.nn.sigmoid(g) * got).astype(jnp.bfloat16)

    first_down = [True]

    def down(c0, c1):
        piece = weight(3, c0, c1)
        feed = dot_nt(right_d[:, c0:c1], piece)
        for c in range(c0, c1, 256):
            back = dot_nn(cot_ref[...], weight(3, c, c + 256))
            g, u = gate_ref[:, c:c + 256], up_ref[:, c:c + 256]
            s = jax.nn.sigmoid(g)
            right_g[:, c:c + 256] = (back * u * (s * (1.0 + g * (1.0 - s)))).astype(jnp.bfloat16)
            right_u[:, c:c + 256] = (back * (g * s)).astype(jnp.bfloat16)
        up_part = dot_nt(right_g[:, c0:c1], weight(1, c0, c1)) + dot_nt(right_u[:, c0:c1], weight(2, c0, c1))
        if first_down[0]:
            feed_ref[...] = feed
            upstream_ref[...] = up_part
            first_down[0] = False
        else:
            feed_ref[...] += feed
            upstream_ref[...] += up_part

    def close_feed():
        hidden = hidden_ref[...]
        out_ref[...] = (hidden + feed_ref[...]).astype(jnp.bfloat16)
        inverse = lax.rsqrt(jnp.mean(hidden * hidden, axis=-1, keepdims=True) + NORM_EPS)
        unit = hidden * inverse
        upstream = upstream_ref[...]
        gains_ref[1:2, :] = jnp.sum(upstream * unit, axis=0, keepdims=True)
        scaled = upstream * gain(gain_two_ref)
        residual = cot_ref[...].astype(jnp.float32) + inverse * (
            scaled - unit * jnp.mean(scaled * unit, axis=-1, keepdims=True))
        hidden_ref[...] = residual
        low = residual.astype(jnp.bfloat16)
        branch_t[...] = low.T
        mixed_grad_ref[...] = dot_nn(low, weight(0, out_start, out_start + query_width)).astype(jnp.bfloat16)
        kv_grad_ref[...] = jnp.zeros_like(kv_grad_ref)

    def attend_back(i, u):
        cols = pair_columns(i, u)
        tile, grad_tile = query_low[:, cols], mixed_grad_ref[:, cols]
        halves = []
        for odd in (False, True):
            h = 2 * per_group * u + 2 * i + int(odd)
            j = 2 * u + (2 * i + int(odd)) // per_group
            query, grad = head_half(odd, tile), head_half(odd, grad_tile)
            probs = jnp.exp(scores_of(query, j) - log_ref[h])
            prob_grad = dot_nt(grad, value_two[j])
            inner = jnp.sum(probs * prob_grad, axis=-1, keepdims=True)
            score_grad = (probs * (prob_grad - inner)).astype(jnp.bfloat16)
            halves.append(dot_nn(score_grad, key_two[j]))
            kv_grad_ref[j] += dot_tn(score_grad, query)
            kv_grad_ref[KV_HEADS + j] += dot_tn(probs.astype(jnp.bfloat16), grad)
        lane = lax.broadcasted_iota(jnp.int32, halves[0].shape, 1)
        both = ATTENTION_SCALE * jnp.where(lane < HEAD_DIM, halves[0], halves[1])
        right_a[:, cols] = turn_back(both, cosine_ref[...], sine_ref[...]).astype(jnp.bfloat16)

    def fold(j):
        first, second = kv_grad_ref[j], kv_grad_ref[j + 1]
        first = first + pltpu.roll(first, HEAD_DIM, 1)
        second = second + pltpu.roll(second, HEAD_DIM, 1)
        lane = lax.broadcasted_iota(jnp.int32, first.shape, 1)
        return jnp.where(lane < HEAD_DIM, first, second)

    def close_attention():
        for j in range(0, KV_HEADS, 2):
            c = kv_start + j * HEAD_DIM
            right_a[:, c:c + 128] = turn_back(
                ATTENTION_SCALE * fold(j), cosine_ref[...], sine_ref[...]).astype(jnp.bfloat16)
            c = value_start + j * HEAD_DIM
            right_a[:, c:c + 128] = fold(KV_HEADS + j).astype(jnp.bfloat16)
        upstream = dot_nt(right_a[:, :out_start], weight(0, 0, out_start))
        inputs = tokens_ref[...].astype(jnp.float32)
        inverse = lax.rsqrt(jnp.mean(inputs * inputs, axis=-1, keepdims=True) + NORM_EPS)
        unit = inputs * inverse
        gains_ref[0:1, :] = jnp.sum(upstream * unit, axis=0, keepdims=True)
        scaled = upstream * gain(gain_one_ref)
        grad_ref[...] = (hidden_ref[...] + inverse * (
            scaled - unit * jnp.mean(scaled * unit, axis=-1, keepdims=True))).astype(jnp.bfloat16)

    per_block = n // 4
    tasks = [((), 3.0, open_norm), ((), 1.5, tables)]
    for c in range(per_block):
        c0, c1 = chunks[c][1], chunks[c][1] + chunks[c][2]
        if c0 < out_start:
            tasks.append(((c,), 0.8, functools.partial(project, c0, c1)))
    for i in range(per_group):
        tasks.append(((), 3.0, functools.partial(over_sets(attend), i)))
    tasks.append((tuple(range(per_block)), 1.5, mix))
    tasks.append(((), 1.2, second_norm))
    for b, run, cost in ((1, gate, 0.5), (2, up, 0.7), (3, down, 2.5)):
        for c in range(per_block):
            k = b * per_block + c
            tasks.append(((k,), cost, functools.partial(run, chunks[k][1], chunks[k][1] + chunks[k][2])))
    tasks.append(((), 3.0, close_feed))
    for i in range(per_group):
        tasks.append(((), 7.0, functools.partial(over_sets(attend_back), i)))
    tasks.append(((), 3.0, close_attention))
    finished = set()
    gains_ref[...] = jnp.zeros_like(gains_ref)

    def advance(budget):
        while tasks and budget > 0 and all(k in finished for k in tasks[0][0]):
            _, cost, run = tasks.pop(0)
            run()
            budget -= cost

    ahead = 4
    for k in range(min(ahead, n)):
        start(k, 0)
    for t in range(n + 2 * nph):
        for lag in range(nph - 1, -1, -1):
            k = t - 2 * lag
            if 0 <= k < n:
                ps = phases(k)
                if lag < len(ps):
                    for c in started[k, ps[lag]]:
                        c.wait_recv()
                    if lag == 0:
                        locals_[k].wait()
                        if k + ahead < n:
                            start(k + ahead, 0)
                    if lag + 1 < len(ps):
                        start(k, ps[lag + 1])
                    else:
                        finished.add(k)
        advance(BUDGET)
    advance(1e9)
    for cs in started.values():
        for c in cs:
            c.wait_send()


BUDGET = 3.5


def run_layer(tokens, cotangent, gain_one, gain_two, segments, parents, weights, widths, shard_count):
    factors = shard_factors(shard_count)
    count, model = tokens.shape
    query_width, kv_width, hidden_width = widths
    rows = weights[0].shape[0]
    half = HEAD_DIM // 2
    frequency = jnp.power(ROPE_BASE, jnp.arange(half, dtype=jnp.float32) * (-2.0 / HEAD_DIM))
    frequency = jnp.tile(frequency, 128 // half).reshape(1, 128)
    n = len(gather_chunks(3072, 4))
    links = sum(f - 1 for f in factors) + 2
    bf, f32 = jnp.bfloat16, jnp.float32
    vm, anywhere = pl.BlockSpec(memory_space=pltpu.VMEM), pl.BlockSpec(memory_space=pl.ANY)
    turned = jax.ShapeDtypeStruct((model, count), bf)
    flat = jax.ShapeDtypeStruct((count, model), bf)
    wide = jax.ShapeDtypeStruct((count, hidden_width), bf)
    return pl.pallas_call(
        functools.partial(layer_kernel, factors, widths),
        out_shape=[flat, flat, turned, turned, turned, turned, wide, wide, wide, wide,
                   jax.ShapeDtypeStruct((8, model), f32)],
        in_specs=[vm] * 7 + [anywhere] * 7,
        out_specs=[vm] * 11,
        scratch_shapes=[pltpu.VMEM(factors + (rows, hidden_width), bf)] * 4 + [
            pltpu.VMEM((count, model), bf),
            pltpu.VMEM((count, query_width), bf),
            pltpu.VMEM((KV_HEADS, count, 128), bf),
            pltpu.VMEM((KV_HEADS, count, 128), bf),
            pltpu.VMEM((HEADS, count, 1), f32),
            pltpu.VMEM((count, model), f32),
            pltpu.VMEM((count, model), bf),
            pltpu.VMEM((count, hidden_width), f32),
            pltpu.VMEM((count, hidden_width), f32),
            pltpu.VMEM((count, model), f32),
            pltpu.VMEM((count, model), f32),
            pltpu.VMEM((count, query_width), bf),
            pltpu.VMEM((2 * KV_HEADS, count, 128), f32),
            pltpu.VMEM((count, 128), f32),
            pltpu.VMEM((count, 128), f32),
            pltpu.VMEM((count, count), f32),
            pltpu.VMEM((rows, 3072), bf),
            pltpu.SemaphoreType.DMA((n,)),
            pltpu.SemaphoreType.DMA((n, links)),
            pltpu.SemaphoreType.DMA((n, links)),
            pltpu.SemaphoreType.DMA((4,)),
        ],
        compiler_params=pltpu.CompilerParams(collective_id=0, has_side_effects=True, vmem_limit_bytes=67043328),
        name="run_layer",
    )(tokens, cotangent, gain_one.reshape(1, -1), gain_two.reshape(1, -1), segments, parents, frequency, *weights)


def scatter_kernel(factors, parts, blocks, layout, *refs):
    nf = len(factors)
    nl = len(layout["lefts"])
    lefts = refs[:nl]
    rights = refs[nl:nl + blocks]
    small_in = refs[nl + blocks]
    at = nl + blocks + 1
    params = layout["params"]
    weights = refs[at:at + params]
    moments = refs[at + params:at + 2 * params]
    variances = refs[at + 2 * params:at + 3 * params]
    at += 3 * params
    outs = refs[at:at + blocks]
    small_out, norm_out = refs[at + blocks:at + blocks + 2]
    scratch = list(refs[at + blocks + 2:])
    stage, pair_in, wide_y, final = scratch[:4]
    lean = scratch[4:4 + nf]
    quart = scratch[4 + nf:4 + 2 * nf]
    lean_y = scratch[4 + 2 * nf]
    small = scratch[5 + 2 * nf:5 + 2 * nf + nf + 2]
    rest = scratch[5 + 2 * nf + nf + 2:]
    norm_slots = rest[:nf]
    held_m, held_v, held_w, step_acc, weight_acc = rest[nf:nf + 5]
    send_sem, recv_sem, out_sem, small_send, small_recv, fetch_sem, norm_send, norm_recv = rest[nf + 5:]
    rows = final.shape[1]
    steps = final.shape[0]
    ring = stage.shape[0]
    rep, shard = lax.axis_index("rep"), lax.axis_index("shard")
    y, core = lax.div(rep, 2), lax.rem(rep, 2)
    coords = coordinates(shard, factors)
    y_peer = ((1 - y) * 2 + core, shard)
    core_peer = (y * 2 + 1 - core, shard)

    def factor_peer(i, d):
        moved = list(coords)
        moved[i] = lax.rem(coords[i] + d, factors[i])
        return (rep, index_of(moved, factors)), moved[i]

    everyone = [y_peer, core_peer]
    for i, f in enumerate(factors):
        everyone += [factor_peer(i, d)[0] for d in range(1, f)]
    barrier = pltpu.get_barrier_semaphore()
    for p in everyone:
        pl.semaphore_signal(barrier, inc=1, device_id=p, device_id_type=MESH)

    order = list(range(nf - 1, -1, -1))
    column = {"core": 0, "y_wide": 1, "y_lean": 2, "y_back": 3, "core_back": 4}
    used = 5
    for i in order:
        column["lean", i] = used
        used += factors[i] - 1
        column["quart", i] = used
        used += factors[i] - 1

    def remote(k, c, src, dst, peer):
        return pltpu.make_async_remote_copy(
            src_ref=src, dst_ref=dst, send_sem=send_sem.at[lax.rem(k, ring), c],
            recv_sem=recv_sem.at[k, c], device_id=peer, device_id_type=MESH)

    half, quarter = 512, 128
    mine = pl.multiple_of(core * half, half)
    other = pl.multiple_of((1 - core) * half, half)
    my_q = pl.multiple_of(256 + y * quarter, quarter)
    other_q = pl.multiple_of(256 + (1 - y) * quarter, quarter)
    whole = (slice(None),) * nf

    def core_copy(k):
        slot = lax.rem(k, ring)
        return [remote(k, column["core"], stage.at[(slot,) + whole + (slice(None), pl.ds(other, half))], pair_in.at[k], core_peer)]

    def y_wide_copy(k):
        return [remote(k, column["y_wide"], pair_in.at[(k,) + whole + (slice(None), pl.ds(other_q, quarter))], wide_y.at[k], y_peer)]

    def view(kind, i, k):
        if i == nf - 1:
            if kind == "lean":
                return pair_in.at[(k,) + whole + (slice(None), pl.ds(0, 256))]
            return wide_y.at[k]
        box = lean if kind == "lean" else quart
        return box[i + 1].at[k, 0]

    def factor_copies(kind, i, k):
        box = lean if kind == "lean" else quart
        source = view(kind, i, k)
        out = []
        for d in range(1, factors[i]):
            peer, j = factor_peer(i, d)
            out.append(remote(k, column[kind, i] + d - 1, source.at[(slice(None),) * i + (j,)], box[i].at[k, d - 1], peer))
        return out

    def factor_sum(kind, i, k):
        box = lean if kind == "lean" else quart
        total = view(kind, i, k)[(slice(None),) * i + (coords[i],)].astype(jnp.float32)
        for d in range(1, factors[i]):
            total = total + box[i][k, d - 1].astype(jnp.float32)
        return total

    def y_lean_copy(k):
        return [remote(k, column["y_lean"], lean[0].at[k, 0], lean_y.at[k], y_peer)]

    def y_back_copy(k):
        where = (k, slice(None), pl.ds(pl.multiple_of(mine + my_q, quarter), quarter))
        return [remote(k, column["y_back"], final.at[where], final.at[where], y_peer)]

    def core_back_copy(k):
        where = (k, slice(None), pl.ds(mine, half))
        return [remote(k, column["core_back"], final.at[where], final.at[where], core_peer)]

    def begin(copies):
        for c in copies:
            c.start()

    def finish(copies):
        for c in copies:
            c.wait()

    def product(left, right_ref, cols, slot, at, part):
        width = cols[1] - cols[0]
        for c in range(0, width, 256):
            w = min(256, width - c)
            right = right_ref[:, cols[0] + c:cols[0] + c + w]
            if rows % 16 == 0:
                lhs = left[:, part].reshape(-1, left.shape[-1])
                got = jnp.dot(lhs, right, preferred_element_type=jnp.float32).astype(jnp.bfloat16)
                stage[(slot,) + whole + (slice(None), slice(at + c, at + c + w))] = got.reshape(factors + (rows, w))
            else:
                def one(s, carry):
                    got = jnp.dot(left[s, part], right, preferred_element_type=jnp.float32).astype(jnp.bfloat16)
                    where = tuple(coordinates(s, factors))
                    stage[(slot,) + where + (slice(None), slice(at + c, at + c + w))] = got
                    return carry
                lax.fori_loop(0, left.shape[0], one, 0)

    groups = layout["groups"]

    def compute(k):
        group, part = lax.div(k, parts), lax.rem(k, parts)
        slot = lax.rem(k, ring)
        for g, pieces in enumerate(groups):
            @pl.when(group == g)
            def _():
                at = 0
                for left, right, c0, c1 in pieces:
                    product(lefts[left], rights[right], (c0, c1), slot, at, part)
                    at += c1 - c0

    def out_copies(k, g, part):
        block, start = layout["places"][g]
        return pltpu.make_async_copy(final.at[k], outs[block].at[pl.ds(pl.multiple_of(part * rows, rows), rows), pl.ds(start, 1024)], out_sem.at[k])

    stages = [[] for _ in range(nf + 5)]

    def stage0(k):
        compute(k)
        begin(core_copy(k))

    def stage1(k):
        finish(core_copy(k))
        slot = lax.rem(k, ring)
        pair_in[k] = (pair_in[k].astype(jnp.float32) + stage[(slot,) + whole + (slice(None), pl.ds(mine, half))].astype(jnp.float32)).astype(jnp.bfloat16)
        begin(y_wide_copy(k))
        begin(factor_copies("lean", order[0], k))

    def middle(pos):
        def run(k):
            i = order[pos]
            if pos == 0:
                finish(y_wide_copy(k))
                wide_y[k] = (wide_y[k].astype(jnp.float32) + pair_in[(k,) + whole + (slice(None), pl.ds(my_q, quarter))].astype(jnp.float32)).astype(jnp.bfloat16)
            else:
                before = order[pos - 1]
                finish(factor_copies("quart", before, k))
                quart[before][k, 0] = factor_sum("quart", before, k).astype(jnp.bfloat16)
            begin(factor_copies("quart", i, k))
            finish(factor_copies("lean", i, k))
            lean[i][k, 0] = factor_sum("lean", i, k).astype(jnp.bfloat16)
            if pos + 1 < nf:
                begin(factor_copies("lean", order[pos + 1], k))
            else:
                begin(y_lean_copy(k))
        return run

    def settle(k):
        finish(factor_copies("quart", 0, k))
        final[k, :, pl.ds(pl.multiple_of(mine + my_q, quarter), quarter)] = factor_sum("quart", 0, k).astype(jnp.bfloat16)
        begin(y_back_copy(k))
        finish(y_lean_copy(k))
        final[k, :, pl.ds(mine, 256)] = (lean[0][k, 0].astype(jnp.float32) + lean_y[k].astype(jnp.float32)).astype(jnp.bfloat16)

    def give(k):
        finish(y_back_copy(k))
        begin(core_back_copy(k))

    hold = held_m.shape[0]

    def fetches(k, g, part):
        slot = lax.rem(k, hold)
        down = pl.ds(pl.multiple_of(part * rows, rows), rows)
        found = []
        c = 0
        for j, (param, first, width) in enumerate(layout["cuts"][g]):
            for box, source, column_of in ((held_m, moments, 0), (held_v, variances, 4), (held_w, weights, 8)):
                found.append(pltpu.make_async_copy(
                    source[param].at[down, pl.ds(first, width)], box.at[slot, :, pl.ds(c, width)],
                    fetch_sem.at[slot, column_of + j]))
            c += width
        return found

    def by_group(k, action):
        group, part = lax.div(k, parts), lax.rem(k, parts)
        for g in range(len(groups)):
            pl.when(group == g)(lambda g=g: action(k, g, part))

    def fetch(k):
        by_group(k, lambda k, g, part: begin(fetches(k, g, part)))

    def leave(k):
        finish(core_back_copy(k))
        by_group(k, lambda k, g, part: out_copies(k, g, part).start())
        by_group(k, lambda k, g, part: finish(fetches(k, g, part)))
        slot, group = lax.rem(k, hold), lax.div(k, parts)
        gradient = final[k].astype(jnp.float32)
        weight = held_w[slot].astype(jnp.float32)
        direction = adam_direction(weight, gradient, held_m[slot], held_v[slot])[2]
        step_acc[group] += jnp.sum(direction * direction, axis=0, keepdims=True)
        weight_acc[group] += jnp.sum(weight * weight, axis=0, keepdims=True)

    lags = list(layout["lags"])
    stages = [stage0, stage1] + [middle(p) for p in range(nf)] + [settle, give, leave, fetch]
    lags.append(lags[-1] - 3)
    step_acc[...] = jnp.zeros_like(step_acc)
    weight_acc[...] = jnp.zeros_like(weight_acc)

    small_stages = [("core", 2, core, lambda d: core_peer), ("y", 2, y, lambda d: y_peer)]
    for i in order:
        small_stages.append((i, factors[i], coords[i], lambda d, i=i: factor_peer(i, d)[0]))
    small_base = []
    count = 0
    for s in small_stages:
        small_base.append(count)
        count += s[1] - 1

    def small_copies(j):
        _, f, own, peer = small_stages[j]
        return [pltpu.make_async_remote_copy(src_ref=small[j].at[own], dst_ref=small[j].at[own],
                 send_sem=small_send.at[small_base[j] + d - 1], recv_sem=small_recv.at[small_base[j] + d - 1],
                 device_id=peer(d), device_id_type=MESH) for d in range(1, f)]

    def small_step(j):
        if j > 0:
            finish(small_copies(j - 1))
            total = small[j - 1][0]
            for a in range(1, small_stages[j - 1][1]):
                total = total + small[j - 1][a]
        else:
            total = small_in[...]
        if j < len(small_stages):
            small[j][small_stages[j][2]] = total
            begin(small_copies(j))
        else:
            small_out[...] = total

    pl.semaphore_wait(barrier, len(everyone))

    def step(t, carry):
        for lag, run in reversed(list(zip(lags, stages))):
            k = t - lag
            @pl.when((k >= 0) & (k < steps))
            def _():
                run(k)
        for j in range(len(small_stages) + 1):
            pl.when(t == j + 1)(functools.partial(small_step, j))
        return carry
    lax.fori_loop(0, steps + max(lags), step, 0)

    lines = lax.broadcasted_iota(jnp.int32, (16, 128), 0)
    total = jnp.zeros((16, 128), jnp.float32)
    for acc, offset in ((step_acc, 0), (weight_acc, 8)):
        sums = [None] * params
        for g in range(len(groups)):
            c = 0
            for param, _, width in layout["cuts"][g]:
                value = jnp.sum(acc[g, :, c:c + width])
                sums[param] = value if sums[param] is None else sums[param] + value
                c += width
        for param in range(params):
            total = jnp.where(lines == offset + param, sums[param], total)
    done = 0
    for i in order:
        norm_slots[i][coords[i]] = total
        copies = []
        for d in range(1, factors[i]):
            where = norm_slots[i].at[coords[i]]
            copies.append(pltpu.make_async_remote_copy(
                src_ref=where, dst_ref=where, send_sem=norm_send.at[done], recv_sem=norm_recv.at[done],
                device_id=factor_peer(i, d)[0], device_id_type=MESH))
            done += 1
        begin(copies)
        finish(copies)
        total = norm_slots[i][0]
        for a in range(1, factors[i]):
            total = total + norm_slots[i][a]
    norm_out[...] = total

    def drain(k, carry):
        group, part = lax.div(k, parts), lax.rem(k, parts)
        for g in range(len(groups)):
            pl.when(group == g)(lambda g=g: out_copies(k, g, part).wait())
        return carry
    lax.fori_loop(0, steps, drain, 0)


def scatter_gradients(lefts, rights, small, weights, moments, variances, layout, shard_count, lags=None):
    factors = shard_factors(shard_count)
    nf = len(factors)
    model, tokens = lefts[0].shape
    rows_all = model // shard_count
    parts = 3 if rows_all % 48 == 0 else 1
    rows = rows_all // parts
    blocks = len(rights)
    steps = len(layout["groups"]) * parts
    layout = dict(layout)
    layout["lags"] = lags or ([0, 1] + [1 + 2 * (p + 1) for p in range(nf + 1)] + [1 + 2 * (nf + 1) + 1, 1 + 2 * (nf + 1) + 2])
    ring = layout["lags"][-1] + 1 if layout["lags"][-1] < 4 else 4
    layout["lefts"] = lefts
    turned = [v.reshape(shard_count, parts, rows, tokens) for v in lefts]
    bf = jnp.bfloat16
    lean = [pltpu.VMEM((steps, factors[i] - 1) + factors[:i] + (rows, 256), bf) for i in range(nf)]
    quart = [pltpu.VMEM((steps, factors[i] - 1) + factors[:i] + (rows, 128), bf) for i in range(nf)]
    order = list(range(nf - 1, -1, -1))
    smalls = [pltpu.VMEM((f,) + small.shape, jnp.float32) for f in [2, 2] + [factors[i] for i in order]]
    ncol = 5 + 2 * sum(f - 1 for f in factors)
    nsmall = 2 + sum(f - 1 for f in factors)
    vm = pl.BlockSpec(memory_space=pltpu.VMEM)
    layout["lefts"] = list(range(len(lefts)))
    params = layout["params"] = len(moments)
    anywhere = pl.BlockSpec(memory_space=pl.ANY)
    hold = 5
    outs = pl.pallas_call(
        functools.partial(scatter_kernel, factors, parts, blocks, layout),
        out_shape=[jax.ShapeDtypeStruct((rows_all, rights[0].shape[1]), bf)] * blocks + [jax.ShapeDtypeStruct(small.shape, jnp.float32), jax.ShapeDtypeStruct((16, 128), jnp.float32)],
        in_specs=[vm] * (len(lefts) + blocks + 1) + [anywhere] * (3 * params),
        out_specs=[anywhere] * blocks + [vm, vm],
        scratch_shapes=[
            pltpu.VMEM((ring,) + factors + (rows, 1024), bf),
            pltpu.VMEM((steps,) + factors + (rows, 512), bf),
            pltpu.VMEM((steps,) + factors + (rows, 128), bf),
            pltpu.VMEM((steps, rows, 1024), bf),
        ] + lean + quart + [pltpu.VMEM((steps, rows, 256), bf)] + smalls + [
            pltpu.VMEM((f, 16, 128), jnp.float32) for f in factors
        ] + [
            pltpu.VMEM((hold, rows, 1024), jnp.float32),
            pltpu.VMEM((hold, rows, 1024), jnp.float32),
            pltpu.VMEM((hold, rows, 1024), bf),
            pltpu.VMEM((len(layout["groups"]), 1, 1024), jnp.float32),
            pltpu.VMEM((len(layout["groups"]), 1, 1024), jnp.float32),
            pltpu.SemaphoreType.DMA((ring, ncol)),
            pltpu.SemaphoreType.DMA((steps, ncol)),
            pltpu.SemaphoreType.DMA((steps,)),
            pltpu.SemaphoreType.DMA((nsmall,)),
            pltpu.SemaphoreType.DMA((nsmall,)),
            pltpu.SemaphoreType.DMA((hold, 12)),
            pltpu.SemaphoreType.DMA((nsmall,)),
            pltpu.SemaphoreType.DMA((nsmall,)),
        ],
        compiler_params=pltpu.CompilerParams(collective_id=1, has_side_effects=True, vmem_limit_bytes=62 << 20),
        name="scatter_gradients",
    )(*turned, *rights, small, *weights, *moments, *variances)
    return outs[:blocks], outs[blocks], outs[blocks + 1]


def gradient_layout(widths):
    spans, start = [], 0
    for param, width in enumerate(widths[:4]):
        spans.append((param, start, start + width))
        start += width
    cut = spans[3][1]
    groups, places, cuts = [], [], []
    for block in (1, 2, 3):
        for c in range(0, widths[3 + block], 1024):
            groups.append([(3 if block == 3 else 2, block, c, c + 1024)])
            places.append((block, c))
            cuts.append([(3 + block, c, 1024)])
    for c in range(0, start, 1024):
        pieces = [(0, 0, c, min(c + 1024, cut)), (1, 0, max(c, cut), c + 1024)]
        groups.append([p for p in pieces if p[2] < p[3]])
        places.append((0, c))
        found = []
        for param, low, high in spans:
            if max(low, c) < min(high, c + 1024):
                found.append((param, max(low, c) - low, min(high, c + 1024) - max(low, c)))
        cuts.append(found)
    return {"groups": groups, "places": places, "cuts": cuts}


def tree_layout(segment_row, parent_row):
    segment_count = parent_row.shape[0]
    labels = jnp.arange(segment_count, dtype=jnp.int32)
    parent_hot = (parent_row[:, None] == labels[None, :]).astype(jnp.int32)
    identity = (labels[:, None] == labels[None, :]).astype(jnp.int32)

    ancestry = jnp.minimum(identity + parent_hot, 1)
    reach = 1
    while reach < segment_count:
        ancestry = jnp.minimum(jnp.sum(ancestry[:, :, None] * ancestry[None, :, :], axis=1), 1)
        reach *= 2
    segment_hot = (segment_row[:, None] == labels[None, :]).astype(jnp.int32)
    lengths = jnp.sum(segment_hot, axis=0, dtype=jnp.int32)
    depth_sum = jnp.dot(ancestry - identity, lengths)
    token_index = jnp.arange(segment_row.shape[0], dtype=jnp.int32)
    earlier = jnp.sum(
        (segment_row[None, :] < segment_row[:, None]).astype(jnp.int32), axis=1, dtype=jnp.int32
    )
    positions = token_index - earlier + jnp.dot(segment_hot, depth_sum)
    reach_count = jnp.dot(jnp.dot(segment_hot, ancestry), segment_hot.T)
    visible = (reach_count > 0) & (token_index[None, :] <= token_index[:, None])
    return (positions, visible)


def rope_tables(positions, head_size):
    half_size = head_size // 2
    exponent = jnp.arange(half_size, dtype=jnp.float32) * (-2.0 / head_size)
    frequency = jnp.power(ROPE_BASE, exponent)
    angles = positions.astype(jnp.float32)[:, None] * frequency[None, :]
    angles = jnp.concatenate([angles, angles], axis=1)
    return (jnp.cos(angles), jnp.sin(angles))


def rotate(states, cosine_table, sine_table):
    half_size = states.shape[-1] // 2
    turned = jnp.concatenate([-states[..., half_size:], states[..., :half_size]], axis=-1)
    return states * cosine_table[:, None, :] + turned * sine_table[:, None, :]


def unrotate(gradient, cosine_table, sine_table):
    half_size = gradient.shape[-1] // 2
    scaled = gradient * sine_table[:, None, :]
    turned = jnp.concatenate([scaled[..., half_size:], -scaled[..., :half_size]], axis=-1)
    return gradient * cosine_table[:, None, :] + turned


def dense(left_side, right_side):
    return jnp.dot(left_side, right_side, preferred_element_type=jnp.float32)


def dense_back(left_side, right_side):
    return lax.dot_general(
        left_side, right_side, (((1,), (1,)), ((), ())), preferred_element_type=jnp.float32
    )


def dense_rows(left_side, right_side):
    return lax.dot_general(
        left_side, right_side, (((0,), (0,)), ((), ())), preferred_element_type=jnp.float32
    )


def normalize(inputs):
    inverse_root = lax.rsqrt(jnp.mean(inputs * inputs, axis=-1, keepdims=True) + NORM_EPS)
    return (inputs * inverse_root, inverse_root)


def norm_backward(upstream, unit_rows, inverse_root, gain_vector):
    scaled = upstream * gain_vector
    return inverse_root * (
        scaled - unit_rows * jnp.mean(scaled * unit_rows, axis=-1, keepdims=True)
    )


def attention_scores(query_turned, key_turned, visible):
    scores = ATTENTION_SCALE * jnp.einsum(
        "tkgd,ukd->kgtu", query_turned, key_turned, preferred_element_type=jnp.float32
    )
    return jnp.where(visible[None, None], scores, MASK_FILL)


def adam_direction(weight, gradient, moment, variance):
    next_moment = BETA_FIRST * moment + (1.0 - BETA_FIRST) * gradient
    next_variance = BETA_SECOND * variance + (1.0 - BETA_SECOND) * gradient * gradient
    direction = next_moment / (jnp.sqrt(next_variance) + ADAM_EPS) + DECAY_RATE * weight
    return (next_moment, next_variance, direction)


def apply_kernel(items, params, *refs):
    grads, weights = refs[:4], refs[4:4 + params]
    at = 4 + params
    moments, variances = refs[at:at + params], refs[at + params:at + 2 * params]
    at += 2 * params
    norm_ref, small_ref = refs[at:at + 2]
    gains, gain_moments, gain_variances = refs[at + 2:at + 4], refs[at + 4:at + 6], refs[at + 6:at + 8]
    at += 8
    updates, next_moments, next_variances = refs[at:at + params], refs[at + params:at + 2 * params], refs[at + 2 * params:at + 3 * params]
    at += 3 * params
    gain_outs, pairs_ref = refs[at:at + 6], refs[at + 6]
    held_g, held_w, held_m, held_v, held_u, in_sem, out_sem = refs[at + 7:]
    ring = held_m.shape[0]
    rows = held_m.shape[1]
    chunk = 16 if rows % 16 == 0 else rows

    def inward(i):
        param, c0, width, block, start = items[i]
        slot = i % ring
        pairs = ((grads[block].at[:, pl.ds(start, width)], held_g), (weights[param].at[:, pl.ds(c0, width)], held_w),
                 (moments[param].at[:, pl.ds(c0, width)], held_m), (variances[param].at[:, pl.ds(c0, width)], held_v))
        return [pltpu.make_async_copy(src, box.at[slot, :, pl.ds(0, width)], in_sem.at[slot, j])
                for j, (src, box) in enumerate(pairs)]

    def outward(i):
        param, c0, width, _, _ = items[i]
        slot = i % ring
        pairs = ((held_m, next_moments), (held_v, next_variances), (held_u, updates))
        return [pltpu.make_async_copy(box.at[slot, :, pl.ds(0, width)], dst[param].at[:, pl.ds(c0, width)], out_sem.at[slot, j])
                for j, (box, dst) in enumerate(pairs)]

    n = len(items)
    for i in range(min(2, n)):
        for c in inward(i):
            c.start()
    for j in range(2):
        outcome = adam_direction(gains[j][...], small_ref[j:j + 1, :], gain_moments[j][...], gain_variances[j][...])
        gain_sum = jnp.sum(gains[j][...] * gains[j][...], axis=1, keepdims=True)
        step_sum = jnp.sum(outcome[2] * outcome[2], axis=1, keepdims=True)
        gain_outs[j][...] = -STEP_RATE * jnp.sqrt(gain_sum) * lax.rsqrt(step_sum + TRUST_EPS) * outcome[2]
        gain_outs[2 + j][...] = outcome[0]
        gain_outs[4 + j][...] = outcome[1]
        line = lax.broadcasted_iota(jnp.int32, (8, 128), 0)
        lane = lax.broadcasted_iota(jnp.int32, (8, 128), 1)
        own = jnp.where(lane == 0, jnp.sqrt(gain_sum), jnp.sqrt(step_sum))
        if j == 0:
            matrix = jnp.where(lane == 0, jnp.sqrt(norm_ref[8:16, :]), jnp.sqrt(norm_ref[0:8, :]))
            pairs_ref[0:8, :] = jnp.where(line == 7, own, matrix)
        else:
            pairs_ref[8:16, :] = own
    for i in range(n):
        param, c0, width, _, _ = items[i]
        slot = i % ring
        if i + 2 < n:
            if i + 2 >= ring:
                for c in outward(i + 2 - ring):
                    c.wait()
            for c in inward(i + 2):
                c.start()
        for c in inward(i):
            c.wait()
        factor = -STEP_RATE * (
            jnp.sqrt(norm_ref[8 + param:9 + param, 0:1]) * lax.rsqrt(norm_ref[param:param + 1, 0:1] + TRUST_EPS))

        def body(r, carry):
            where = (slot, pl.ds(pl.multiple_of(r * chunk, chunk), chunk), slice(0, width))
            outcome = adam_direction(
                held_w[where].astype(jnp.float32), held_g[where].astype(jnp.float32), held_m[where], held_v[where])
            held_m[where] = outcome[0]
            held_v[where] = outcome[1]
            held_u[where] = factor * outcome[2]
            return carry
        lax.fori_loop(0, rows // chunk, body, 0)
        for c in outward(i):
            c.start()
    for i in range(max(0, n - ring), n):
        for c in outward(i):
            c.wait()


def apply_steps(grads, weights, moments, variances, norms, small, gains, gain_moments, gain_variances):
    params = len(weights)
    rows = weights[0].shape[0]
    items, start = [], 0
    for param, weight in enumerate(weights):
        width = weight.shape[1]
        if param < 4:
            items.append((param, 0, width, 0, start))
            start += width
        else:
            items += [(param, c, 1024, param - 3, c) for c in range(0, width, 1024)]
    widest = max(item[2] for item in items)
    ring = 4
    f32, bf = jnp.float32, jnp.bfloat16
    vm, anywhere = pl.BlockSpec(memory_space=pltpu.VMEM), pl.BlockSpec(memory_space=pl.ANY)
    shapes = [jax.ShapeDtypeStruct(w.shape, f32) for w in weights]
    line = jax.ShapeDtypeStruct((1, gains[0].shape[0]), f32)
    flat = [v.reshape(1, -1) for v in (*gains, *gain_moments, *gain_variances)]
    outs = pl.pallas_call(
        functools.partial(apply_kernel, items, params),
        out_shape=shapes * 3 + [line] * 6 + [jax.ShapeDtypeStruct((16, 128), f32)],
        in_specs=[anywhere] * (4 + 3 * params) + [vm] * 8,
        out_specs=[anywhere] * (3 * params) + [vm] * 7,
        scratch_shapes=[
            pltpu.VMEM((ring, rows, widest), bf),
            pltpu.VMEM((ring, rows, widest), bf),
            pltpu.VMEM((ring, rows, widest), f32),
            pltpu.VMEM((ring, rows, widest), f32),
            pltpu.VMEM((ring, rows, widest), f32),
            pltpu.SemaphoreType.DMA((ring, 4)),
            pltpu.SemaphoreType.DMA((ring, 3)),
        ],
        compiler_params=pltpu.CompilerParams(vmem_limit_bytes=60 << 20),
        name="apply_steps",
    )(*grads, *weights, *moments, *variances, norms, small, *flat)
    return outs[:params], outs[params:2 * params], outs[2 * params:3 * params], outs[3 * params:3 * params + 6], outs[-1]


def layer_apart(
    tokens_in, cotangent, norm_attention, norm_feedforward, segment_ids, parent_ids, weights, widths, shard_count
):
    query_width, kv_width, hidden_width = widths
    token_count = tokens_in.shape[0]
    per_group = HEADS // KV_HEADS
    positions, visible = tree_layout(segment_ids[0], parent_ids[0])
    cosine_table, sine_table = rope_tables(positions, HEAD_DIM)
    shards = [jnp.concatenate(weights[:4], axis=1), *weights[4:]]
    inputs = tokens_in.astype(jnp.float32)
    unit_one, inverse_one = normalize(inputs)
    normed_one = (unit_one * norm_attention).astype(jnp.bfloat16)
    second_cut = query_width + kv_width
    third_cut = query_width + 2 * kv_width
    full_attention, full_gate, full_up, full_down = gather_weights(shards, shard_count)
    full_input, full_output = full_attention[:, :third_cut], full_attention[:, third_cut:]
    input_states = dense(normed_one, full_input)
    query_states = input_states[:, :query_width]
    key_states = input_states[:, query_width:second_cut]
    value_states = input_states[:, second_cut:]
    query_turned = rotate(
        query_states.reshape(token_count, HEADS, HEAD_DIM), cosine_table, sine_table
    ).astype(jnp.bfloat16)
    query_turned = query_turned.reshape(token_count, KV_HEADS, per_group, HEAD_DIM)
    key_turned = rotate(
        key_states.reshape(token_count, KV_HEADS, HEAD_DIM), cosine_table, sine_table
    ).astype(jnp.bfloat16)
    value_heads = value_states.astype(jnp.bfloat16).reshape(token_count, KV_HEADS, HEAD_DIM)
    scores = attention_scores(query_turned, key_turned, visible)
    row_max = jnp.max(scores, axis=-1, keepdims=True)
    log_total = row_max + jnp.log(jnp.sum(jnp.exp(scores - row_max), axis=-1, keepdims=True))
    softmax_low = jnp.exp(scores - log_total).astype(jnp.bfloat16)
    mixed_low = jnp.einsum(
        "kgtu,ukd->tkgd", softmax_low, value_heads, preferred_element_type=jnp.float32
    )
    mixed_low = mixed_low.reshape(token_count, query_width).astype(jnp.bfloat16)
    attention_branch = dense_back(mixed_low, full_output)
    hidden_state = inputs + RESIDUAL_SCALE * attention_branch
    unit_two, inverse_two = normalize(hidden_state)
    normed_two = (unit_two * norm_feedforward).astype(jnp.bfloat16)
    gate_states = dense(normed_two, full_gate)
    up_states = dense(normed_two, full_up)
    sigmoid_gate = jax.nn.sigmoid(gate_states)
    swish = gate_states * sigmoid_gate
    activated_low = (swish * up_states).astype(jnp.bfloat16)
    feed_branch = dense_back(activated_low, full_down)
    layer_out = (hidden_state + RESIDUAL_SCALE * feed_branch).astype(jnp.bfloat16)
    upstream = cotangent.astype(jnp.float32)
    down_grad = (RESIDUAL_SCALE * upstream).astype(jnp.bfloat16)
    activation_grad = dense(down_grad, full_down)
    slope = sigmoid_gate * (1.0 + gate_states * (1.0 - sigmoid_gate))
    gate_grad = (activation_grad * up_states * slope).astype(jnp.bfloat16)
    up_grad = (activation_grad * swish).astype(jnp.bfloat16)
    normed_two_grad = dense_back(gate_grad, full_gate) + dense_back(up_grad, full_up)
    gain_part_two = jnp.sum(normed_two_grad * unit_two, axis=0)
    residual_grad = upstream + norm_backward(
        normed_two_grad, unit_two, inverse_two, norm_feedforward
    )
    branch_grad = (RESIDUAL_SCALE * residual_grad).astype(jnp.bfloat16)
    mixed_grad = dense(branch_grad, full_output)
    mixed_grad_low = mixed_grad.astype(jnp.bfloat16).reshape(
        token_count, KV_HEADS, per_group, HEAD_DIM
    )
    scores = attention_scores(query_turned, key_turned, visible)
    softmax_out = jnp.exp(scores - log_total)
    softmax_low = softmax_out.astype(jnp.bfloat16)
    probability_grad = jnp.einsum(
        "tkgd,ukd->kgtu", mixed_grad_low, value_heads, preferred_element_type=jnp.float32
    )
    row_inner = jnp.sum(softmax_out * probability_grad, axis=-1, keepdims=True)
    score_grad = (softmax_out * (probability_grad - row_inner)).astype(jnp.bfloat16)
    value_grad = jnp.einsum(
        "kgtu,tkgd->ukd", softmax_low, mixed_grad_low, preferred_element_type=jnp.float32
    )
    query_turn_grad = ATTENTION_SCALE * jnp.einsum(
        "kgtu,ukd->tkgd", score_grad, key_turned, preferred_element_type=jnp.float32
    )
    key_turn_grad = ATTENTION_SCALE * jnp.einsum(
        "kgtu,tkgd->ukd", score_grad, query_turned, preferred_element_type=jnp.float32
    )
    query_grad = unrotate(
        query_turn_grad.reshape(token_count, HEADS, HEAD_DIM), cosine_table, sine_table
    ).reshape(token_count, query_width)
    key_grad = unrotate(key_turn_grad, cosine_table, sine_table).reshape(token_count, kv_width)
    projection_grad = jnp.concatenate(
        [query_grad, key_grad, value_grad.reshape(token_count, kv_width)], axis=1
    ).astype(jnp.bfloat16)
    normed_one_grad = dense_back(projection_grad, full_input)
    gain_part_one = jnp.sum(normed_one_grad * unit_one, axis=0)
    tokens_grad = (
        residual_grad + norm_backward(normed_one_grad, unit_one, inverse_one, norm_attention)
    ).astype(jnp.bfloat16)
    small = jnp.concatenate(
        [gain_part_one[None], gain_part_two[None], jnp.zeros((6, gain_part_one.shape[0]), jnp.float32)]
    )
    attention_right = jnp.concatenate([projection_grad, mixed_low], axis=1)
    lefts = [normed_one.T, branch_grad.T, normed_two.T, down_grad.T]
    return layer_out, tokens_grad, lefts, attention_right, gate_grad, up_grad, activated_low, small


def on_device(
    shard_count,
    tokens_in,
    cotangent,
    segment_ids,
    parent_ids,
    weight_query,
    weight_key,
    weight_value,
    weight_output,
    weight_gate,
    weight_up,
    weight_down,
    norm_attention,
    norm_feedforward,
    moment_query,
    moment_key,
    moment_value,
    moment_output,
    moment_gate,
    moment_up,
    moment_down,
    variance_query,
    variance_key,
    variance_value,
    variance_output,
    variance_gate,
    variance_up,
    variance_down,
    moment_norm_attention,
    moment_norm_feedforward,
    variance_norm_attention,
    variance_norm_feedforward,
):
    query_width = weight_query.shape[1]
    kv_width = weight_key.shape[1]
    hidden_width = weight_gate.shape[1]
    weight_list = [
        weight_query,
        weight_key,
        weight_value,
        weight_output,
        weight_gate,
        weight_up,
        weight_down,
    ]
    moment_list = [
        moment_query,
        moment_key,
        moment_value,
        moment_output,
        moment_gate,
        moment_up,
        moment_down,
    ]
    variance_list = [
        variance_query,
        variance_key,
        variance_value,
        variance_output,
        variance_gate,
        variance_up,
        variance_down,
    ]
    widths = (query_width, kv_width, hidden_width)
    if weight_query.shape[0] % 16 == 0:
        (layer_out, tokens_grad, *lefts, attention_right, gate_grad, up_grad, activated_low, small) = run_layer(
            tokens_in, cotangent, norm_attention, norm_feedforward, segment_ids, parent_ids, weight_list,
            widths, shard_count)
    else:
        (layer_out, tokens_grad, lefts, attention_right, gate_grad, up_grad, activated_low, small) = layer_apart(
            tokens_in, cotangent, norm_attention, norm_feedforward, segment_ids, parent_ids, weight_list,
            widths, shard_count)
    blocks, small_total, norm_squares = scatter_gradients(
        lefts,
        [attention_right, gate_grad, up_grad, activated_low],
        small,
        weight_list,
        moment_list,
        variance_list,
        gradient_layout([weight.shape[1] for weight in weight_list]),
        shard_count,
    )
    updates, next_moments, next_variances, gain_outs, pairs = apply_steps(
        blocks, weight_list, moment_list, variance_list, norm_squares, small_total,
        (norm_attention, norm_feedforward), (moment_norm_attention, moment_norm_feedforward),
        (variance_norm_attention, variance_norm_feedforward))
    return (
        layer_out,
        tokens_grad,
        *updates,
        *next_moments,
        *next_variances,
        *[v.reshape(-1) for v in gain_outs],
        pairs[:9, :2],
    )


def solution(mesh):
    in_specs = (
        P(("rep", "shard"), None),
        P(("rep", "shard"), None),
        P(("rep", "shard"), None),
        P(("rep", "shard"), None),
        P("shard", None),
        P("shard", None),
        P("shard", None),
        P("shard", None),
        P("shard", None),
        P("shard", None),
        P("shard", None),
        P(),
        P(),
        P("shard", None),
        P("shard", None),
        P("shard", None),
        P("shard", None),
        P("shard", None),
        P("shard", None),
        P("shard", None),
        P("shard", None),
        P("shard", None),
        P("shard", None),
        P("shard", None),
        P("shard", None),
        P("shard", None),
        P("shard", None),
        P(),
        P(),
        P(),
        P(),
    )
    out_specs = (
        P(("rep", "shard"), None),
        P(("rep", "shard"), None),
        P("shard", None),
        P("shard", None),
        P("shard", None),
        P("shard", None),
        P("shard", None),
        P("shard", None),
        P("shard", None),
        P("shard", None),
        P("shard", None),
        P("shard", None),
        P("shard", None),
        P("shard", None),
        P("shard", None),
        P("shard", None),
        P("shard", None),
        P("shard", None),
        P("shard", None),
        P("shard", None),
        P("shard", None),
        P("shard", None),
        P("shard", None),
        P(),
        P(),
        P(),
        P(),
        P(),
        P(),
        P(),
    )
    return jax.shard_map(
        functools.partial(on_device, mesh.shape["shard"]), mesh=mesh, in_specs=in_specs, out_specs=out_specs, check_vma=False
    )
```
